32 devices in a mesh: cfd: 16 (over z, x, core), ac: 2 (over y).
Axes of the slice: x: 2, y: 2, z: 4, core: 2. Of those that a mesh axis runs over, the one named last changes fastest.
Arguments:
- surface_raw: bfloat16 [5, 4096, 1024], P(None, ('cfd', 'ac')), may hold values from -6 to 6
- area_normals: bfloat16 [3, 4096], P(None, ('cfd', 'ac')), may hold values from -6 to 6
- kernel_weights: bfloat16 [2, 3, 2048, 4096], P(None, None, None, ('cfd', 'ac')), may hold values from -0.078125 to 0.078125
- block_map: int32 [2, 16, 16], P('ac', 'cfd'), may hold values from 0 to 15, as said below
- band_observers: int32 [16, 128], replicated, may hold values from 0 to 2047, as said below
- band_lags: int32 [16], replicated, may hold values from 0 to 511
Outputs:
- acoustic: float32 [2048, 512], P('cfd', 'ac')
The draws below stay inside these ranges and needn't reach their ends.
Inputs may be any that keep to these rules, and one draw needn't show every extreme that they name: block_map[j, s, :] is a permutation of 0 to 15 for every j and s. `band_observers`: every observer appears exactly once.
All inputs are finite; a program needn't handle non-finite values.
Results may differ from the reference program's by a relative error of at most 0.0042.
Values may be sent and summed in bfloat16 or wider, within the bound.
A program may use at most 64 MiB of HBM per device.

```python
import jax
import jax.numpy as jnp
from jax import lax

OBS = 2048
BANDS = 16
OBS_BAND = 128
TAPS = 2
BLOCK = 8
FACES = 4096
WINDOW = 1024
OUT_STEPS = 512
N_CFD = 16
N_AC = 2


def draw_band_observers(key, part):
    shuffled = jax.random.permutation(jax.random.fold_in(key, 11), OBS)
    return shuffled.astype(jnp.int32).reshape(BANDS, OBS // BANDS)


def draw_block_map(key, part):
    key_list = jax.random.split(jax.random.fold_in(key, 23), N_AC * N_CFD)
    orders = jax.vmap(lambda single_key: jax.random.permutation(single_key, N_CFD))(key_list)
    return orders.astype(jnp.int32).reshape(N_AC, N_CFD, N_CFD)


def set_ends(entries, stream_key, low, top_value):
    longest = entries.shape.index(max(entries.shape))
    spots = []
    for shift in (0, 1):
        where = [jax.random.randint(jax.random.fold_in(stream_key, axis), (), 0, length) for axis, length in enumerate(entries.shape)]
        where[longest] = (where[longest] + shift) % entries.shape[longest]
        spots.append(tuple(where))
    return entries.at[spots[0]].set(low).at[spots[1]].set(top_value)


def spiked(entries, rng, source, target, parts, factor):
    owner, partner = [(jnp.arange(entries.shape[axis_at]) // (entries.shape[axis_at] // parts)).reshape([-1 if axis == axis_at else 1 for axis in range(entries.ndim)]) for axis_at in (source, target)]
    chosen = jax.random.permutation(rng, parts)[partner]
    strong = (owner == chosen) | (owner == (partner + parts // 2) % parts)
    return jnp.where(strong, factor * entries, entries)


def block_scale(rng, shape, pieces, least, high):
    def one(dim, shards_of):
        draws = jax.random.uniform(jax.random.fold_in(jax.random.fold_in(rng, 6), dim), (shards_of,), jnp.float32, least / len(pieces), high / len(pieces))
        return jnp.repeat(jnp.exp(draws), shape[dim] // shards_of).reshape((-1,) + (1,) * (len(shape) - dim - 1))

    factor_of = one(*pieces[0])
    for cut in pieces[1:]:
        factor_of = factor_of * one(*cut)
    return factor_of


def gaussian(rng, dims, width, most, cuts=(), kind=jnp.bfloat16):
    values = width * jax.random.normal(rng, dims, jnp.float32)
    if cuts:
        values = values * block_scale(rng, dims, cuts, -0.22, 0.18)
    return jnp.clip(values, -most, most).astype(kind)


def gaussian_with(key, dims, scale, limit, cuts, heavy, held_as=jnp.bfloat16):
    result = scale * jax.random.normal(key, dims, jnp.float32)
    if cuts:
        result = result * block_scale(key, dims, cuts, -0.22, 0.18)
    return jnp.clip(spiked(result, jax.random.fold_in(key, 3), *heavy), -limit, limit).astype(held_as)


def setup_inputs(seed: int = 0) -> dict:
    seeds = jax.random.split(jax.random.key(seed), 7)
    surface_raw = gaussian(seeds[0], (5, FACES, WINDOW), 1.0, 6.0, ((1, 32),))
    area_normals = gaussian(seeds[1], (3, FACES), 1.0, 6.0, ((1, 32),))
    kernel_weights = gaussian_with(seeds[2], (TAPS, 3, OBS, FACES), (6 * FACES) ** -0.5, 0.078125, ((3, 32),), (3, 2, 32, 2.75))
    block_map = draw_block_map(jax.random.fold_in(seeds[6], 71), 0)
    band_observers = draw_band_observers(jax.random.fold_in(seeds[6], 71), 0)
    band_lags = set_ends(jax.random.randint(seeds[5], (BANDS,), 0, OUT_STEPS), jax.random.fold_in(seeds[5], 1), 0, OUT_STEPS - 1).astype(jnp.int32)
    return dict(surface_raw=surface_raw, area_normals=area_normals, kernel_weights=kernel_weights, block_map=block_map, band_observers=band_observers, band_lags=band_lags)


def thickness(surface, normals):
    along = surface[2].astype(jnp.float32) * normals[0].astype(jnp.float32)[:, None]
    along = along + surface[3].astype(jnp.float32) * normals[1].astype(jnp.float32)[:, None]
    along = along + surface[4].astype(jnp.float32) * normals[2].astype(jnp.float32)[:, None]
    return (surface[1].astype(jnp.float32) * along).astype(jnp.bfloat16)


def rates(series):
    step = series[:, 1:].astype(jnp.float32) - series[:, :-1].astype(jnp.float32)
    first = jnp.zeros((series.shape[0], 1), jnp.float32)
    return jnp.concatenate([first, step], axis=1).astype(jnp.bfloat16)


def reference(surface_raw, area_normals, kernel_weights, block_map, band_observers, band_lags):
    thick = thickness(surface_raw, area_normals)
    stacked = jnp.stack([thick, surface_raw[0]])
    shaped = stacked.reshape(2, N_CFD, N_AC, N_CFD, BLOCK, WINDOW)
    picks = jnp.transpose(block_map, (1, 0, 2))[None, :, :, :, None, None]
    moved = jnp.take_along_axis(shaped, picks, axis=3)
    moved = jnp.transpose(moved, (0, 3, 2, 1, 4, 5)).reshape(2, FACES, WINDOW)
    sources = jnp.stack([rates(moved[0]), rates(moved[1]), moved[1]])

    def one_band(acoustic, band_index):
        members = band_observers[band_index]
        delay = band_lags[band_index]
        start = (band_index * OBS_BAND).astype(jnp.int32)
        chosen = lax.dynamic_slice_in_dim(kernel_weights, start, OBS_BAND, 2).astype(jnp.float32)
        windows = jnp.stack([lax.dynamic_slice_in_dim(sources, (OUT_STEPS - delay - shift_step).astype(jnp.int32), OUT_STEPS, 2) for shift_step in range(TAPS)]).astype(jnp.float32)
        contribution = jnp.einsum("kcof,kcft->ot", chosen, windows, precision=lax.Precision.HIGHEST)
        return acoustic.at[members].set(contribution), None

    initial = jnp.zeros((OBS, OUT_STEPS), jnp.float32)
    acoustic, _ = lax.scan(one_band, initial, jnp.arange(BANDS, dtype=jnp.int32))
    return acoustic
```

```python
import functools

import jax
import jax.numpy as jnp
from jax import lax
from jax.experimental import pallas as pl
from jax.experimental.pallas import tpu as pltpu
from jax.sharding import PartitionSpec as P

LANES = 128


def prepare_kernel(src_ref, normals_ref, surface_ref, out_ref):
    along = surface_ref[2].astype(jnp.float32) * normals_ref[:, 0:1]
    along = along + surface_ref[3].astype(jnp.float32) * normals_ref[:, 1:2]
    along = along + surface_ref[4].astype(jnp.float32) * normals_ref[:, 2:3]
    thick = (surface_ref[1].astype(jnp.float32) * along).astype(jnp.bfloat16)
    both = jnp.concatenate([thick, surface_ref[0]], axis=0)
    rows = both.shape[0]
    column = lax.broadcasted_iota(jnp.int32, (rows, rows), 1)
    onehot = jnp.where(column == src_ref[...], 1.0, 0.0).astype(jnp.bfloat16)
    picked = jnp.dot(onehot, both, preferred_element_type=jnp.float32)
    out_ref[...] = picked.astype(jnp.bfloat16)


def prepare(surface_raw, area_normals, block_order):
    faces, steps = surface_raw.shape[1:]
    blocks = block_order.shape[0]
    size = faces // blocks
    src = (
        jnp.arange(2, dtype=jnp.int32)[None, :, None] * faces
        + block_order[:, None, None] * size
        + jnp.arange(size, dtype=jnp.int32)[None, None, :]
    ).reshape(2 * faces, 1)
    return pl.pallas_call(
        prepare_kernel,
        out_shape=jax.ShapeDtypeStruct((2 * faces, steps), jnp.bfloat16),
        name="prepare",
    )(src, area_normals.T.astype(jnp.float32), surface_raw)


def scatter_bands(lags_ref, ids_ref, arrived_ref, weights_ref, sources, band, rows):
    index = pl.program_id(0)
    taps, terms, width, faces = weights_ref.shape
    steps = sources.shape[1]
    out_len = steps // 2
    chunks = out_len // LANES

    @pl.when(index == 0)
    def _():
        series = arrived_ref[...].astype(jnp.float32)
        if len(arrived_ref.shape) == 4:
            thick = series[:, 0].reshape(faces, steps)
            pressure = series[:, 1].reshape(faces, steps)
        else:
            thick, pressure = series[:faces], series[faces:]
        step = lax.broadcasted_iota(jnp.int32, (faces, steps), 1)

        def rate(x):
            moved = jnp.where(step > 0, x - pltpu.roll(x, 1, 1), 0.0)
            return moved.astype(jnp.bfloat16).astype(jnp.float32)

        for c, x in enumerate((rate(thick), rate(pressure), pressure)):
            for k in range(taps):
                late = pltpu.roll(x, k, 1) if k else x
                sources[pl.ds((k * terms + c) * faces, faces), :] = late.astype(jnp.bfloat16)

    start = out_len - lags_ref[index]
    tile = jnp.minimum(start // LANES, steps // LANES - chunks - 1)
    rest = start - tile * LANES
    shift = lax.rem(LANES - rest, LANES)
    chosen = jnp.concatenate(
        [weights_ref[k, c] for k in range(taps) for c in range(terms)], axis=1
    )
    window = sources[:, pl.ds(pl.multiple_of(tile * LANES, LANES), out_len + LANES)]
    wide = jnp.dot(chosen, window, preferred_element_type=jnp.float32)
    lane = lax.broadcasted_iota(jnp.int32, (width, LANES), 1)
    parts = [
        pltpu.roll(wide[:, t * LANES : (t + 1) * LANES], shift, 1) for t in range(chunks + 1)
    ]
    for t in range(chunks):
        band[pl.ds(t, width, stride=chunks), :] = jnp.where(
            lane < LANES - rest, parts[t], parts[t + 1]
        )

    unroll = 32

    @pl.loop(0, width // unroll)
    def _(group):
        slots = [group * unroll + m for m in range(unroll)]
        places = [ids_ref[index * width + slot] for slot in slots]
        values = [
            band[pl.ds(pl.multiple_of(slot * chunks, chunks), chunks), :] for slot in slots
        ]
        for place, value in zip(places, values):
            rows[pl.ds(pl.multiple_of(place * chunks, chunks), chunks), :] = value


def halves_kernel(
    lags_ref, ids_ref, mine_ref, arrived_ref, weights_ref, kept_ref, sent_ref, sources, band, rows
):
    scatter_bands(lags_ref, ids_ref, arrived_ref, weights_ref, sources, band, rows)
    pairs, height, out_len = kept_ref.shape
    chunks = out_len // LANES
    mine = mine_ref[0]

    @pl.when(pl.program_id(0) == pl.num_programs(0) - 1)
    def _():
        for pair in range(pairs):
            for t in range(chunks):
                lanes = slice(t * LANES, (t + 1) * LANES)
                for out, owner in ((kept_ref, 2 * pair + mine), (sent_ref, 2 * pair + 1 - mine)):
                    first = pl.multiple_of(owner * (height * chunks), height * chunks)
                    part = rows[pl.ds(first + t, height, stride=chunks), :]
                    out[pair, :, lanes] = part.astype(out.dtype)


def banded_call(kernel, outs, arrived, kernel_weights, band_observers, band_lags, mine):
    taps, terms, observers, faces = kernel_weights.shape
    bands, width = band_observers.shape
    steps = arrived.shape[-1]
    chunks = steps // 2 // LANES
    rank = len(arrived.shape)
    return pl.pallas_call(
        kernel,
        out_shape=outs,
        grid_spec=pltpu.PrefetchScalarGridSpec(
            num_scalar_prefetch=3,
            grid=(bands,),
            in_specs=[
                pl.BlockSpec(arrived.shape, lambda b, *_: (0,) * rank),
                pl.BlockSpec((taps, terms, width, faces), lambda b, *_: (0, 0, b, 0)),
            ],
            out_specs=jax.tree.map(
                lambda o: pl.BlockSpec(o.shape, lambda b, *_: (0,) * len(o.shape)), outs
            ),
            scratch_shapes=[
                pltpu.VMEM((taps * terms * faces, steps), jnp.bfloat16),
                pltpu.VMEM((width * chunks, LANES), jnp.float32),
                pltpu.VMEM((observers * chunks, LANES), jnp.float32),
            ],
        ),
        compiler_params=pltpu.CompilerParams(dimension_semantics=("arbitrary",)),
        name="bands",
    )(band_lags, band_observers.reshape(-1), mine, arrived, kernel_weights)


def halve(total, axis, bit):
    size = lax.axis_size(axis)
    mine = (lax.axis_index(axis) >> bit) & 1
    if axis == "cfd":
        owners, rows, times = total.shape
        pairs = total.reshape(owners // 2, 2, rows, times)
        first, second = pairs[:, 0], pairs[:, 1]
    else:
        first, second = jnp.split(total, 2, axis=2)
    kept = jnp.where(mine == 1, second, first)
    sent = jnp.where(mine == 1, first, second).astype(jnp.bfloat16)
    partners = [(i, i ^ (1 << bit)) for i in range(size)]
    return kept + lax.ppermute(sent, axis, partners).astype(jnp.float32)


def exchange_sums(kept, sent):
    owners = lax.axis_size("cfd")
    near = [("cfd", b) for b in range(owners.bit_length() - 1)]
    across = [("ac", b) for b in reversed(range(lax.axis_size("ac").bit_length() - 1))]
    orders = (near[:2] + across + near[2:], near[:1] + across + near[1:])
    partners = [(i, i ^ 1) for i in range(owners)]
    total = kept + lax.ppermute(sent, "cfd", partners).astype(jnp.float32)
    streams = jnp.split(total, len(orders), axis=1)
    for step in range(1, len(near) + len(across)):
        streams = [halve(part, *order[step]) for part, order in zip(streams, orders)]
    return jnp.concatenate([part[0] for part in streams], axis=0)


def flip(place, mask):
    out = place
    for bit in range(mask.bit_length()):
        if mask >> bit & 1:
            out = out + (1 << bit) * (1 - 2 * lax.rem(lax.div(place, 1 << bit), 2))
    return out


def fused_kernel(
    lags_ref,
    map_ref,
    ids_ref,
    normals_ref,
    surface_ref,
    weights_ref,
    out_ref,
    surface,
    weights,
    normals,
    outgoing,
    arrived,
    sources,
    spread,
    found,
    inverse,
    slots,
    rows,
    core_out,
    core_in,
    x_out,
    x_in,
    x_kept,
    y_out,
    y_in,
    y_kept,
    xy_out,
    xy_in,
    z_out,
    z_in,
    load_sems,
    block_send,
    block_recv,
    core_send,
    core_recv,
    first_send,
    first_recv,
    second_send,
    second_recv,
    z_send,
    z_recv,
):
    me = lax.axis_index("cfd")
    owners = outgoing.shape[0]
    zs = owners // 4
    core, x, z = lax.rem(me, 2), lax.rem(lax.div(me, 2), 2), lax.div(me, 4)
    y = lax.axis_index("ac")
    taps, terms, observers, faces = weights.shape
    bands, width = ids_ref.shape
    size, steps = surface.shape[2:]
    out_len = steps // 2
    chunks = out_len // LANES
    height = observers // owners
    near = owners // zs

    get_surface = pltpu.make_async_copy(surface_ref, surface, load_sems.at[0])
    get_weights = pltpu.make_async_copy(weights_ref, weights, load_sems.at[1])
    get_surface.start()

    def remote(src, dst, send, recv, **peer):
        return pltpu.make_async_remote_copy(
            src_ref=src, dst_ref=dst, send_sem=send, recv_sem=recv,
            device_id=peer, device_id_type=pl.DeviceIdType.MESH,
        )

    barrier = pltpu.get_barrier_semaphore()
    for k in range(1, owners):
        pl.semaphore_signal(
            barrier, inc=1, device_id={"cfd": flip(me, k)}, device_id_type=pl.DeviceIdType.MESH
        )
    pl.semaphore_signal(barrier, inc=1, device_id={"ac": 1 - y}, device_id_type=pl.DeviceIdType.MESH)

    wide = normals_ref[...].astype(jnp.float32)
    tall = jnp.concatenate([wide, jnp.zeros((LANES - wide.shape[0], faces), jnp.float32)], axis=0)
    normals[...] = tall.T.reshape(owners, size, LANES)
    get_surface.wait()
    get_weights.start()
    pl.semaphore_wait(barrier, owners)

    def thick_block(place):
        along = surface[2, place].astype(jnp.float32) * normals[place, :, 0:1]
        along = along + surface[3, place].astype(jnp.float32) * normals[place, :, 1:2]
        along = along + surface[4, place].astype(jnp.float32) * normals[place, :, 2:3]
        return (surface[1, place].astype(jnp.float32) * along).astype(jnp.bfloat16)

    block_copies = {}
    order = sorted(range(1, owners), key=lambda k: SEND_ORDER(k, near))
    for k in order:
        peer = flip(me, k)
        place = map_ref[peer]
        outgoing[k, 0] = thick_block(place)
        outgoing[k, 1] = surface[0, place]
        block_copies[k] = remote(
            outgoing.at[k], arrived.at[me], block_send.at[k], block_recv.at[k], cfd=peer
        )
        block_copies[k].start()
    place = map_ref[me]
    arrived[me, 0] = thick_block(place)
    arrived[me, 1] = surface[0, place]

    ids = ids_ref[...]
    down = jnp.concatenate([ids, jnp.zeros((LANES - bands, width), jnp.int32)], axis=0).T
    for b in range(bands):
        spread[b] = jnp.broadcast_to(down[:, b : b + 1], (width, LANES))
    lane = lax.broadcasted_iota(jnp.int32, (width, LANES), 1)
    slot = lax.broadcasted_iota(jnp.int32, (width, LANES), 0)

    @pl.loop(0, observers // LANES)
    def _(part):
        def add(b, total):
            hit = spread[b] == lane + part * LANES
            return jnp.where(hit, slot + b * width, total)

        total = lax.fori_loop(0, bands, add, jnp.zeros((width, LANES), jnp.int32))
        found[pl.ds(part, 1), :] = jnp.max(total, axis=0, keepdims=True)

    get_inverse = pltpu.make_async_copy(found, inverse, load_sems.at[2])
    get_inverse.start()

    step = lax.broadcasted_iota(jnp.int32, (near * size, steps), 1)

    def rate(series):
        moved = jnp.where(step > 0, series - pltpu.roll(series, 1, 1), 0.0)
        return moved.astype(jnp.bfloat16).astype(jnp.float32)

    for j in [0, 1] + list(range(2, zs)):
        for k in range(near * j, near * j + near):
            if k:
                block_copies[k].wait()
        first = flip(z, j) * near
        series = arrived[pl.ds(first, near)].astype(jnp.float32)
        thick = series[:, 0].reshape(near * size, steps)
        pressure = series[:, 1].reshape(near * size, steps)
        for c, value in enumerate((rate(thick), rate(pressure), pressure)):
            for k in range(taps):
                late = pltpu.roll(value, k, 1) if k else value
                top = (k * terms + c) * faces + first * size
                here = pl.ds(pl.multiple_of(top, near * size), near * size)
                for t in range(steps // LANES):
                    sources[t, here, :] = late[:, t * LANES : (t + 1) * LANES].astype(jnp.bfloat16)
    get_weights.wait()

    @pl.loop(0, bands)
    def _(b):
        start = out_len - lags_ref[b]
        tile = jnp.minimum(lax.div(start, LANES), steps // LANES - chunks - 1)
        rest = start - tile * LANES
        shift = lax.rem(LANES - rest, LANES)
        here = pl.ds(pl.multiple_of(b * width, width), width)
        chosen = jnp.concatenate(
            [weights[k, c, here, :] for k in range(taps) for c in range(terms)], axis=1
        )
        window = jnp.concatenate([sources[tile + t] for t in range(chunks + 1)], axis=1)
        whole = jnp.dot(chosen, window, preferred_element_type=jnp.float32)
        parts = [
            pltpu.roll(whole[:, t * LANES : (t + 1) * LANES], shift, 1) for t in range(chunks + 1)
        ]
        for t in range(chunks):
            slots[pl.ds(b * (width * chunks) + t, width, stride=chunks), :] = jnp.where(
                lane < LANES - rest, parts[t], parts[t + 1]
            )

    get_inverse.wait()
    unroll = 32

    def gather(owner):
        base = owner * height

        @pl.loop(0, height // unroll)
        def _(group):
            for m in range(unroll):
                at = base + group * unroll + m
                found_at = inverse[lax.div(at, LANES), lax.rem(at, LANES)]
                value = slots.reshape(observers, chunks, LANES)[found_at]
                rows[pl.ds(pl.multiple_of(at * chunks, chunks), chunks), :] = value

    def unit(owner, t):
        return rows[pl.ds(owner * (height * chunks) + t, height, stride=chunks), :]

    def narrow(value):
        return value.astype(jnp.bfloat16)

    def wide_of(value):
        return value.astype(jnp.float32)

    half = chunks // 2
    core_copies, x_copies, y_copies, xy_copies, yx_copies, z_copies = {}, {}, {}, {}, {}, {}
    turn = list(range(2, zs)) + [1, 0]

    def send_core(j):
        top = flip(z, j) * near
        for other in range(2):
            gather(top + other * 2 + 1 - core)
        for other in range(2):
            for t in range(chunks):
                core_out[j, other, t] = narrow(unit(top + other * 2 + 1 - core, t))
        core_copies[j] = remote(
            core_out.at[j], core_in.at[j], core_send.at[j], core_recv.at[j], cfd=flip(me, 1)
        )
        core_copies[j].start()
        for other in range(2):
            gather(top + other * 2 + core)

    def send_first(j):
        top = flip(z, j) * near
        core_copies[j].wait()

        def total(other, t):
            return unit(top + other * 2 + core, t) + wide_of(core_in[j, other, t])

        for side in range(2):
            x_out[j, side] = narrow(total(1 - x, side * half))
        x_copies[j] = remote(
            x_out.at[j], x_in.at[j], first_send.at[0, j], first_recv.at[0, j], cfd=flip(me, 2)
        )
        x_copies[j].start()
        for other in range(2):
            y_out[j, other] = narrow(total(other, (1 - y) * half + 1))
        y_copies[j] = remote(
            y_out.at[j], y_in.at[j], first_send.at[1, j], first_recv.at[1, j], ac=1 - y
        )
        y_copies[j].start()
        for side in range(2):
            x_kept[j, side] = total(x, side * half)
        for other in range(2):
            y_kept[j, other] = total(other, y * half + 1)

    def send_second(j):
        x_copies[j].wait()
        xy_out[0, j] = narrow(x_kept[j, 1 - y] + wide_of(x_in[j, 1 - y]))
        xy_copies[j] = remote(
            xy_out.at[0, j], xy_in.at[0, j], second_send.at[0, j], second_recv.at[0, j], ac=1 - y
        )
        xy_copies[j].start()
        y_copies[j].wait()
        xy_out[1, j] = narrow(y_kept[j, 1 - x] + wide_of(y_in[j, 1 - x]))
        yx_copies[j] = remote(
            xy_out.at[1, j], xy_in.at[1, j], second_send.at[1, j], second_recv.at[1, j],
            cfd=flip(me, 2),
        )
        yx_copies[j].start()

    def finish_second(j):
        xy_copies[j].wait()
        from_x = x_kept[j, y] + wide_of(x_in[j, y]) + wide_of(xy_in[0, j])
        yx_copies[j].wait()
        from_y = y_kept[j, x] + wide_of(y_in[j, x]) + wide_of(xy_in[1, j])
        return from_x, from_y

    def send_z(j):
        for stream, value in enumerate(finish_second(j)):
            z_out[j, stream] = narrow(value)
        z_copies[j] = remote(
            z_out.at[j], z_in.at[j], z_send.at[j], z_recv.at[j], cfd=flip(me, near * j)
        )
        z_copies[j].start()

    for place, j in enumerate(turn):
        send_core(j)
        if place:
            send_first(turn[place - 1])
    send_first(turn[-1])
    for j in turn:
        send_second(j)
    for j in turn[:-1]:
        send_z(j)
    results = list(finish_second(0))
    for j in turn[:-1]:
        z_copies[j].wait()
        results = [value + wide_of(z_in[j, s]) for s, value in enumerate(results)]
    for s, value in enumerate(results):
        out_ref[:, s * LANES : (s + 1) * LANES] = value


def SEND_ORDER(k, near):
    j = k // near
    return (0, 3, 1, 2)[j] if j < 4 else j, k


def fused(surface_raw, area_normals, kernel_weights, block_map, band_observers, band_lags):
    owners, halves = lax.axis_size("cfd"), lax.axis_size("ac")
    faces, steps = surface_raw.shape[1:]
    taps, terms, observers, _ = kernel_weights.shape
    bands, width = band_observers.shape
    size, height = faces // owners, observers // owners
    chunks = steps // 2 // LANES
    zs = owners // 4
    near = owners // zs
    bf16, f32, i32 = jnp.bfloat16, jnp.float32, jnp.int32
    tile = (height, LANES)
    dma = pltpu.SemaphoreType.DMA
    vmem, smem, hbm = (
        pl.BlockSpec(memory_space=space) for space in (pltpu.VMEM, pltpu.SMEM, pl.ANY)
    )
    return pl.pallas_call(
        fused_kernel,
        out_shape=jax.ShapeDtypeStruct((height, chunks // halves * LANES), f32),
        in_specs=[smem, smem, vmem, vmem, hbm, hbm],
        out_specs=vmem,
        scratch_shapes=[
            pltpu.VMEM((surface_raw.shape[0], owners, size, steps), bf16),
            pltpu.VMEM(kernel_weights.shape, bf16),
            pltpu.VMEM((owners, size, LANES), f32),
            pltpu.VMEM((owners, 2, size, steps), bf16),
            pltpu.VMEM((owners, 2, size, steps), bf16),
            pltpu.VMEM((steps // LANES, taps * terms * faces, LANES), bf16),
            pltpu.VMEM((bands, width, LANES), i32),
            pltpu.VMEM((observers // LANES, LANES), i32),
            pltpu.SMEM((observers // LANES, LANES), i32),
            pltpu.VMEM((observers * chunks, LANES), f32),
            pltpu.VMEM((observers * chunks, LANES), f32),
            pltpu.VMEM((zs, 2, chunks) + tile, bf16),
            pltpu.VMEM((zs, 2, chunks) + tile, bf16),
            pltpu.VMEM((zs, 2) + tile, bf16),
            pltpu.VMEM((zs, 2) + tile, bf16),
            pltpu.VMEM((zs, 2) + tile, f32),
            pltpu.VMEM((zs, 2) + tile, bf16),
            pltpu.VMEM((zs, 2) + tile, bf16),
            pltpu.VMEM((zs, 2) + tile, f32),
            pltpu.VMEM((2, zs) + tile, bf16),
            pltpu.VMEM((2, zs) + tile, bf16),
            pltpu.VMEM((zs, 2) + tile, bf16),
            pltpu.VMEM((zs, 2) + tile, bf16),
            dma((3,)),
            dma((owners,)),
            dma((owners,)),
            dma((zs,)),
            dma((zs,)),
            dma((2, zs)),
            dma((2, zs)),
            dma((2, zs)),
            dma((2, zs)),
            dma((zs,)),
            dma((zs,)),
        ],
        compiler_params=pltpu.CompilerParams(
            collective_id=0, has_side_effects=True, vmem_limit_bytes=60 * 2**20
        ),
        name="fused",
    )(
        band_lags,
        block_map[0, 0],
        band_observers,
        area_normals,
        surface_raw.reshape(surface_raw.shape[0], owners, size, steps),
        kernel_weights,
    )


def fits_fused(owners, halves, surface_raw, kernel_weights, band_observers):
    faces, steps = surface_raw.shape[1:]
    tiles = halves * 2
    return (
        halves == 2
        and owners % 4 == 0
        and owners & (owners - 1) == 0
        and faces == LANES
        and band_observers.shape[1] == LANES
        and faces // owners % 8 == 0
        and steps == 2 * tiles * LANES
        and kernel_weights.shape[2] % (owners * 32) == 0
    )


def general(surface_raw, area_normals, kernel_weights, block_map, band_observers, band_lags):
    blocks = lax.axis_size("cfd")
    faces, steps = surface_raw.shape[1:]
    size = faces // blocks
    outgoing = prepare(surface_raw, area_normals, block_map[0, 0])
    arrived = lax.all_to_all(outgoing, "cfd", split_axis=0, concat_axis=0, tiled=True)
    arrived = arrived.reshape(blocks, 2, size, steps)
    if size % 8:
        arrived = arrived.transpose(1, 0, 2, 3).reshape(2 * faces, steps)
    shape = (blocks // 2, kernel_weights.shape[2] // blocks, steps // 2)
    kept, sent = banded_call(
        halves_kernel,
        [jax.ShapeDtypeStruct(shape, kind) for kind in (jnp.float32, jnp.bfloat16)],
        arrived,
        kernel_weights,
        band_observers,
        band_lags,
        (lax.axis_index("cfd") & 1).astype(jnp.int32).reshape(1),
    )
    return exchange_sums(kept, sent)


def local(surface_raw, area_normals, kernel_weights, block_map, band_observers, band_lags):
    owners, halves = lax.axis_size("cfd"), lax.axis_size("ac")
    fast = fits_fused(owners, halves, surface_raw, kernel_weights, band_observers)
    run = fused if fast else general
    return run(surface_raw, area_normals, kernel_weights, block_map, band_observers, band_lags)


def solution(mesh):
    placed = (
        P(None, ("cfd", "ac"), None),
        P(None, ("cfd", "ac")),
        P(None, None, None, ("cfd", "ac")),
        P("ac", "cfd", None),
        P(),
        P(),
    )
    return jax.shard_map(
        local, mesh=mesh, in_specs=placed, out_specs=P("cfd", "ac"), check_vma=False
    )
```

```python
import functools

import jax
import jax.numpy as jnp
from jax import lax
from jax.experimental import pallas as pl
from jax.experimental.pallas import tpu as pltpu
from jax.sharding import PartitionSpec as P

LANES = 128


def prepare_kernel(src_ref, normals_ref, surface_ref, out_ref):
    along = surface_ref[2].astype(jnp.float32) * normals_ref[:, 0:1]
    along = along + surface_ref[3].astype(jnp.float32) * normals_ref[:, 1:2]
    along = along + surface_ref[4].astype(jnp.float32) * normals_ref[:, 2:3]
    thick = (surface_ref[1].astype(jnp.float32) * along).astype(jnp.bfloat16)
    both = jnp.concatenate([thick, surface_ref[0]], axis=0)
    rows = both.shape[0]
    column = lax.broadcasted_iota(jnp.int32, (rows, rows), 1)
    onehot = jnp.where(column == src_ref[...], 1.0, 0.0).astype(jnp.bfloat16)
    picked = jnp.dot(onehot, both, preferred_element_type=jnp.float32)
    out_ref[...] = picked.astype(jnp.bfloat16)


def prepare(surface_raw, area_normals, block_order):
    faces, steps = surface_raw.shape[1:]
    blocks = block_order.shape[0]
    size = faces // blocks
    src = (
        jnp.arange(2, dtype=jnp.int32)[None, :, None] * faces
        + block_order[:, None, None] * size
        + jnp.arange(size, dtype=jnp.int32)[None, None, :]
    ).reshape(2 * faces, 1)
    return pl.pallas_call(
        prepare_kernel,
        out_shape=jax.ShapeDtypeStruct((2 * faces, steps), jnp.bfloat16),
        name="prepare",
    )(src, area_normals.T.astype(jnp.float32), surface_raw)


def scatter_bands(lags_ref, ids_ref, arrived_ref, weights_ref, sources, band, rows):
    index = pl.program_id(0)
    taps, terms, width, faces = weights_ref.shape
    steps = sources.shape[1]
    out_len = steps // 2
    chunks = out_len // LANES

    @pl.when(index == 0)
    def _():
        series = arrived_ref[...].astype(jnp.float32)
        if len(arrived_ref.shape) == 4:
            thick = series[:, 0].reshape(faces, steps)
            pressure = series[:, 1].reshape(faces, steps)
        else:
            thick, pressure = series[:faces], series[faces:]
        step = lax.broadcasted_iota(jnp.int32, (faces, steps), 1)

        def rate(x):
            moved = jnp.where(step > 0, x - pltpu.roll(x, 1, 1), 0.0)
            return moved.astype(jnp.bfloat16).astype(jnp.float32)

        for c, x in enumerate((rate(thick), rate(pressure), pressure)):
            for k in range(taps):
                late = pltpu.roll(x, k, 1) if k else x
                sources[pl.ds((k * terms + c) * faces, faces), :] = late.astype(jnp.bfloat16)

    start = out_len - lags_ref[index]
    tile = jnp.minimum(start // LANES, steps // LANES - chunks - 1)
    rest = start - tile * LANES
    shift = lax.rem(LANES - rest, LANES)
    chosen = jnp.concatenate(
        [weights_ref[k, c] for k in range(taps) for c in range(terms)], axis=1
    )
    window = sources[:, pl.ds(pl.multiple_of(tile * LANES, LANES), out_len + LANES)]
    wide = jnp.dot(chosen, window, preferred_element_type=jnp.float32)
    lane = lax.broadcasted_iota(jnp.int32, (width, LANES), 1)
    parts = [
        pltpu.roll(wide[:, t * LANES : (t + 1) * LANES], shift, 1) for t in range(chunks + 1)
    ]
    for t in range(chunks):
        band[pl.ds(t, width, stride=chunks), :] = jnp.where(
            lane < LANES - rest, parts[t], parts[t + 1]
        )

    unroll = 32

    @pl.loop(0, width // unroll)
    def _(group):
        slots = [group * unroll + m for m in range(unroll)]
        places = [ids_ref[index * width + slot] for slot in slots]
        values = [
            band[pl.ds(pl.multiple_of(slot * chunks, chunks), chunks), :] for slot in slots
        ]
        for place, value in zip(places, values):
            rows[pl.ds(pl.multiple_of(place * chunks, chunks), chunks), :] = value


def halves_kernel(
    lags_ref, ids_ref, mine_ref, arrived_ref, weights_ref, kept_ref, sent_ref, sources, band, rows
):
    scatter_bands(lags_ref, ids_ref, arrived_ref, weights_ref, sources, band, rows)
    pairs, height, out_len = kept_ref.shape
    chunks = out_len // LANES
    mine = mine_ref[0]

    @pl.when(pl.program_id(0) == pl.num_programs(0) - 1)
    def _():
        for pair in range(pairs):
            for t in range(chunks):
                lanes = slice(t * LANES, (t + 1) * LANES)
                for out, owner in ((kept_ref, 2 * pair + mine), (sent_ref, 2 * pair + 1 - mine)):
                    first = pl.multiple_of(owner * (height * chunks), height * chunks)
                    part = rows[pl.ds(first + t, height, stride=chunks), :]
                    out[pair, :, lanes] = part.astype(out.dtype)


def banded_call(kernel, outs, arrived, kernel_weights, band_observers, band_lags, mine):
    taps, terms, observers, faces = kernel_weights.shape
    bands, width = band_observers.shape
    steps = arrived.shape[-1]
    chunks = steps // 2 // LANES
    rank = len(arrived.shape)
    return pl.pallas_call(
        kernel,
        out_shape=outs,
        grid_spec=pltpu.PrefetchScalarGridSpec(
            num_scalar_prefetch=3,
            grid=(bands,),
            in_specs=[
                pl.BlockSpec(arrived.shape, lambda b, *_: (0,) * rank),
                pl.BlockSpec((taps, terms, width, faces), lambda b, *_: (0, 0, b, 0)),
            ],
            out_specs=jax.tree.map(
                lambda o: pl.BlockSpec(o.shape, lambda b, *_: (0,) * len(o.shape)), outs
            ),
            scratch_shapes=[
                pltpu.VMEM((taps * terms * faces, steps), jnp.bfloat16),
                pltpu.VMEM((width * chunks, LANES), jnp.float32),
                pltpu.VMEM((observers * chunks, LANES), jnp.float32),
            ],
        ),
        compiler_params=pltpu.CompilerParams(dimension_semantics=("arbitrary",)),
        name="bands",
    )(band_lags, band_observers.reshape(-1), mine, arrived, kernel_weights)


def halve(total, axis, bit):
    size = lax.axis_size(axis)
    mine = (lax.axis_index(axis) >> bit) & 1
    if axis == "cfd":
        owners, rows, times = total.shape
        pairs = total.reshape(owners // 2, 2, rows, times)
        first, second = pairs[:, 0], pairs[:, 1]
    else:
        first, second = jnp.split(total, 2, axis=2)
    kept = jnp.where(mine == 1, second, first)
    sent = jnp.where(mine == 1, first, second).astype(jnp.bfloat16)
    partners = [(i, i ^ (1 << bit)) for i in range(size)]
    return kept + lax.ppermute(sent, axis, partners).astype(jnp.float32)


def exchange_sums(kept, sent):
    owners = lax.axis_size("cfd")
    near = [("cfd", b) for b in range(owners.bit_length() - 1)]
    across = [("ac", b) for b in reversed(range(lax.axis_size("ac").bit_length() - 1))]
    orders = (near[:2] + across + near[2:], near[:1] + across + near[1:])
    partners = [(i, i ^ 1) for i in range(owners)]
    total = kept + lax.ppermute(sent, "cfd", partners).astype(jnp.float32)
    streams = jnp.split(total, len(orders), axis=1)
    for step in range(1, len(near) + len(across)):
        streams = [halve(part, *order[step]) for part, order in zip(streams, orders)]
    return jnp.concatenate([part[0] for part in streams], axis=0)


def flip(place, mask):
    out = place
    for bit in range(mask.bit_length()):
        if mask >> bit & 1:
            out = out + (1 << bit) * (1 - 2 * lax.rem(lax.div(place, 1 << bit), 2))
    return out


def fused_kernel(
    lags_ref,
    map_ref,
    ids_ref,
    normals_ref,
    surface_ref,
    weights_ref,
    first_ref,
    second_ref,
    surface,
    weights,
    normals,
    outgoing,
    arrived,
    sources,
    before,
    wide,
    spread,
    found,
    inverse,
    slots,
    rows,
    core_out,
    core_in,
    x_out,
    x_in,
    x_kept,
    y_out,
    y_in,
    y_kept,
    xy_out,
    xy_in,
    z_out,
    z_in,
    load_sems,
    block_send,
    block_recv,
    core_send,
    core_recv,
    first_send,
    first_recv,
    second_send,
    second_recv,
    z_send,
    z_recv,
):
    me = lax.axis_index("cfd")
    owners, pieces = outgoing.shape[:2]
    span = outgoing.shape[-1]
    zs = owners // 4
    core, x, z = lax.rem(me, 2), lax.rem(lax.div(me, 2), 2), lax.div(me, 4)
    y = lax.axis_index("ac")
    taps, terms, observers, faces = weights.shape
    bands, width = ids_ref.shape
    size, steps = surface.shape[2:]
    out_len = steps // 2
    chunks = out_len // LANES
    height = observers // owners
    near = owners // zs

    get_surface = pltpu.make_async_copy(surface_ref, surface, load_sems.at[0])
    get_weights = pltpu.make_async_copy(weights_ref, weights, load_sems.at[1])
    get_surface.start()

    def remote(src, dst, send, recv, **peer):
        return pltpu.make_async_remote_copy(
            src_ref=src, dst_ref=dst, send_sem=send, recv_sem=recv,
            device_id=peer, device_id_type=pl.DeviceIdType.MESH,
        )

    barrier = pltpu.get_barrier_semaphore()
    for k in range(1, owners):
        pl.semaphore_signal(
            barrier, inc=1, device_id={"cfd": flip(me, k)}, device_id_type=pl.DeviceIdType.MESH
        )
    pl.semaphore_signal(barrier, inc=1, device_id={"ac": 1 - y}, device_id_type=pl.DeviceIdType.MESH)

    flat = normals_ref[...].astype(jnp.float32)
    tall = jnp.concatenate([flat, jnp.zeros((LANES - flat.shape[0], faces), jnp.float32)], axis=0)
    normals[...] = tall.T.reshape(owners, size, LANES)
    get_surface.wait()
    get_weights.start()

    def thick_block(place):
        along = surface[2, place].astype(jnp.float32) * normals[place, :, 0:1]
        along = along + surface[3, place].astype(jnp.float32) * normals[place, :, 1:2]
        along = along + surface[4, place].astype(jnp.float32) * normals[place, :, 2:3]
        return (surface[1, place].astype(jnp.float32) * along).astype(jnp.bfloat16)

    def cut(value, c):
        return value[:, c * span : (c + 1) * span]

    order = sorted(range(1, owners), key=lambda k: send_order(k, near))
    for k in order:
        place = map_ref[flip(me, k)]
        thick, pressure = thick_block(place), surface[0, place]
        for c in range(pieces):
            outgoing[k, c, 0], outgoing[k, c, 1] = cut(thick, c), cut(pressure, c)
    place = map_ref[me]
    thick, pressure = thick_block(place), surface[0, place]
    for c in range(pieces):
        arrived[c, me, 0], arrived[c, me, 1] = cut(thick, c), cut(pressure, c)
    pl.semaphore_wait(barrier, owners)
    block_copies = {}
    for c in range(pieces):
        for k in order:
            block_copies[c, k] = remote(
                outgoing.at[k, c],
                arrived.at[c, me],
                block_send.at[k, c],
                block_recv.at[k, c],
                cfd=flip(me, k),
            )
            block_copies[c, k].start()

    ids = ids_ref[...]
    down = jnp.concatenate([ids, jnp.zeros((LANES - bands, width), jnp.int32)], axis=0).T
    for b in range(bands):
        spread[b] = jnp.broadcast_to(down[:, b : b + 1], (width, LANES))
    lane = lax.broadcasted_iota(jnp.int32, (width, LANES), 1)
    slot = lax.broadcasted_iota(jnp.int32, (width, LANES), 0)

    @pl.loop(0, observers // LANES)
    def _(part):
        def add(b, total):
            hit = spread[b] == lane + part * LANES
            return jnp.where(hit, slot + b * width, total)

        total = lax.fori_loop(0, bands, add, jnp.zeros((width, LANES), jnp.int32))
        found[pl.ds(part, 1), :] = jnp.max(total, axis=0, keepdims=True)

    get_inverse = pltpu.make_async_copy(found, inverse, load_sems.at[2])
    get_inverse.start()

    start_lane = lax.broadcasted_iota(jnp.int32, (faces, LANES), 1) == 0
    rows_each = 4 * width

    def source_tile(c, u):
        tile = c * (span // LANES) + u
        lanes = slice(u * LANES, (u + 1) * LANES)

        def late(value, place):
            turned = pltpu.roll(value, 1, 1)
            moved = jnp.where(start_lane, before[place], turned) if tile else turned
            before[place] = turned
            return moved

        for n in range(2):
            value = arrived[c, :, n, :, lanes].astype(jnp.float32).reshape(faces, LANES)
            last = late(value, 2 * n)
            rate = value - last
            if tile == 0:
                rate = jnp.where(start_lane, 0.0, rate)
            rate = rate.astype(jnp.bfloat16).astype(jnp.float32)
            taken = [(n, rate, late(rate, 2 * n + 1))]
            if n == 1:
                taken.append((2, value, last))
            for term, now, then in taken:
                for k, series in enumerate((now, then)):
                    here = pl.ds((k * terms + term) * faces, faces)
                    sources[here, lanes] = series.astype(jnp.bfloat16)

    for c in range(pieces):
        for k in order:
            block_copies[c, k].wait()
        for u in range(span // LANES):
            source_tile(c, u)
        if c == 0:
            get_weights.wait()

        @pl.loop(0, observers // rows_each)
        def _(part):
            here = pl.ds(pl.multiple_of(part * rows_each, rows_each), rows_each)
            chosen = jnp.concatenate(
                [weights[k, t, here, :] for k in range(taps) for t in range(terms)], axis=1
            )
            product = jnp.dot(chosen, sources[...], preferred_element_type=jnp.float32)
            for u in range(span // LANES):
                wide[c * (span // LANES) + u, pl.ds(part * 4, 4)] = product[
                    :, u * LANES : (u + 1) * LANES
                ].reshape(4, width, LANES)

    @pl.loop(0, bands)
    def _(b):
        start = out_len - lags_ref[b]
        tile = jnp.minimum(lax.div(start, LANES), steps // LANES - chunks - 1)
        rest = start - tile * LANES
        shift = lax.rem(LANES - rest, LANES)
        parts = [pltpu.roll(wide[tile + t, b], shift, 1) for t in range(chunks + 1)]
        for t in range(chunks):
            slots[pl.ds(b * (width * chunks) + t, width, stride=chunks), :] = jnp.where(
                lane < LANES - rest, parts[t], parts[t + 1]
            )

    get_inverse.wait()
    unroll = 32

    def gather(owner):
        @pl.loop(0, height // unroll)
        def _(group):
            first = group * unroll
            places = [inverse[owner, first + m] for m in range(unroll)]
            values = [slots.reshape(observers, chunks, LANES)[place] for place in places]
            top = pl.multiple_of((owner * height + first) * chunks, unroll * chunks)
            for m, value in enumerate(values):
                rows[pl.ds(top + m * chunks, chunks), :] = value

    def unit(owner, t):
        return rows[pl.ds(owner * (height * chunks) + t, height, stride=chunks), :]

    def narrow(value):
        return value.astype(jnp.bfloat16)

    def wide_of(value):
        return value.astype(jnp.float32)

    half = chunks // 2
    core_copies, x_copies, y_copies, xy_copies, yx_copies, z_copies = {}, {}, {}, {}, {}, {}
    turn = list(range(2, zs)) + [1, 0]

    def send_core(j):
        top = flip(z, j) * near
        for other in range(2):
            gather(top + other * 2 + 1 - core)
        for other in range(2):
            for t in range(chunks):
                core_out[j, other, t] = narrow(unit(top + other * 2 + 1 - core, t))
        core_copies[j] = remote(
            core_out.at[j], core_in.at[j], core_send.at[j], core_recv.at[j], cfd=flip(me, 1)
        )
        core_copies[j].start()
        for other in range(2):
            gather(top + other * 2 + core)

    def send_first(j):
        top = flip(z, j) * near
        core_copies[j].wait()

        def total(other, t):
            return unit(top + other * 2 + core, t) + wide_of(core_in[j, other, t])

        for side in range(2):
            x_out[j, side] = narrow(total(1 - x, side * half))
        x_copies[j] = remote(
            x_out.at[j], x_in.at[j], first_send.at[0, j], first_recv.at[0, j], cfd=flip(me, 2)
        )
        x_copies[j].start()
        for other in range(2):
            y_out[j, other] = narrow(total(other, (1 - y) * half + 1))
        y_copies[j] = remote(
            y_out.at[j], y_in.at[j], first_send.at[1, j], first_recv.at[1, j], ac=1 - y
        )
        y_copies[j].start()
        for side in range(2):
            x_kept[j, side] = total(x, side * half)
        for other in range(2):
            y_kept[j, other] = total(other, y * half + 1)

    def send_second(j):
        x_copies[j].wait()
        xy_out[0, j] = narrow(x_kept[j, 1 - y] + wide_of(x_in[j, 1 - y]))
        xy_copies[j] = remote(
            xy_out.at[0, j], xy_in.at[0, j], second_send.at[0, j], second_recv.at[0, j], ac=1 - y
        )
        xy_copies[j].start()
        y_copies[j].wait()
        xy_out[1, j] = narrow(y_kept[j, 1 - x] + wide_of(y_in[j, 1 - x]))
        yx_copies[j] = remote(
            xy_out.at[1, j], xy_in.at[1, j], second_send.at[1, j], second_recv.at[1, j],
            cfd=flip(me, 2),
        )
        yx_copies[j].start()

    def finish_second(j):
        xy_copies[j].wait()
        from_x = x_kept[j, y] + wide_of(x_in[j, y]) + wide_of(xy_in[0, j])
        yx_copies[j].wait()
        from_y = y_kept[j, x] + wide_of(y_in[j, x]) + wide_of(xy_in[1, j])
        return from_x, from_y

    def send_z(j):
        for stream, value in enumerate(finish_second(j)):
            z_out[j, stream] = narrow(value)
        z_copies[j] = remote(
            z_out.at[j], z_in.at[j], z_send.at[j], z_recv.at[j], cfd=flip(me, near * j)
        )
        z_copies[j].start()

    for step in range(zs + 4):
        if step < zs:
            send_core(turn[step])
        if 1 <= step < zs:
            send_first(turn[step - 1])
        if 3 <= step < zs + 3:
            send_second(turn[step - 3])
        if step == zs:
            send_first(turn[-1])
        if 4 <= step < zs + 3:
            send_z(turn[step - 4])
    results = list(finish_second(0))
    for j in turn[:-1]:
        z_copies[j].wait()
        results = [value + wide_of(z_in[j, s]) for s, value in enumerate(results)]
    for value, result_ref in zip(results, (first_ref, second_ref)):
        result_ref[...] = value


def send_order(k, near):
    j = k // near
    return (0, 3, 1, 2)[j] if j < 4 else j, k


def fused(surface_raw, area_normals, kernel_weights, block_map, band_observers, band_lags):
    owners, halves = lax.axis_size("cfd"), lax.axis_size("ac")
    faces, steps = surface_raw.shape[1:]
    taps, terms, observers, _ = kernel_weights.shape
    bands, width = band_observers.shape
    size, height = faces // owners, observers // owners
    chunks = steps // 2 // LANES
    zs = owners // 4
    near = owners // zs
    bf16, f32, i32 = jnp.bfloat16, jnp.float32, jnp.int32
    tile = (height, LANES)
    dma = pltpu.SemaphoreType.DMA
    vmem, smem, hbm = (
        pl.BlockSpec(memory_space=space) for space in (pltpu.VMEM, pltpu.SMEM, pl.ANY)
    )
    pieces = 4
    span = steps // pieces
    first, second = pl.pallas_call(
        fused_kernel,
        out_shape=[jax.ShapeDtypeStruct(tile, f32)] * 2,
        in_specs=[smem, smem, vmem, vmem, hbm, hbm],
        out_specs=[vmem, vmem],
        scratch_shapes=[
            pltpu.VMEM((surface_raw.shape[0], owners, size, steps), bf16),
            pltpu.VMEM(kernel_weights.shape, bf16),
            pltpu.VMEM((owners, size, LANES), f32),
            pltpu.VMEM((owners, pieces, 2, size, span), bf16),
            pltpu.VMEM((pieces, owners, 2, size, span), bf16),
            pltpu.VMEM((taps * terms * faces, span), bf16),
            pltpu.VMEM((4,) + tile, f32),
            pltpu.VMEM((steps // LANES, bands, width, LANES), f32),
            pltpu.VMEM((bands, width, LANES), i32),
            pltpu.VMEM((observers // LANES, LANES), i32),
            pltpu.SMEM((observers // LANES, LANES), i32),
            pltpu.VMEM((observers * chunks, LANES), f32),
            pltpu.VMEM((observers * chunks, LANES), f32),
            pltpu.VMEM((zs, 2, chunks) + tile, bf16),
            pltpu.VMEM((zs, 2, chunks) + tile, bf16),
            pltpu.VMEM((zs, 2) + tile, bf16),
            pltpu.VMEM((zs, 2) + tile, bf16),
            pltpu.VMEM((zs, 2) + tile, f32),
            pltpu.VMEM((zs, 2) + tile, bf16),
            pltpu.VMEM((zs, 2) + tile, bf16),
            pltpu.VMEM((zs, 2) + tile, f32),
            pltpu.VMEM((2, zs) + tile, bf16),
            pltpu.VMEM((2, zs) + tile, bf16),
            pltpu.VMEM((zs, 2) + tile, bf16),
            pltpu.VMEM((zs, 2) + tile, bf16),
            dma((3,)),
            dma((owners, pieces)),
            dma((owners, pieces)),
            dma((zs,)),
            dma((zs,)),
            dma((2, zs)),
            dma((2, zs)),
            dma((2, zs)),
            dma((2, zs)),
            dma((zs,)),
            dma((zs,)),
        ],
        compiler_params=pltpu.CompilerParams(
            collective_id=0, has_side_effects=True, vmem_limit_bytes=60 * 2**20
        ),
        name="fused",
    )(
        band_lags,
        block_map[0, 0],
        band_observers,
        area_normals,
        surface_raw.reshape(surface_raw.shape[0], owners, size, steps),
        kernel_weights,
    )
    return jnp.concatenate([first, second], axis=1)


def fits_fused(owners, halves, surface_raw, kernel_weights, band_observers):
    faces, steps = surface_raw.shape[1:]
    tiles = halves * 2
    return (
        halves == 2
        and owners % 4 == 0
        and owners & (owners - 1) == 0
        and faces == LANES
        and band_observers.shape[1] == LANES
        and faces // owners % 8 == 0
        and steps == 2 * tiles * LANES
        and kernel_weights.shape[:1] + kernel_weights.shape[2:3] == (2, owners * LANES)
        and band_observers.shape[0] % 4 == 0
    )


def general(surface_raw, area_normals, kernel_weights, block_map, band_observers, band_lags):
    blocks = lax.axis_size("cfd")
    faces, steps = surface_raw.shape[1:]
    size = faces // blocks
    outgoing = prepare(surface_raw, area_normals, block_map[0, 0])
    arrived = lax.all_to_all(outgoing, "cfd", split_axis=0, concat_axis=0, tiled=True)
    arrived = arrived.reshape(blocks, 2, size, steps)
    if size % 8:
        arrived = arrived.transpose(1, 0, 2, 3).reshape(2 * faces, steps)
    shape = (blocks // 2, kernel_weights.shape[2] // blocks, steps // 2)
    kept, sent = banded_call(
        halves_kernel,
        [jax.ShapeDtypeStruct(shape, kind) for kind in (jnp.float32, jnp.bfloat16)],
        arrived,
        kernel_weights,
        band_observers,
        band_lags,
        (lax.axis_index("cfd") & 1).astype(jnp.int32).reshape(1),
    )
    return exchange_sums(kept, sent)


def local(surface_raw, area_normals, kernel_weights, block_map, band_observers, band_lags):
    owners, halves = lax.axis_size("cfd"), lax.axis_size("ac")
    fast = fits_fused(owners, halves, surface_raw, kernel_weights, band_observers)
    run = fused if fast else general
    return run(surface_raw, area_normals, kernel_weights, block_map, band_observers, band_lags)


def solution(mesh):
    placed = (
        P(None, ("cfd", "ac"), None),
        P(None, ("cfd", "ac")),
        P(None, None, None, ("cfd", "ac")),
        P("ac", "cfd", None),
        P(),
        P(),
    )
    return jax.shard_map(
        local, mesh=mesh, in_specs=placed, out_specs=P("cfd", "ac"), check_vma=False
    )
```

```python
import functools

import jax
import jax.numpy as jnp
from jax import lax
from jax.experimental import pallas as pl
from jax.experimental.pallas import tpu as pltpu
from jax.sharding import PartitionSpec as P

LANES = 128


def prepare_kernel(src_ref, normals_ref, surface_ref, out_ref):
    along = surface_ref[2].astype(jnp.float32) * normals_ref[:, 0:1]
    along = along + surface_ref[3].astype(jnp.float32) * normals_ref[:, 1:2]
    along = along + surface_ref[4].astype(jnp.float32) * normals_ref[:, 2:3]
    thick = (surface_ref[1].astype(jnp.float32) * along).astype(jnp.bfloat16)
    both = jnp.concatenate([thick, surface_ref[0]], axis=0)
    rows = both.shape[0]
    column = lax.broadcasted_iota(jnp.int32, (rows, rows), 1)
    onehot = jnp.where(column == src_ref[...], 1.0, 0.0).astype(jnp.bfloat16)
    picked = jnp.dot(onehot, both, preferred_element_type=jnp.float32)
    out_ref[...] = picked.astype(jnp.bfloat16)


def prepare(surface_raw, area_normals, block_order):
    faces, steps = surface_raw.shape[1:]
    blocks = block_order.shape[0]
    size = faces // blocks
    src = (
        jnp.arange(2, dtype=jnp.int32)[None, :, None] * faces
        + block_order[:, None, None] * size
        + jnp.arange(size, dtype=jnp.int32)[None, None, :]
    ).reshape(2 * faces, 1)
    return pl.pallas_call(
        prepare_kernel,
        out_shape=jax.ShapeDtypeStruct((2 * faces, steps), jnp.bfloat16),
        name="prepare",
    )(src, area_normals.T.astype(jnp.float32), surface_raw)


def scatter_bands(lags_ref, ids_ref, arrived_ref, weights_ref, sources, band, rows):
    index = pl.program_id(0)
    taps, terms, width, faces = weights_ref.shape
    steps = sources.shape[1]
    out_len = steps // 2
    chunks = out_len // LANES

    @pl.when(index == 0)
    def _():
        series = arrived_ref[...].astype(jnp.float32)
        if len(arrived_ref.shape) == 4:
            thick = series[:, 0].reshape(faces, steps)
            pressure = series[:, 1].reshape(faces, steps)
        else:
            thick, pressure = series[:faces], series[faces:]
        step = lax.broadcasted_iota(jnp.int32, (faces, steps), 1)

        def rate(x):
            moved = jnp.where(step > 0, x - pltpu.roll(x, 1, 1), 0.0)
            return moved.astype(jnp.bfloat16).astype(jnp.float32)

        for c, x in enumerate((rate(thick), rate(pressure), pressure)):
            for k in range(taps):
                late = pltpu.roll(x, k, 1) if k else x
                sources[pl.ds((k * terms + c) * faces, faces), :] = late.astype(jnp.bfloat16)

    start = out_len - lags_ref[index]
    tile = jnp.minimum(start // LANES, steps // LANES - chunks - 1)
    rest = start - tile * LANES
    shift = lax.rem(LANES - rest, LANES)
    chosen = jnp.concatenate(
        [weights_ref[k, c] for k in range(taps) for c in range(terms)], axis=1
    )
    window = sources[:, pl.ds(pl.multiple_of(tile * LANES, LANES), out_len + LANES)]
    wide = jnp.dot(chosen, window, preferred_element_type=jnp.float32)
    lane = lax.broadcasted_iota(jnp.int32, (width, LANES), 1)
    parts = [
        pltpu.roll(wide[:, t * LANES : (t + 1) * LANES], shift, 1) for t in range(chunks + 1)
    ]
    for t in range(chunks):
        band[pl.ds(t, width, stride=chunks), :] = jnp.where(
            lane < LANES - rest, parts[t], parts[t + 1]
        )

    unroll = 32

    @pl.loop(0, width // unroll)
    def _(group):
        slots = [group * unroll + m for m in range(unroll)]
        places = [ids_ref[index * width + slot] for slot in slots]
        values = [
            band[pl.ds(pl.multiple_of(slot * chunks, chunks), chunks), :] for slot in slots
        ]
        for place, value in zip(places, values):
            rows[pl.ds(pl.multiple_of(place * chunks, chunks), chunks), :] = value


def halves_kernel(
    lags_ref, ids_ref, mine_ref, arrived_ref, weights_ref, kept_ref, sent_ref, sources, band, rows
):
    scatter_bands(lags_ref, ids_ref, arrived_ref, weights_ref, sources, band, rows)
    pairs, height, out_len = kept_ref.shape
    chunks = out_len // LANES
    mine = mine_ref[0]

    @pl.when(pl.program_id(0) == pl.num_programs(0) - 1)
    def _():
        for pair in range(pairs):
            for t in range(chunks):
                lanes = slice(t * LANES, (t + 1) * LANES)
                for out, owner in ((kept_ref, 2 * pair + mine), (sent_ref, 2 * pair + 1 - mine)):
                    first = pl.multiple_of(owner * (height * chunks), height * chunks)
                    part = rows[pl.ds(first + t, height, stride=chunks), :]
                    out[pair, :, lanes] = part.astype(out.dtype)


def banded_call(kernel, outs, arrived, kernel_weights, band_observers, band_lags, mine):
    taps, terms, observers, faces = kernel_weights.shape
    bands, width = band_observers.shape
    steps = arrived.shape[-1]
    chunks = steps // 2 // LANES
    rank = len(arrived.shape)
    return pl.pallas_call(
        kernel,
        out_shape=outs,
        grid_spec=pltpu.PrefetchScalarGridSpec(
            num_scalar_prefetch=3,
            grid=(bands,),
            in_specs=[
                pl.BlockSpec(arrived.shape, lambda b, *_: (0,) * rank),
                pl.BlockSpec((taps, terms, width, faces), lambda b, *_: (0, 0, b, 0)),
            ],
            out_specs=jax.tree.map(
                lambda o: pl.BlockSpec(o.shape, lambda b, *_: (0,) * len(o.shape)), outs
            ),
            scratch_shapes=[
                pltpu.VMEM((taps * terms * faces, steps), jnp.bfloat16),
                pltpu.VMEM((width * chunks, LANES), jnp.float32),
                pltpu.VMEM((observers * chunks, LANES), jnp.float32),
            ],
        ),
        compiler_params=pltpu.CompilerParams(dimension_semantics=("arbitrary",)),
        name="bands",
    )(band_lags, band_observers.reshape(-1), mine, arrived, kernel_weights)


def halve(total, axis, bit):
    size = lax.axis_size(axis)
    mine = (lax.axis_index(axis) >> bit) & 1
    if axis == "cfd":
        owners, rows, times = total.shape
        pairs = total.reshape(owners // 2, 2, rows, times)
        first, second = pairs[:, 0], pairs[:, 1]
    else:
        first, second = jnp.split(total, 2, axis=2)
    kept = jnp.where(mine == 1, second, first)
    sent = jnp.where(mine == 1, first, second).astype(jnp.bfloat16)
    partners = [(i, i ^ (1 << bit)) for i in range(size)]
    return kept + lax.ppermute(sent, axis, partners).astype(jnp.float32)


def exchange_sums(kept, sent):
    owners = lax.axis_size("cfd")
    near = [("cfd", b) for b in range(owners.bit_length() - 1)]
    across = [("ac", b) for b in reversed(range(lax.axis_size("ac").bit_length() - 1))]
    orders = (near[:2] + across + near[2:], near[:1] + across + near[1:])
    partners = [(i, i ^ 1) for i in range(owners)]
    total = kept + lax.ppermute(sent, "cfd", partners).astype(jnp.float32)
    streams = jnp.split(total, len(orders), axis=1)
    for step in range(1, len(near) + len(across)):
        streams = [halve(part, *order[step]) for part, order in zip(streams, orders)]
    return jnp.concatenate([part[0] for part in streams], axis=0)


def flip(place, mask):
    out = place
    for bit in range(mask.bit_length()):
        if mask >> bit & 1:
            out = out + (1 << bit) * (1 - 2 * lax.rem(lax.div(place, 1 << bit), 2))
    return out


def fused_kernel(
    lags_ref,
    map_ref,
    ids_ref,
    normals_ref,
    surface_ref,
    weights_ref,
    first_ref,
    second_ref,
    lags,
    block_at,
    ids_here,
    flat_normals,
    surface,
    weights,
    normals,
    outgoing,
    arrived,
    sources,
    before,
    wide,
    spread,
    found,
    inverse,
    slots,
    rows,
    core_out,
    core_in,
    x_out,
    x_in,
    x_kept,
    y_out,
    y_in,
    y_kept,
    xy_out,
    xy_in,
    z_out,
    z_in,
    load_sems,
    block_send,
    block_recv,
    core_send,
    core_recv,
    first_send,
    first_recv,
    second_send,
    second_recv,
    z_send,
    z_recv,
):
    me = lax.axis_index("cfd")
    owners, pieces = outgoing.shape[:2]
    span = outgoing.shape[-1]
    zs = owners // 4
    core, x, z = lax.rem(me, 2), lax.rem(lax.div(me, 2), 2), lax.div(me, 4)
    y = lax.axis_index("ac")
    taps, terms, observers, faces = weights.shape
    bands, width = ids_here.shape
    size, steps = surface.shape[2:]
    out_len = steps // 2
    chunks = out_len // LANES
    height = observers // owners
    near = owners // zs

    get_surface = pltpu.make_async_copy(surface_ref, surface, load_sems.at[0])
    get_weights = pltpu.make_async_copy(weights_ref, weights, load_sems.at[1])
    get_surface.start()
    small = [
        pltpu.make_async_copy(src, dst, load_sems.at[3 + n])
        for n, (src, dst) in enumerate(
            (
                (normals_ref, flat_normals),
                (map_ref, block_at),
                (ids_ref, ids_here),
                (lags_ref, lags),
            )
        )
    ]
    for copy in small:
        copy.start()

    def remote(src, dst, send, recv, **peer):
        return pltpu.make_async_remote_copy(
            src_ref=src, dst_ref=dst, send_sem=send, recv_sem=recv,
            device_id=peer, device_id_type=pl.DeviceIdType.MESH,
        )

    barrier = pltpu.get_barrier_semaphore()
    for k in range(1, owners):
        pl.semaphore_signal(
            barrier, inc=1, device_id={"cfd": flip(me, k)}, device_id_type=pl.DeviceIdType.MESH
        )
    pl.semaphore_signal(barrier, inc=1, device_id={"ac": 1 - y}, device_id_type=pl.DeviceIdType.MESH)

    for copy in small:
        copy.wait()
    flat = flat_normals[...].astype(jnp.float32)
    tall = jnp.concatenate([flat, jnp.zeros((LANES - flat.shape[0], faces), jnp.float32)], axis=0)
    normals[...] = tall.T.reshape(owners, size, LANES)
    get_surface.wait()
    get_weights.start()

    def thick_block(place):
        along = surface[2, place].astype(jnp.float32) * normals[place, :, 0:1]
        along = along + surface[3, place].astype(jnp.float32) * normals[place, :, 1:2]
        along = along + surface[4, place].astype(jnp.float32) * normals[place, :, 2:3]
        return (surface[1, place].astype(jnp.float32) * along).astype(jnp.bfloat16)

    def cut(value, c):
        return value[:, c * span : (c + 1) * span]

    order = sorted(range(1, owners), key=lambda k: send_order(k, near))
    for k in order:
        place = block_at[flip(me, k)]
        thick, pressure = thick_block(place), surface[0, place]
        for c in range(pieces):
            outgoing[k, c, 0], outgoing[k, c, 1] = cut(thick, c), cut(pressure, c)
    place = block_at[me]
    thick, pressure = thick_block(place), surface[0, place]
    for c in range(pieces):
        arrived[c, me, 0], arrived[c, me, 1] = cut(thick, c), cut(pressure, c)
    pl.semaphore_wait(barrier, owners)
    block_copies = {}
    for c in range(pieces):
        for k in order:
            block_copies[c, k] = remote(
                outgoing.at[k, c],
                arrived.at[c, me],
                block_send.at[k, c],
                block_recv.at[k, c],
                cfd=flip(me, k),
            )
            block_copies[c, k].start()

    ids = ids_here[...]
    down = jnp.concatenate([ids, jnp.zeros((LANES - bands, width), jnp.int32)], axis=0).T
    for b in range(bands):
        spread[b] = jnp.broadcast_to(down[:, b : b + 1], (width, LANES))
    lane = lax.broadcasted_iota(jnp.int32, (width, LANES), 1)
    slot = lax.broadcasted_iota(jnp.int32, (width, LANES), 0)

    @pl.loop(0, observers // LANES)
    def _(part):
        def add(b, total):
            hit = spread[b] == lane + part * LANES
            return jnp.where(hit, slot + b * width, total)

        total = lax.fori_loop(0, bands, add, jnp.zeros((width, LANES), jnp.int32))
        found[pl.ds(part, 1), :] = jnp.max(total, axis=0, keepdims=True)

    get_inverse = pltpu.make_async_copy(found, inverse, load_sems.at[2])
    get_inverse.start()

    start_lane = lax.broadcasted_iota(jnp.int32, (faces, LANES), 1) == 0
    bands_each = 8
    rows_each = bands_each * width

    def source_tile(c, u):
        tile = c * (span // LANES) + u
        lanes = slice(u * LANES, (u + 1) * LANES)

        def late(value, place):
            turned = pltpu.roll(value, 1, 1)
            moved = jnp.where(start_lane, before[place], turned) if tile else turned
            before[place] = turned
            return moved

        for n in range(2):
            value = arrived[c, :, n, :, lanes].astype(jnp.float32).reshape(faces, LANES)
            last = late(value, 2 * n)
            rate = value - last
            if tile == 0:
                rate = jnp.where(start_lane, 0.0, rate)
            rate = rate.astype(jnp.bfloat16).astype(jnp.float32)
            taken = [(n, rate, late(rate, 2 * n + 1))]
            if n == 1:
                taken.append((2, value, last))
            for term, now, then in taken:
                for k, series in enumerate((now, then)):
                    here = pl.ds((k * terms + term) * faces, faces)
                    sources[here, lanes] = series.astype(jnp.bfloat16)

    for c in range(pieces):
        for k in order:
            block_copies[c, k].wait()
        for u in range(span // LANES):
            source_tile(c, u)
        if c == 0:
            get_weights.wait()

        @pl.loop(0, observers // rows_each)
        def _(part):
            here = pl.ds(pl.multiple_of(part * rows_each, rows_each), rows_each)
            chosen = jnp.concatenate(
                [weights[k, t, here, :] for k in range(taps) for t in range(terms)], axis=1
            )
            product = jnp.dot(chosen, sources[...], preferred_element_type=jnp.float32)
            for u in range(span // LANES):
                wide[c * (span // LANES) + u, pl.ds(part * bands_each, bands_each)] = product[
                    :, u * LANES : (u + 1) * LANES
                ].reshape(bands_each, width, LANES)

    def shift_band(b):
        start = out_len - lags[b]
        tile = jnp.minimum(lax.div(start, LANES), steps // LANES - chunks - 1)
        rest = start - tile * LANES
        shift = lax.rem(LANES - rest, LANES)
        parts = [pltpu.roll(wide[tile + t, b], shift, 1) for t in range(chunks + 1)]
        for t in range(chunks):
            slots[pl.ds(b * (width * chunks) + t, width, stride=chunks), :] = jnp.where(
                lane < LANES - rest, parts[t], parts[t + 1]
            )

    @pl.loop(0, bands // 4)
    def _(group):
        for m in range(4):
            shift_band(group * 4 + m)

    get_inverse.wait()
    unroll = 32

    def gather(top, side):
        @pl.loop(0, 2)
        def _(other):
            owner = top + other * 2 + side
            base = pl.multiple_of(owner * (height * chunks), height * chunks)
            for first in range(0, height, unroll):
                places = [inverse[owner, first + m] for m in range(unroll)]
                values = [slots.reshape(observers, chunks, LANES)[place] for place in places]
                for m, value in enumerate(values):
                    rows[pl.ds(base + (first + m) * chunks, chunks), :] = value

    def unit(owner, t):
        return rows[pl.ds(owner * (height * chunks) + t, height, stride=chunks), :]

    def narrow(value):
        return value.astype(jnp.bfloat16)

    def wide_of(value):
        return value.astype(jnp.float32)

    half = chunks // 2
    core_copies, x_copies, y_copies, xy_copies, yx_copies, z_copies = {}, {}, {}, {}, {}, {}
    turn = list(range(2, zs)) + [1, 0]

    def send_core(j):
        top = flip(z, j) * near
        gather(top, 1 - core)
        for other in range(2):
            for t in range(chunks):
                core_out[j, other, t] = narrow(unit(top + other * 2 + 1 - core, t))
        core_copies[j] = remote(
            core_out.at[j], core_in.at[j], core_send.at[j], core_recv.at[j], cfd=flip(me, 1)
        )
        core_copies[j].start()
        gather(top, core)

    def send_first(j):
        top = flip(z, j) * near
        core_copies[j].wait()

        def total(other, t):
            return unit(top + other * 2 + core, t) + wide_of(core_in[j, other, t])

        for side in range(2):
            x_out[j, side] = narrow(total(1 - x, side * half))
        x_copies[j] = remote(
            x_out.at[j], x_in.at[j], first_send.at[0, j], first_recv.at[0, j], cfd=flip(me, 2)
        )
        x_copies[j].start()
        for other in range(2):
            y_out[j, other] = narrow(total(other, (1 - y) * half + 1))
        y_copies[j] = remote(
            y_out.at[j], y_in.at[j], first_send.at[1, j], first_recv.at[1, j], ac=1 - y
        )
        y_copies[j].start()
        for side in range(2):
            x_kept[j, side] = total(x, side * half)
        for other in range(2):
            y_kept[j, other] = total(other, y * half + 1)

    def send_second(j):
        x_copies[j].wait()
        xy_out[0, j] = narrow(x_kept[j, 1 - y] + wide_of(x_in[j, 1 - y]))
        xy_copies[j] = remote(
            xy_out.at[0, j], xy_in.at[0, j], second_send.at[0, j], second_recv.at[0, j], ac=1 - y
        )
        xy_copies[j].start()
        y_copies[j].wait()
        xy_out[1, j] = narrow(y_kept[j, 1 - x] + wide_of(y_in[j, 1 - x]))
        yx_copies[j] = remote(
            xy_out.at[1, j], xy_in.at[1, j], second_send.at[1, j], second_recv.at[1, j],
            cfd=flip(me, 2),
        )
        yx_copies[j].start()

    def finish_second(j):
        xy_copies[j].wait()
        from_x = x_kept[j, y] + wide_of(x_in[j, y]) + wide_of(xy_in[0, j])
        yx_copies[j].wait()
        from_y = y_kept[j, x] + wide_of(y_in[j, x]) + wide_of(xy_in[1, j])
        return from_x, from_y

    def send_z(j):
        for stream, value in enumerate(finish_second(j)):
            z_out[j, stream] = narrow(value)
        z_copies[j] = remote(
            z_out.at[j], z_in.at[j], z_send.at[j], z_recv.at[j], cfd=flip(me, near * j)
        )
        z_copies[j].start()

    for step in range(zs + 4):
        if step < zs:
            send_core(turn[step])
        if 1 <= step < zs:
            send_first(turn[step - 1])
        if 3 <= step < zs + 3:
            send_second(turn[step - 3])
        if step == zs:
            send_first(turn[-1])
        if 4 <= step < zs + 3:
            send_z(turn[step - 4])
    results = list(finish_second(0))
    for j in turn[:-1]:
        z_copies[j].wait()
        results = [value + wide_of(z_in[j, s]) for s, value in enumerate(results)]
    for value, result_ref in zip(results, (first_ref, second_ref)):
        result_ref[...] = value


def send_order(k, near):
    j = k // near
    return (0, 3, 1, 2)[j] if j < 4 else j, k


def fused(surface_raw, area_normals, kernel_weights, block_map, band_observers, band_lags):
    owners, halves = lax.axis_size("cfd"), lax.axis_size("ac")
    faces, steps = surface_raw.shape[1:]
    taps, terms, observers, _ = kernel_weights.shape
    bands, width = band_observers.shape
    size, height = faces // owners, observers // owners
    chunks = steps // 2 // LANES
    zs = owners // 4
    near = owners // zs
    bf16, f32, i32 = jnp.bfloat16, jnp.float32, jnp.int32
    tile = (height, LANES)
    dma = pltpu.SemaphoreType.DMA
    vmem, hbm = (pl.BlockSpec(memory_space=space) for space in (pltpu.VMEM, pltpu.HBM))
    pieces = 4
    span = steps // pieces
    first, second = pl.pallas_call(
        fused_kernel,
        out_shape=[jax.ShapeDtypeStruct(tile, f32)] * 2,
        in_specs=[hbm] * 6,
        out_specs=[vmem, vmem],
        scratch_shapes=[
            pltpu.SMEM((bands,), i32),
            pltpu.SMEM((owners,), i32),
            pltpu.VMEM((bands, width), i32),
            pltpu.VMEM(area_normals.shape, bf16),
            pltpu.VMEM((surface_raw.shape[0], owners, size, steps), bf16),
            pltpu.VMEM(kernel_weights.shape, bf16),
            pltpu.VMEM((owners, size, LANES), f32),
            pltpu.VMEM((owners, pieces, 2, size, span), bf16),
            pltpu.VMEM((pieces, owners, 2, size, span), bf16),
            pltpu.VMEM((taps * terms * faces, span), bf16),
            pltpu.VMEM((4,) + tile, f32),
            pltpu.VMEM((steps // LANES, bands, width, LANES), f32),
            pltpu.VMEM((bands, width, LANES), i32),
            pltpu.VMEM((observers // LANES, LANES), i32),
            pltpu.SMEM((observers // LANES, LANES), i32),
            pltpu.VMEM((observers * chunks, LANES), f32),
            pltpu.VMEM((observers * chunks, LANES), f32),
            pltpu.VMEM((zs, 2, chunks) + tile, bf16),
            pltpu.VMEM((zs, 2, chunks) + tile, bf16),
            pltpu.VMEM((zs, 2) + tile, bf16),
            pltpu.VMEM((zs, 2) + tile, bf16),
            pltpu.VMEM((zs, 2) + tile, f32),
            pltpu.VMEM((zs, 2) + tile, bf16),
            pltpu.VMEM((zs, 2) + tile, bf16),
            pltpu.VMEM((zs, 2) + tile, f32),
            pltpu.VMEM((2, zs) + tile, bf16),
            pltpu.VMEM((2, zs) + tile, bf16),
            pltpu.VMEM((zs, 2) + tile, bf16),
            pltpu.VMEM((zs, 2) + tile, bf16),
            dma((7,)),
            dma((owners, pieces)),
            dma((owners, pieces)),
            dma((zs,)),
            dma((zs,)),
            dma((2, zs)),
            dma((2, zs)),
            dma((2, zs)),
            dma((2, zs)),
            dma((zs,)),
            dma((zs,)),
        ],
        compiler_params=pltpu.CompilerParams(
            collective_id=0, has_side_effects=True, vmem_limit_bytes=40 * 2**20
        ),
        name="fused",
    )(
        *(
            pltpu.with_memory_space_constraint(value, pltpu.HBM)
            for value in (
                band_lags,
                block_map[0, 0],
                band_observers,
                area_normals,
                surface_raw.reshape(surface_raw.shape[0], owners, size, steps),
                kernel_weights,
            )
        )
    )
    return jnp.concatenate([first, second], axis=1)


def fits_fused(owners, halves, surface_raw, kernel_weights, band_observers):
    faces, steps = surface_raw.shape[1:]
    tiles = halves * 2
    return (
        halves == 2
        and owners % 4 == 0
        and owners & (owners - 1) == 0
        and faces == LANES
        and band_observers.shape[1] == LANES
        and faces // owners % 8 == 0
        and steps == 2 * tiles * LANES
        and kernel_weights.shape[:1] + kernel_weights.shape[2:3] == (2, owners * LANES)
        and band_observers.shape[0] % 8 == 0
    )


def general(surface_raw, area_normals, kernel_weights, block_map, band_observers, band_lags):
    blocks = lax.axis_size("cfd")
    faces, steps = surface_raw.shape[1:]
    size = faces // blocks
    outgoing = prepare(surface_raw, area_normals, block_map[0, 0])
    arrived = lax.all_to_all(outgoing, "cfd", split_axis=0, concat_axis=0, tiled=True)
    arrived = arrived.reshape(blocks, 2, size, steps)
    if size % 8:
        arrived = arrived.transpose(1, 0, 2, 3).reshape(2 * faces, steps)
    shape = (blocks // 2, kernel_weights.shape[2] // blocks, steps // 2)
    kept, sent = banded_call(
        halves_kernel,
        [jax.ShapeDtypeStruct(shape, kind) for kind in (jnp.float32, jnp.bfloat16)],
        arrived,
        kernel_weights,
        band_observers,
        band_lags,
        (lax.axis_index("cfd") & 1).astype(jnp.int32).reshape(1),
    )
    return exchange_sums(kept, sent)


def local(surface_raw, area_normals, kernel_weights, block_map, band_observers, band_lags):
    owners, halves = lax.axis_size("cfd"), lax.axis_size("ac")
    fast = fits_fused(owners, halves, surface_raw, kernel_weights, band_observers)
    run = fused if fast else general
    return run(surface_raw, area_normals, kernel_weights, block_map, band_observers, band_lags)


def solution(mesh):
    placed = (
        P(None, ("cfd", "ac"), None),
        P(None, ("cfd", "ac")),
        P(None, None, None, ("cfd", "ac")),
        P("ac", "cfd", None),
        P(),
        P(),
    )
    return jax.shard_map(
        local, mesh=mesh, in_specs=placed, out_specs=P("cfd", "ac"), check_vma=False
    )
```

```python
import functools

import jax
import jax.numpy as jnp
from jax import lax
from jax.experimental import pallas as pl
from jax.experimental.pallas import tpu as pltpu
from jax.sharding import PartitionSpec as P

LANES = 128


def prepare_kernel(src_ref, normals_ref, surface_ref, out_ref):
    along = surface_ref[2].astype(jnp.float32) * normals_ref[:, 0:1]
    along = along + surface_ref[3].astype(jnp.float32) * normals_ref[:, 1:2]
    along = along + surface_ref[4].astype(jnp.float32) * normals_ref[:, 2:3]
    thick = (surface_ref[1].astype(jnp.float32) * along).astype(jnp.bfloat16)
    both = jnp.concatenate([thick, surface_ref[0]], axis=0)
    rows = both.shape[0]
    column = lax.broadcasted_iota(jnp.int32, (rows, rows), 1)
    onehot = jnp.where(column == src_ref[...], 1.0, 0.0).astype(jnp.bfloat16)
    picked = jnp.dot(onehot, both, preferred_element_type=jnp.float32)
    out_ref[...] = picked.astype(jnp.bfloat16)


def prepare(surface_raw, area_normals, block_order):
    faces, steps = surface_raw.shape[1:]
    blocks = block_order.shape[0]
    size = faces // blocks
    src = (
        jnp.arange(2, dtype=jnp.int32)[None, :, None] * faces
        + block_order[:, None, None] * size
        + jnp.arange(size, dtype=jnp.int32)[None, None, :]
    ).reshape(2 * faces, 1)
    return pl.pallas_call(
        prepare_kernel,
        out_shape=jax.ShapeDtypeStruct((2 * faces, steps), jnp.bfloat16),
        name="prepare",
    )(src, area_normals.T.astype(jnp.float32), surface_raw)


def scatter_bands(lags_ref, ids_ref, arrived_ref, weights_ref, sources, band, rows):
    index = pl.program_id(0)
    taps, terms, width, faces = weights_ref.shape
    steps = sources.shape[1]
    out_len = steps // 2
    chunks = out_len // LANES

    @pl.when(index == 0)
    def _():
        series = arrived_ref[...].astype(jnp.float32)
        if len(arrived_ref.shape) == 4:
            thick = series[:, 0].reshape(faces, steps)
            pressure = series[:, 1].reshape(faces, steps)
        else:
            thick, pressure = series[:faces], series[faces:]
        step = lax.broadcasted_iota(jnp.int32, (faces, steps), 1)

        def rate(x):
            moved = jnp.where(step > 0, x - pltpu.roll(x, 1, 1), 0.0)
            return moved.astype(jnp.bfloat16).astype(jnp.float32)

        for c, x in enumerate((rate(thick), rate(pressure), pressure)):
            for k in range(taps):
                late = pltpu.roll(x, k, 1) if k else x
                sources[pl.ds((k * terms + c) * faces, faces), :] = late.astype(jnp.bfloat16)

    start = out_len - lags_ref[index]
    tile = jnp.minimum(start // LANES, steps // LANES - chunks - 1)
    rest = start - tile * LANES
    shift = lax.rem(LANES - rest, LANES)
    chosen = jnp.concatenate(
        [weights_ref[k, c] for k in range(taps) for c in range(terms)], axis=1
    )
    window = sources[:, pl.ds(pl.multiple_of(tile * LANES, LANES), out_len + LANES)]
    wide = jnp.dot(chosen, window, preferred_element_type=jnp.float32)
    lane = lax.broadcasted_iota(jnp.int32, (width, LANES), 1)
    parts = [
        pltpu.roll(wide[:, t * LANES : (t + 1) * LANES], shift, 1) for t in range(chunks + 1)
    ]
    for t in range(chunks):
        band[pl.ds(t, width, stride=chunks), :] = jnp.where(
            lane < LANES - rest, parts[t], parts[t + 1]
        )

    unroll = 32

    @pl.loop(0, width // unroll)
    def _(group):
        slots = [group * unroll + m for m in range(unroll)]
        places = [ids_ref[index * width + slot] for slot in slots]
        values = [
            band[pl.ds(pl.multiple_of(slot * chunks, chunks), chunks), :] for slot in slots
        ]
        for place, value in zip(places, values):
            rows[pl.ds(pl.multiple_of(place * chunks, chunks), chunks), :] = value


def halves_kernel(
    lags_ref, ids_ref, mine_ref, arrived_ref, weights_ref, kept_ref, sent_ref, sources, band, rows
):
    scatter_bands(lags_ref, ids_ref, arrived_ref, weights_ref, sources, band, rows)
    pairs, height, out_len = kept_ref.shape
    chunks = out_len // LANES
    mine = mine_ref[0]

    @pl.when(pl.program_id(0) == pl.num_programs(0) - 1)
    def _():
        for pair in range(pairs):
            for t in range(chunks):
                lanes = slice(t * LANES, (t + 1) * LANES)
                for out, owner in ((kept_ref, 2 * pair + mine), (sent_ref, 2 * pair + 1 - mine)):
                    first = pl.multiple_of(owner * (height * chunks), height * chunks)
                    part = rows[pl.ds(first + t, height, stride=chunks), :]
                    out[pair, :, lanes] = part.astype(out.dtype)


def banded_call(kernel, outs, arrived, kernel_weights, band_observers, band_lags, mine):
    taps, terms, observers, faces = kernel_weights.shape
    bands, width = band_observers.shape
    steps = arrived.shape[-1]
    chunks = steps // 2 // LANES
    rank = len(arrived.shape)
    return pl.pallas_call(
        kernel,
        out_shape=outs,
        grid_spec=pltpu.PrefetchScalarGridSpec(
            num_scalar_prefetch=3,
            grid=(bands,),
            in_specs=[
                pl.BlockSpec(arrived.shape, lambda b, *_: (0,) * rank),
                pl.BlockSpec((taps, terms, width, faces), lambda b, *_: (0, 0, b, 0)),
            ],
            out_specs=jax.tree.map(
                lambda o: pl.BlockSpec(o.shape, lambda b, *_: (0,) * len(o.shape)), outs
            ),
            scratch_shapes=[
                pltpu.VMEM((taps * terms * faces, steps), jnp.bfloat16),
                pltpu.VMEM((width * chunks, LANES), jnp.float32),
                pltpu.VMEM((observers * chunks, LANES), jnp.float32),
            ],
        ),
        compiler_params=pltpu.CompilerParams(dimension_semantics=("arbitrary",)),
        name="bands",
    )(band_lags, band_observers.reshape(-1), mine, arrived, kernel_weights)


def halve(total, axis, bit):
    size = lax.axis_size(axis)
    mine = (lax.axis_index(axis) >> bit) & 1
    if axis == "cfd":
        owners, rows, times = total.shape
        pairs = total.reshape(owners // 2, 2, rows, times)
        first, second = pairs[:, 0], pairs[:, 1]
    else:
        first, second = jnp.split(total, 2, axis=2)
    kept = jnp.where(mine == 1, second, first)
    sent = jnp.where(mine == 1, first, second).astype(jnp.bfloat16)
    partners = [(i, i ^ (1 << bit)) for i in range(size)]
    return kept + lax.ppermute(sent, axis, partners).astype(jnp.float32)


def exchange_sums(kept, sent):
    owners = lax.axis_size("cfd")
    near = [("cfd", b) for b in range(owners.bit_length() - 1)]
    across = [("ac", b) for b in reversed(range(lax.axis_size("ac").bit_length() - 1))]
    orders = (near[:2] + across + near[2:], near[:1] + across + near[1:])
    partners = [(i, i ^ 1) for i in range(owners)]
    total = kept + lax.ppermute(sent, "cfd", partners).astype(jnp.float32)
    streams = jnp.split(total, len(orders), axis=1)
    for step in range(1, len(near) + len(across)):
        streams = [halve(part, *order[step]) for part, order in zip(streams, orders)]
    return jnp.concatenate([part[0] for part in streams], axis=0)


def flip(place, mask):
    out = place
    for bit in range(mask.bit_length()):
        if mask >> bit & 1:
            out = out + (1 << bit) * (1 - 2 * lax.rem(lax.div(place, 1 << bit), 2))
    return out


def fused_kernel(
    lags_ref,
    map_ref,
    ids_ref,
    normals_ref,
    surface_ref,
    weights_ref,
    first_ref,
    second_ref,
    lags,
    block_at,
    ids_here,
    flat_normals,
    surface,
    weights,
    normals,
    outgoing,
    arrived,
    sources,
    before,
    wide,
    spread,
    found,
    inverse,
    slots,
    rows,
    core_out,
    core_in,
    x_out,
    x_in,
    x_kept,
    y_out,
    y_in,
    y_kept,
    xy_out,
    xy_in,
    z_out,
    z_in,
    load_sems,
    block_send,
    block_recv,
    core_send,
    core_recv,
    first_send,
    first_recv,
    second_send,
    second_recv,
    z_send,
    z_recv,
):
    me = lax.axis_index("cfd")
    owners, pieces = outgoing.shape[:2]
    span = outgoing.shape[-1]
    zs = owners // 4
    core, x, z = lax.rem(me, 2), lax.rem(lax.div(me, 2), 2), lax.div(me, 4)
    y = lax.axis_index("ac")
    taps, terms, observers, faces = weights.shape
    bands, width = ids_here.shape
    size, steps = surface.shape[2:]
    out_len = steps // 2
    chunks = out_len // LANES
    height = observers // owners
    half = chunks // 2
    near = owners // zs

    get_surface = pltpu.make_async_copy(surface_ref, surface, load_sems.at[0])
    get_weights = pltpu.make_async_copy(weights_ref, weights, load_sems.at[1])
    get_surface.start()
    small = [
        pltpu.make_async_copy(src, dst, load_sems.at[3 + n])
        for n, (src, dst) in enumerate(
            (
                (normals_ref, flat_normals),
                (map_ref, block_at),
                (ids_ref, ids_here),
                (lags_ref, lags),
            )
        )
    ]
    for copy in small:
        copy.start()

    def remote(src, dst, send, recv, **peer):
        return pltpu.make_async_remote_copy(
            src_ref=src, dst_ref=dst, send_sem=send, recv_sem=recv,
            device_id=peer, device_id_type=pl.DeviceIdType.MESH,
        )

    barrier = pltpu.get_barrier_semaphore()
    for k in range(1, owners):
        pl.semaphore_signal(
            barrier, inc=1, device_id={"cfd": flip(me, k)}, device_id_type=pl.DeviceIdType.MESH
        )
    pl.semaphore_signal(barrier, inc=1, device_id={"ac": 1 - y}, device_id_type=pl.DeviceIdType.MESH)

    for copy in small:
        copy.wait()
    flat = flat_normals[...].astype(jnp.float32)
    tall = jnp.concatenate([flat, jnp.zeros((LANES - flat.shape[0], faces), jnp.float32)], axis=0)
    normals[...] = tall.T.reshape(owners, size, LANES)
    get_surface.wait()
    get_weights.start()

    def wait_all(ref, sem):
        pltpu.make_async_copy(ref, ref, sem).wait()

    def thick_block(place):
        along = surface[2, place].astype(jnp.float32) * normals[place, :, 0:1]
        along = along + surface[3, place].astype(jnp.float32) * normals[place, :, 1:2]
        along = along + surface[4, place].astype(jnp.float32) * normals[place, :, 2:3]
        return (surface[1, place].astype(jnp.float32) * along).astype(jnp.bfloat16)

    def cut(value, c):
        return value[:, c * span : (c + 1) * span]

    order = sorted(range(1, owners), key=lambda k: send_order(k, near))
    for k in order:
        place = block_at[flip(me, k)]
        thick, pressure = thick_block(place), surface[0, place]
        for c in range(pieces):
            outgoing[k, c, 0], outgoing[k, c, 1] = cut(thick, c), cut(pressure, c)
    place = block_at[me]
    thick, pressure = thick_block(place), surface[0, place]
    for c in range(pieces):
        arrived[c, me, 0], arrived[c, me, 1] = cut(thick, c), cut(pressure, c)
    pl.semaphore_wait(barrier, owners)
    for c in range(pieces):
        for k in order:
            remote(
                outgoing.at[k, c],
                arrived.at[c, me],
                block_send.at[0],
                block_recv.at[c],
                cfd=flip(me, k),
            ).start()

    ids = ids_here[...]
    down = jnp.concatenate([ids, jnp.zeros((LANES - bands, width), jnp.int32)], axis=0).T
    for b in range(bands):
        spread[b] = jnp.broadcast_to(down[:, b : b + 1], (width, LANES))
    lane = lax.broadcasted_iota(jnp.int32, (width, LANES), 1)
    slot = lax.broadcasted_iota(jnp.int32, (width, LANES), 0)

    @pl.loop(0, observers // LANES)
    def _(part):
        def add(b, total):
            hit = spread[b] == lane + part * LANES
            return jnp.where(hit, slot + b * width, total)

        total = lax.fori_loop(0, bands, add, jnp.zeros((width, LANES), jnp.int32))
        found[pl.ds(part, 1), :] = jnp.max(total, axis=0, keepdims=True)

    get_inverse = pltpu.make_async_copy(found, inverse, load_sems.at[2])
    get_inverse.start()

    start_lane = lax.broadcasted_iota(jnp.int32, (faces, LANES), 1) == 0
    bands_each = 8
    rows_each = bands_each * width

    def source_tile(c, u):
        tile = c * (span // LANES) + u
        lanes = slice(u * LANES, (u + 1) * LANES)

        def late(value, place):
            turned = pltpu.roll(value, 1, 1)
            moved = jnp.where(start_lane, before[place], turned) if tile else turned
            before[place] = turned
            return moved

        for n in range(2):
            value = arrived[c, :, n, :, lanes].astype(jnp.float32).reshape(faces, LANES)
            last = late(value, 2 * n)
            rate = value - last
            if tile == 0:
                rate = jnp.where(start_lane, 0.0, rate)
            rate = rate.astype(jnp.bfloat16).astype(jnp.float32)
            taken = [(n, rate, late(rate, 2 * n + 1))]
            if n == 1:
                taken.append((2, value, last))
            for term, now, then in taken:
                for k, series in enumerate((now, then)):
                    here = pl.ds((k * terms + term) * faces, faces)
                    sources[here, lanes] = series.astype(jnp.bfloat16)

    def shift_band(b, first, last):
        start = out_len - lags[b]
        tile = jnp.minimum(lax.div(start, LANES), steps // LANES - chunks - 1)
        rest = start - tile * LANES
        shift = lax.rem(LANES - rest, LANES)
        parts = [pltpu.roll(wide[tile + t, b], shift, 1) for t in range(first, last + 1)]
        early = lane[:8] < LANES - rest
        for top in range(0, width, 8):
            for t in range(first, last):
                now, then = (parts[t - first + n][top : top + 8] for n in range(2))
                here = pl.ds(b * (width * chunks) + top * chunks + t, 8, stride=chunks)
                slots[here, :] = jnp.where(early, now, then)

    for c in range(pieces):
        wait_all(arrived.at[c, pl.ds(0, owners - 1)], block_recv.at[c])
        for u in range(span // LANES):
            source_tile(c, u)
        if c == 0:
            get_weights.wait()

        @pl.loop(0, observers // rows_each)
        def _(part):
            if c == pieces - 1:
                for m in range(bands_each):
                    shift_band(part * bands_each + m, 0, half)
            here = pl.ds(pl.multiple_of(part * rows_each, rows_each), rows_each)
            chosen = jnp.concatenate(
                [weights[k, t, here, :] for k in range(taps) for t in range(terms)], axis=1
            )
            product = jnp.dot(chosen, sources[...], preferred_element_type=jnp.float32)
            for u in range(span // LANES):
                wide[c * (span // LANES) + u, pl.ds(part * bands_each, bands_each)] = product[
                    :, u * LANES : (u + 1) * LANES
                ].reshape(bands_each, width, LANES)

    @pl.loop(0, bands // 4)
    def _(group):
        for m in range(4):
            shift_band(group * 4 + m, half, chunks)

    get_inverse.wait()
    unroll = 32

    def gather(top, side):
        @pl.loop(0, 2)
        def _(other):
            owner = top + other * 2 + side
            base = pl.multiple_of(owner * (height * chunks), height * chunks)
            for first in range(0, height, unroll):
                places = [inverse[owner, first + m] for m in range(unroll)]
                values = [slots.reshape(observers, chunks, LANES)[place] for place in places]
                for m, value in enumerate(values):
                    rows[pl.ds(base + (first + m) * chunks, chunks), :] = value

    def unit(owner, t):
        return rows[pl.ds(owner * (height * chunks) + t, height, stride=chunks), :]

    def narrow(value):
        return value.astype(jnp.bfloat16)

    def wide_of(value):
        return value.astype(jnp.float32)

    core_copies, x_copies, y_copies, xy_copies, yx_copies = {}, {}, {}, {}, {}
    turn = list(range(2, zs)) + [1, 0]

    def send_core(j):
        top = flip(z, j) * near
        gather(top, 1 - core)
        for other in range(2):
            for t in range(chunks):
                core_out[j, other, t] = narrow(unit(top + other * 2 + 1 - core, t))
        core_copies[j] = remote(
            core_out.at[j], core_in.at[j], core_send.at[0], core_recv.at[j], cfd=flip(me, 1)
        )
        core_copies[j].start()
        gather(top, core)

    def send_first(j):
        top = flip(z, j) * near
        core_copies[j].wait_recv()

        def total(other, t):
            return unit(top + other * 2 + core, t) + wide_of(core_in[j, other, t])

        for n, (side, other) in enumerate(((1 - y, 1 - x), (y, x))):
            x_out[j, side] = narrow(total(1 - x, side * half))
            x_copies[j, n] = remote(
                x_out.at[j, side],
                x_in.at[j, side],
                first_send.at[0],
                first_recv.at[0, n, j],
                cfd=flip(me, 2),
            )
            x_copies[j, n].start()
            y_out[j, other] = narrow(total(other, (1 - y) * half + 1))
            y_copies[j, n] = remote(
                y_out.at[j, other],
                y_in.at[j, other],
                first_send.at[1],
                first_recv.at[1, n, j],
                ac=1 - y,
            )
            y_copies[j, n].start()
        for side in range(2):
            x_kept[j, side] = total(x, side * half)
        for other in range(2):
            y_kept[j, other] = total(other, y * half + 1)

    def send_second(j):
        x_copies[j, 0].wait_recv()
        xy_out[0, j] = narrow(x_kept[j, 1 - y] + wide_of(x_in[j, 1 - y]))
        xy_copies[j] = remote(
            xy_out.at[0, j], xy_in.at[0, j], second_send.at[0], second_recv.at[0, j], ac=1 - y
        )
        xy_copies[j].start()
        y_copies[j, 0].wait_recv()
        xy_out[1, j] = narrow(y_kept[j, 1 - x] + wide_of(y_in[j, 1 - x]))
        yx_copies[j] = remote(
            xy_out.at[1, j],
            xy_in.at[1, j],
            second_send.at[0],
            second_recv.at[1, j],
            cfd=flip(me, 2),
        )
        yx_copies[j].start()

    def finish_second(j):
        x_copies[j, 1].wait_recv()
        xy_copies[j].wait_recv()
        from_x = x_kept[j, y] + wide_of(x_in[j, y]) + wide_of(xy_in[0, j])
        y_copies[j, 1].wait_recv()
        yx_copies[j].wait_recv()
        from_y = y_kept[j, x] + wide_of(y_in[j, x]) + wide_of(xy_in[1, j])
        return from_x, from_y

    def send_z(j):
        for stream, value in enumerate(finish_second(j)):
            z_out[j, stream] = narrow(value)
        remote(
            z_out.at[j], z_in.at[j], z_send.at[0], z_recv.at[0], cfd=flip(me, near * j)
        ).start()

    for step in range(zs + 5):
        if step < zs:
            send_core(turn[step])
        if 1 <= step < zs - 1:
            send_first(turn[step - 1])
        if 3 <= step < zs + 3:
            send_second(turn[step - 3])
        if zs - 1 <= step < zs + 1:
            send_first(turn[step - 1])
        if 4 <= step < zs + 3:
            send_z(turn[step - 4])
    results = list(finish_second(0))
    wait_all(outgoing.at[pl.ds(1, owners - 1)], block_send.at[0])
    wait_all(core_out, core_send.at[0])
    wait_all(x_out, first_send.at[0])
    wait_all(y_out, first_send.at[1])
    wait_all(xy_out, second_send.at[0])
    wait_all(z_out.at[pl.ds(1, zs - 1)], z_send.at[0])
    wait_all(z_in.at[pl.ds(1, zs - 1)], z_recv.at[0])
    for j in turn[:-1]:
        results = [value + wide_of(z_in[j, s]) for s, value in enumerate(results)]
    for value, result_ref in zip(results, (first_ref, second_ref)):
        result_ref[...] = value


def send_order(k, near):
    j = k // near
    return (0, 3, 1, 2)[j] if j < 4 else j, k


def fused(surface_raw, area_normals, kernel_weights, block_map, band_observers, band_lags):
    owners, halves = lax.axis_size("cfd"), lax.axis_size("ac")
    faces, steps = surface_raw.shape[1:]
    taps, terms, observers, _ = kernel_weights.shape
    bands, width = band_observers.shape
    size, height = faces // owners, observers // owners
    chunks = steps // 2 // LANES
    zs = owners // 4
    near = owners // zs
    bf16, f32, i32 = jnp.bfloat16, jnp.float32, jnp.int32
    tile = (height, LANES)
    dma = pltpu.SemaphoreType.DMA
    vmem, hbm = (pl.BlockSpec(memory_space=space) for space in (pltpu.VMEM, pltpu.HBM))
    pieces = 4
    span = steps // pieces
    first, second = pl.pallas_call(
        fused_kernel,
        out_shape=[jax.ShapeDtypeStruct(tile, f32)] * 2,
        in_specs=[hbm] * 6,
        out_specs=[vmem, vmem],
        scratch_shapes=[
            pltpu.SMEM((bands,), i32),
            pltpu.SMEM((owners,), i32),
            pltpu.VMEM((bands, width), i32),
            pltpu.VMEM(area_normals.shape, bf16),
            pltpu.VMEM((surface_raw.shape[0], owners, size, steps), bf16),
            pltpu.VMEM(kernel_weights.shape, bf16),
            pltpu.VMEM((owners, size, LANES), f32),
            pltpu.VMEM((owners, pieces, 2, size, span), bf16),
            pltpu.VMEM((pieces, owners, 2, size, span), bf16),
            pltpu.VMEM((taps * terms * faces, span), bf16),
            pltpu.VMEM((4,) + tile, f32),
            pltpu.VMEM((steps // LANES, bands, width, LANES), f32),
            pltpu.VMEM((bands, width, LANES), i32),
            pltpu.VMEM((observers // LANES, LANES), i32),
            pltpu.SMEM((observers // LANES, LANES), i32),
            pltpu.VMEM((observers * chunks, LANES), f32),
            pltpu.VMEM((observers * chunks, LANES), f32),
            pltpu.VMEM((zs, 2, chunks) + tile, bf16),
            pltpu.VMEM((zs, 2, chunks) + tile, bf16),
            pltpu.VMEM((zs, 2) + tile, bf16),
            pltpu.VMEM((zs, 2) + tile, bf16),
            pltpu.VMEM((zs, 2) + tile, f32),
            pltpu.VMEM((zs, 2) + tile, bf16),
            pltpu.VMEM((zs, 2) + tile, bf16),
            pltpu.VMEM((zs, 2) + tile, f32),
            pltpu.VMEM((2, zs) + tile, bf16),
            pltpu.VMEM((2, zs) + tile, bf16),
            pltpu.VMEM((zs, 2) + tile, bf16),
            pltpu.VMEM((zs, 2) + tile, bf16),
            dma((7,)),
            dma((1,)),
            dma((pieces,)),
            dma((1,)),
            dma((zs,)),
            dma((2,)),
            dma((2, 2, zs)),
            dma((1,)),
            dma((2, zs)),
            dma((1,)),
            dma((1,)),
        ],
        compiler_params=pltpu.CompilerParams(
            collective_id=0, has_side_effects=True, vmem_limit_bytes=40 * 2**20
        ),
        name="fused",
    )(
        *(
            pltpu.with_memory_space_constraint(value, pltpu.HBM)
            for value in (
                band_lags,
                block_map[0, 0],
                band_observers,
                area_normals,
                surface_raw.reshape(surface_raw.shape[0], owners, size, steps),
                kernel_weights,
            )
        )
    )
    return jnp.concatenate([first, second], axis=1)


def fits_fused(owners, halves, surface_raw, kernel_weights, band_observers):
    faces, steps = surface_raw.shape[1:]
    tiles = halves * 2
    return (
        halves == 2
        and owners % 4 == 0
        and owners & (owners - 1) == 0
        and faces == LANES
        and band_observers.shape[1] == LANES
        and faces // owners % 8 == 0
        and steps == 2 * tiles * LANES
        and kernel_weights.shape[:1] + kernel_weights.shape[2:3] == (2, owners * LANES)
        and band_observers.shape[0] % 8 == 0
    )


def general(surface_raw, area_normals, kernel_weights, block_map, band_observers, band_lags):
    blocks = lax.axis_size("cfd")
    faces, steps = surface_raw.shape[1:]
    size = faces // blocks
    outgoing = prepare(surface_raw, area_normals, block_map[0, 0])
    arrived = lax.all_to_all(outgoing, "cfd", split_axis=0, concat_axis=0, tiled=True)
    arrived = arrived.reshape(blocks, 2, size, steps)
    if size % 8:
        arrived = arrived.transpose(1, 0, 2, 3).reshape(2 * faces, steps)
    shape = (blocks // 2, kernel_weights.shape[2] // blocks, steps // 2)
    kept, sent = banded_call(
        halves_kernel,
        [jax.ShapeDtypeStruct(shape, kind) for kind in (jnp.float32, jnp.bfloat16)],
        arrived,
        kernel_weights,
        band_observers,
        band_lags,
        (lax.axis_index("cfd") & 1).astype(jnp.int32).reshape(1),
    )
    return exchange_sums(kept, sent)


def local(surface_raw, area_normals, kernel_weights, block_map, band_observers, band_lags):
    owners, halves = lax.axis_size("cfd"), lax.axis_size("ac")
    fast = fits_fused(owners, halves, surface_raw, kernel_weights, band_observers)
    run = fused if fast else general
    return run(surface_raw, area_normals, kernel_weights, block_map, band_observers, band_lags)


def solution(mesh):
    placed = (
        P(None, ("cfd", "ac"), None),
        P(None, ("cfd", "ac")),
        P(None, None, None, ("cfd", "ac")),
        P("ac", "cfd", None),
        P(),
        P(),
    )
    return jax.shard_map(
        local, mesh=mesh, in_specs=placed, out_specs=P("cfd", "ac"), check_vma=False
    )
```

```python
import functools

import jax
import jax.numpy as jnp
from jax import lax
from jax.experimental import pallas as pl
from jax.experimental.pallas import tpu as pltpu
from jax.sharding import PartitionSpec as P

LANES = 128


def prepare_kernel(src_ref, normals_ref, surface_ref, out_ref):
    along = surface_ref[2].astype(jnp.float32) * normals_ref[:, 0:1]
    along = along + surface_ref[3].astype(jnp.float32) * normals_ref[:, 1:2]
    along = along + surface_ref[4].astype(jnp.float32) * normals_ref[:, 2:3]
    thick = (surface_ref[1].astype(jnp.float32) * along).astype(jnp.bfloat16)
    both = jnp.concatenate([thick, surface_ref[0]], axis=0)
    rows = both.shape[0]
    column = lax.broadcasted_iota(jnp.int32, (rows, rows), 1)
    onehot = jnp.where(column == src_ref[...], 1.0, 0.0).astype(jnp.bfloat16)
    picked = jnp.dot(onehot, both, preferred_element_type=jnp.float32)
    out_ref[...] = picked.astype(jnp.bfloat16)


def prepare(surface_raw, area_normals, block_order):
    faces, steps = surface_raw.shape[1:]
    blocks = block_order.shape[0]
    size = faces // blocks
    src = (
        jnp.arange(2, dtype=jnp.int32)[None, :, None] * faces
        + block_order[:, None, None] * size
        + jnp.arange(size, dtype=jnp.int32)[None, None, :]
    ).reshape(2 * faces, 1)
    return pl.pallas_call(
        prepare_kernel,
        out_shape=jax.ShapeDtypeStruct((2 * faces, steps), jnp.bfloat16),
        name="prepare",
    )(src, area_normals.T.astype(jnp.float32), surface_raw)


def scatter_bands(lags_ref, ids_ref, arrived_ref, weights_ref, sources, band, rows):
    index = pl.program_id(0)
    taps, terms, width, faces = weights_ref.shape
    steps = sources.shape[1]
    out_len = steps // 2
    chunks = out_len // LANES

    @pl.when(index == 0)
    def _():
        series = arrived_ref[...].astype(jnp.float32)
        if len(arrived_ref.shape) == 4:
            thick = series[:, 0].reshape(faces, steps)
            pressure = series[:, 1].reshape(faces, steps)
        else:
            thick, pressure = series[:faces], series[faces:]
        step = lax.broadcasted_iota(jnp.int32, (faces, steps), 1)

        def rate(x):
            moved = jnp.where(step > 0, x - pltpu.roll(x, 1, 1), 0.0)
            return moved.astype(jnp.bfloat16).astype(jnp.float32)

        for c, x in enumerate((rate(thick), rate(pressure), pressure)):
            for k in range(taps):
                late = pltpu.roll(x, k, 1) if k else x
                sources[pl.ds((k * terms + c) * faces, faces), :] = late.astype(jnp.bfloat16)

    start = out_len - lags_ref[index]
    tile = jnp.minimum(start // LANES, steps // LANES - chunks - 1)
    rest = start - tile * LANES
    shift = lax.rem(LANES - rest, LANES)
    chosen = jnp.concatenate(
        [weights_ref[k, c] for k in range(taps) for c in range(terms)], axis=1
    )
    window = sources[:, pl.ds(pl.multiple_of(tile * LANES, LANES), out_len + LANES)]
    wide = jnp.dot(chosen, window, preferred_element_type=jnp.float32)
    lane = lax.broadcasted_iota(jnp.int32, (width, LANES), 1)
    parts = [
        pltpu.roll(wide[:, t * LANES : (t + 1) * LANES], shift, 1) for t in range(chunks + 1)
    ]
    for t in range(chunks):
        band[pl.ds(t, width, stride=chunks), :] = jnp.where(
            lane < LANES - rest, parts[t], parts[t + 1]
        )

    unroll = 32

    @pl.loop(0, width // unroll)
    def _(group):
        slots = [group * unroll + m for m in range(unroll)]
        places = [ids_ref[index * width + slot] for slot in slots]
        values = [
            band[pl.ds(pl.multiple_of(slot * chunks, chunks), chunks), :] for slot in slots
        ]
        for place, value in zip(places, values):
            rows[pl.ds(pl.multiple_of(place * chunks, chunks), chunks), :] = value


def halves_kernel(
    lags_ref, ids_ref, mine_ref, arrived_ref, weights_ref, kept_ref, sent_ref, sources, band, rows
):
    scatter_bands(lags_ref, ids_ref, arrived_ref, weights_ref, sources, band, rows)
    pairs, height, out_len = kept_ref.shape
    chunks = out_len // LANES
    mine = mine_ref[0]

    @pl.when(pl.program_id(0) == pl.num_programs(0) - 1)
    def _():
        for pair in range(pairs):
            for t in range(chunks):
                lanes = slice(t * LANES, (t + 1) * LANES)
                for out, owner in ((kept_ref, 2 * pair + mine), (sent_ref, 2 * pair + 1 - mine)):
                    first = pl.multiple_of(owner * (height * chunks), height * chunks)
                    part = rows[pl.ds(first + t, height, stride=chunks), :]
                    out[pair, :, lanes] = part.astype(out.dtype)


def banded_call(kernel, outs, arrived, kernel_weights, band_observers, band_lags, mine):
    taps, terms, observers, faces = kernel_weights.shape
    bands, width = band_observers.shape
    steps = arrived.shape[-1]
    chunks = steps // 2 // LANES
    rank = len(arrived.shape)
    return pl.pallas_call(
        kernel,
        out_shape=outs,
        grid_spec=pltpu.PrefetchScalarGridSpec(
            num_scalar_prefetch=3,
            grid=(bands,),
            in_specs=[
                pl.BlockSpec(arrived.shape, lambda b, *_: (0,) * rank),
                pl.BlockSpec((taps, terms, width, faces), lambda b, *_: (0, 0, b, 0)),
            ],
            out_specs=jax.tree.map(
                lambda o: pl.BlockSpec(o.shape, lambda b, *_: (0,) * len(o.shape)), outs
            ),
            scratch_shapes=[
                pltpu.VMEM((taps * terms * faces, steps), jnp.bfloat16),
                pltpu.VMEM((width * chunks, LANES), jnp.float32),
                pltpu.VMEM((observers * chunks, LANES), jnp.float32),
            ],
        ),
        compiler_params=pltpu.CompilerParams(dimension_semantics=("arbitrary",)),
        name="bands",
    )(band_lags, band_observers.reshape(-1), mine, arrived, kernel_weights)


def halve(total, axis, bit):
    size = lax.axis_size(axis)
    mine = (lax.axis_index(axis) >> bit) & 1
    if axis == "cfd":
        owners, rows, times = total.shape
        pairs = total.reshape(owners // 2, 2, rows, times)
        first, second = pairs[:, 0], pairs[:, 1]
    else:
        first, second = jnp.split(total, 2, axis=2)
    kept = jnp.where(mine == 1, second, first)
    sent = jnp.where(mine == 1, first, second).astype(jnp.bfloat16)
    partners = [(i, i ^ (1 << bit)) for i in range(size)]
    return kept + lax.ppermute(sent, axis, partners).astype(jnp.float32)


def exchange_sums(kept, sent):
    owners = lax.axis_size("cfd")
    near = [("cfd", b) for b in range(owners.bit_length() - 1)]
    across = [("ac", b) for b in reversed(range(lax.axis_size("ac").bit_length() - 1))]
    orders = (near[:2] + across + near[2:], near[:1] + across + near[1:])
    partners = [(i, i ^ 1) for i in range(owners)]
    total = kept + lax.ppermute(sent, "cfd", partners).astype(jnp.float32)
    streams = jnp.split(total, len(orders), axis=1)
    for step in range(1, len(near) + len(across)):
        streams = [halve(part, *order[step]) for part, order in zip(streams, orders)]
    return jnp.concatenate([part[0] for part in streams], axis=0)


def flip(place, mask):
    out = place
    for bit in range(mask.bit_length()):
        if mask >> bit & 1:
            out = out + (1 << bit) * (1 - 2 * lax.rem(lax.div(place, 1 << bit), 2))
    return out


def fused_kernel(
    lags_ref,
    map_ref,
    ids_ref,
    normals_ref,
    surface_ref,
    weights_ref,
    first_ref,
    second_ref,
    lags,
    block_at,
    ids_here,
    flat_normals,
    surface,
    weights,
    normals,
    outgoing,
    arrived,
    sources,
    before,
    wide,
    spread,
    found,
    inverse,
    slots,
    rows,
    core_out,
    core_in,
    x_out,
    x_in,
    x_kept,
    y_out,
    y_in,
    y_kept,
    xy_out,
    xy_in,
    z_out,
    z_in,
    load_sems,
    block_send,
    block_recv,
    core_send,
    core_recv,
    first_send,
    first_recv,
    second_send,
    second_recv,
    z_send,
    z_recv,
):
    me = lax.axis_index("cfd")
    owners, pieces = outgoing.shape[:2]
    span = outgoing.shape[-1]
    zs = owners // 4
    core, x, z = lax.rem(me, 2), lax.rem(lax.div(me, 2), 2), lax.div(me, 4)
    y = lax.axis_index("ac")
    taps, terms, observers, faces = weights.shape
    bands, width = ids_here.shape
    size, steps = surface.shape[2:]
    out_len = steps // 2
    chunks = out_len // LANES
    height = observers // owners
    half = chunks // 2
    near = owners // zs

    get_surface = pltpu.make_async_copy(surface_ref, surface, load_sems.at[0])
    get_weights = pltpu.make_async_copy(weights_ref, weights, load_sems.at[1])
    get_surface.start()
    small = [
        pltpu.make_async_copy(src, dst, load_sems.at[3 + n])
        for n, (src, dst) in enumerate(
            (
                (normals_ref, flat_normals),
                (map_ref, block_at),
                (ids_ref, ids_here),
                (lags_ref, lags),
            )
        )
    ]
    for copy in small:
        copy.start()

    def remote(src, dst, send, recv, **peer):
        return pltpu.make_async_remote_copy(
            src_ref=src, dst_ref=dst, send_sem=send, recv_sem=recv,
            device_id=peer, device_id_type=pl.DeviceIdType.MESH,
        )

    barrier = pltpu.get_barrier_semaphore()
    for k in range(1, owners):
        pl.semaphore_signal(
            barrier, inc=1, device_id={"cfd": flip(me, k)}, device_id_type=pl.DeviceIdType.MESH
        )
    pl.semaphore_signal(barrier, inc=1, device_id={"ac": 1 - y}, device_id_type=pl.DeviceIdType.MESH)

    for copy in small:
        copy.wait()
    flat = flat_normals[...].astype(jnp.float32)
    tall = jnp.concatenate([flat, jnp.zeros((LANES - flat.shape[0], faces), jnp.float32)], axis=0)
    normals[...] = tall.T.reshape(owners, size, LANES)
    get_surface.wait()
    get_weights.start()

    def wait_all(ref, sem):
        pltpu.make_async_copy(ref, ref, sem).wait()

    def thick_block(place):
        along = surface[2, place].astype(jnp.float32) * normals[place, :, 0:1]
        along = along + surface[3, place].astype(jnp.float32) * normals[place, :, 1:2]
        along = along + surface[4, place].astype(jnp.float32) * normals[place, :, 2:3]
        return (surface[1, place].astype(jnp.float32) * along).astype(jnp.bfloat16)

    def cut(value, c):
        return value[:, c * span : (c + 1) * span]

    order = sorted(range(1, owners), key=lambda k: send_order(k, near))
    for k in order:
        place = block_at[flip(me, k)]
        thick, pressure = thick_block(place), surface[0, place]
        for c in range(pieces):
            outgoing[k, c, 0], outgoing[k, c, 1] = cut(thick, c), cut(pressure, c)
    place = block_at[me]
    thick, pressure = thick_block(place), surface[0, place]
    for c in range(pieces):
        arrived[c, me, 0], arrived[c, me, 1] = cut(thick, c), cut(pressure, c)
    pl.semaphore_wait(barrier, owners)
    for c in range(pieces):
        for k in order:
            remote(
                outgoing.at[k, c],
                arrived.at[c, me],
                block_send.at[0],
                block_recv.at[c],
                cfd=flip(me, k),
            ).start()

    ids = ids_here[...]
    down = jnp.concatenate([ids, jnp.zeros((LANES - bands, width), jnp.int32)], axis=0).T
    for b in range(bands):
        spread[b] = jnp.broadcast_to(down[:, b : b + 1], (width, LANES))
    lane = lax.broadcasted_iota(jnp.int32, (width, LANES), 1)
    slot = lax.broadcasted_iota(jnp.int32, (width, LANES), 0)

    @pl.loop(0, observers // LANES)
    def _(part):
        def add(b, total):
            hit = spread[b] == lane + part * LANES
            return jnp.where(hit, slot + b * width, total)

        total = lax.fori_loop(0, bands, add, jnp.zeros((width, LANES), jnp.int32))
        found[pl.ds(part, 1), :] = jnp.max(total, axis=0, keepdims=True)

    get_inverse = pltpu.make_async_copy(found, inverse, load_sems.at[2])
    get_inverse.start()

    start_lane = lax.broadcasted_iota(jnp.int32, (faces, LANES), 1) == 0
    bands_each = 8
    rows_each = bands_each * width

    def source_tile(c, u):
        tile = c * (span // LANES) + u
        lanes = slice(u * LANES, (u + 1) * LANES)

        def late(value, place):
            turned = pltpu.roll(value, 1, 1)
            moved = jnp.where(start_lane, before[place], turned) if tile else turned
            before[place] = turned
            return moved

        for n in range(2):
            value = arrived[c, :, n, :, lanes].astype(jnp.float32).reshape(faces, LANES)
            last = late(value, 2 * n)
            rate = value - last
            if tile == 0:
                rate = jnp.where(start_lane, 0.0, rate)
            rate = rate.astype(jnp.bfloat16).astype(jnp.float32)
            taken = [(n, rate, late(rate, 2 * n + 1))]
            if n == 1:
                taken.append((2, value, last))
            for term, now, then in taken:
                for k, series in enumerate((now, then)):
                    here = pl.ds((k * terms + term) * faces, faces)
                    sources[here, lanes] = series.astype(jnp.bfloat16)

    def shift_band(b, first, last):
        start = out_len - lags[b]
        tile = jnp.minimum(lax.div(start, LANES), steps // LANES - chunks - 1)
        rest = start - tile * LANES
        shift = lax.rem(LANES - rest, LANES)
        early = lane[:8] >= rest
        for top in range(0, width, 8):
            tiles = [wide[tile + t, b, top : top + 8] for t in range(first, last + 1)]
            for t in range(first, last):
                here = pl.ds(b * (width * chunks) + top * chunks + t, 8, stride=chunks)
                mixed = jnp.where(early, tiles[t - first], tiles[t - first + 1])
                slots[here, :] = pltpu.roll(mixed, shift, 1)

    for c in range(pieces):
        wait_all(arrived.at[c, pl.ds(0, owners - 1)], block_recv.at[c])
        for u in range(span // LANES):
            source_tile(c, u)
        if c == 0:
            get_weights.wait()

        @pl.loop(0, observers // rows_each)
        def _(part):
            if c == pieces - 1:
                for m in range(bands_each):
                    shift_band(part * bands_each + m, 0, half)
            here = pl.ds(pl.multiple_of(part * rows_each, rows_each), rows_each)
            chosen = jnp.concatenate(
                [weights[k, t, here, :] for k in range(taps) for t in range(terms)], axis=1
            )
            product = jnp.dot(chosen, sources[...], preferred_element_type=jnp.float32)
            for u in range(span // LANES):
                wide[c * (span // LANES) + u, pl.ds(part * bands_each, bands_each)] = product[
                    :, u * LANES : (u + 1) * LANES
                ].reshape(bands_each, width, LANES)

    @pl.loop(0, bands // 4)
    def _(group):
        for m in range(4):
            shift_band(group * 4 + m, half, chunks)

    get_inverse.wait()
    unroll = 32

    def gather(top, side):
        @pl.loop(0, 2)
        def _(other):
            owner = top + other * 2 + side
            base = pl.multiple_of(owner * (height * chunks), height * chunks)
            for first in range(0, height, unroll):
                places = [inverse[owner, first + m] for m in range(unroll)]
                values = [slots.reshape(observers, chunks, LANES)[place] for place in places]
                for m, value in enumerate(values):
                    rows[pl.ds(base + (first + m) * chunks, chunks), :] = value

    def unit(owner, t):
        return rows[pl.ds(owner * (height * chunks) + t, height, stride=chunks), :]

    def narrow(value):
        return value.astype(jnp.bfloat16)

    def wide_of(value):
        return value.astype(jnp.float32)

    core_copies, x_copies, y_copies, xy_copies, yx_copies = {}, {}, {}, {}, {}

    def send_core(j):
        top = flip(z, j) * near
        gather(top, 1 - core)
        for other in range(2):
            for t in range(chunks):
                core_out[j, other, t] = narrow(unit(top + other * 2 + 1 - core, t))
        core_copies[j] = remote(
            core_out.at[j], core_in.at[j], core_send.at[0], core_recv.at[j], cfd=flip(me, 1)
        )
        core_copies[j].start()
        gather(top, core)

    def send_first(j):
        top = flip(z, j) * near
        core_copies[j].wait_recv()

        def total(other, t):
            return unit(top + other * 2 + core, t) + wide_of(core_in[j, other, t])

        for n, (side, other) in enumerate(((1 - y, 1 - x), (y, x))):
            x_out[j, side] = narrow(total(1 - x, side * half))
            x_copies[j, n] = remote(
                x_out.at[j, side],
                x_in.at[j, side],
                first_send.at[0],
                first_recv.at[0, n, j],
                cfd=flip(me, 2),
            )
            x_copies[j, n].start()
            y_out[j, other] = narrow(total(other, (1 - y) * half + 1))
            y_copies[j, n] = remote(
                y_out.at[j, other],
                y_in.at[j, other],
                first_send.at[1],
                first_recv.at[1, n, j],
                ac=1 - y,
            )
            y_copies[j, n].start()
        for side in range(2):
            x_kept[j, side] = total(x, side * half)
        for other in range(2):
            y_kept[j, other] = total(other, y * half + 1)

    def send_second(j):
        x_copies[j, 0].wait_recv()
        xy_out[0, j] = narrow(x_kept[j, 1 - y] + wide_of(x_in[j, 1 - y]))
        xy_copies[j] = remote(
            xy_out.at[0, j], xy_in.at[0, j], second_send.at[0], second_recv.at[0, j], ac=1 - y
        )
        xy_copies[j].start()
        y_copies[j, 0].wait_recv()
        xy_out[1, j] = narrow(y_kept[j, 1 - x] + wide_of(y_in[j, 1 - x]))
        yx_copies[j] = remote(
            xy_out.at[1, j],
            xy_in.at[1, j],
            second_send.at[0],
            second_recv.at[1, j],
            cfd=flip(me, 2),
        )
        yx_copies[j].start()

    def finish_second(j):
        x_copies[j, 1].wait_recv()
        xy_copies[j].wait_recv()
        from_x = x_kept[j, y] + wide_of(x_in[j, y]) + wide_of(xy_in[0, j])
        y_copies[j, 1].wait_recv()
        yx_copies[j].wait_recv()
        from_y = y_kept[j, x] + wide_of(y_in[j, x]) + wide_of(xy_in[1, j])
        return from_x, from_y

    def send_z(j, peer, passed, sems):
        for stream, value in enumerate(finish_second(j)):
            if passed:
                z_wait(passed, stream)
                value = value + wide_of(z_in[passed, stream])
            z_out[j, stream] = narrow(value)
            remote(
                z_out.at[j, stream],
                z_in.at[j, stream],
                z_send.at[0],
                z_recv.at[sems[stream]],
                cfd=flip(me, near * peer),
            ).start()

    def z_wait(j, stream):
        wait_all(z_in.at[j, stream], z_recv.at[1 + stream])

    send_core(3)
    send_core(2)
    send_first(3)
    send_core(1)
    send_first(2)
    send_core(0)
    send_second(3)
    send_first(1)
    send_second(2)
    send_first(0)
    send_z(3, 1, 0, (1, 2))
    send_second(1)
    send_z(2, 2, 3, (0, 0))
    send_second(0)
    send_z(1, 1, 0, (0, 0))
    results = list(finish_second(0))
    wait_all(outgoing.at[pl.ds(1, owners - 1)], block_send.at[0])
    wait_all(core_out, core_send.at[0])
    wait_all(x_out, first_send.at[0])
    wait_all(y_out, first_send.at[1])
    wait_all(xy_out, second_send.at[0])
    wait_all(z_out.at[pl.ds(1, zs - 1)], z_send.at[0])
    wait_all(z_in.at[pl.ds(1, 2)], z_recv.at[0])
    for j in (1, 2):
        results = [value + wide_of(z_in[j, s]) for s, value in enumerate(results)]
    for value, result_ref in zip(results, (first_ref, second_ref)):
        result_ref[...] = value


def send_order(k, near):
    j = k // near
    return (0, 3, 1, 2)[j] if j < 4 else j, k


def fused(surface_raw, area_normals, kernel_weights, block_map, band_observers, band_lags):
    owners, halves = lax.axis_size("cfd"), lax.axis_size("ac")
    faces, steps = surface_raw.shape[1:]
    taps, terms, observers, _ = kernel_weights.shape
    bands, width = band_observers.shape
    size, height = faces // owners, observers // owners
    chunks = steps // 2 // LANES
    zs = owners // 4
    near = owners // zs
    bf16, f32, i32 = jnp.bfloat16, jnp.float32, jnp.int32
    tile = (height, LANES)
    dma = pltpu.SemaphoreType.DMA
    vmem, hbm = (pl.BlockSpec(memory_space=space) for space in (pltpu.VMEM, pltpu.HBM))
    pieces = 4
    span = steps // pieces
    first, second = pl.pallas_call(
        fused_kernel,
        out_shape=[jax.ShapeDtypeStruct(tile, f32)] * 2,
        in_specs=[hbm] * 6,
        out_specs=[vmem, vmem],
        scratch_shapes=[
            pltpu.SMEM((bands,), i32),
            pltpu.SMEM((owners,), i32),
            pltpu.VMEM((bands, width), i32),
            pltpu.VMEM(area_normals.shape, bf16),
            pltpu.VMEM((surface_raw.shape[0], owners, size, steps), bf16),
            pltpu.VMEM(kernel_weights.shape, bf16),
            pltpu.VMEM((owners, size, LANES), f32),
            pltpu.VMEM((owners, pieces, 2, size, span), bf16),
            pltpu.VMEM((pieces, owners, 2, size, span), bf16),
            pltpu.VMEM((taps * terms * faces, span), bf16),
            pltpu.VMEM((4,) + tile, f32),
            pltpu.VMEM((steps // LANES, bands, width, LANES), f32),
            pltpu.VMEM((bands, width, LANES), i32),
            pltpu.VMEM((observers // LANES, LANES), i32),
            pltpu.SMEM((observers // LANES, LANES), i32),
            pltpu.VMEM((observers * chunks, LANES), f32),
            pltpu.VMEM((observers * chunks, LANES), f32),
            pltpu.VMEM((zs, 2, chunks) + tile, bf16),
            pltpu.VMEM((zs, 2, chunks) + tile, bf16),
            pltpu.VMEM((zs, 2) + tile, bf16),
            pltpu.VMEM((zs, 2) + tile, bf16),
            pltpu.VMEM((zs, 2) + tile, f32),
            pltpu.VMEM((zs, 2) + tile, bf16),
            pltpu.VMEM((zs, 2) + tile, bf16),
            pltpu.VMEM((zs, 2) + tile, f32),
            pltpu.VMEM((2, zs) + tile, bf16),
            pltpu.VMEM((2, zs) + tile, bf16),
            pltpu.VMEM((zs, 2) + tile, bf16),
            pltpu.VMEM((zs, 2) + tile, bf16),
            dma((7,)),
            dma((1,)),
            dma((pieces,)),
            dma((1,)),
            dma((zs,)),
            dma((2,)),
            dma((2, 2, zs)),
            dma((1,)),
            dma((2, zs)),
            dma((1,)),
            dma((3,)),
        ],
        compiler_params=pltpu.CompilerParams(
            collective_id=0, has_side_effects=True, vmem_limit_bytes=40 * 2**20
        ),
        name="fused",
    )(
        *(
            pltpu.with_memory_space_constraint(value, pltpu.HBM)
            for value in (
                band_lags,
                block_map[0, 0],
                band_observers,
                area_normals,
                surface_raw.reshape(surface_raw.shape[0], owners, size, steps),
                kernel_weights,
            )
        )
    )
    return jnp.concatenate([first, second], axis=1)


def fits_fused(owners, halves, surface_raw, kernel_weights, band_observers):
    faces, steps = surface_raw.shape[1:]
    tiles = halves * 2
    return (
        halves == 2
        and owners == 4 * 4
        and faces == LANES
        and band_observers.shape[1] == LANES
        and faces // owners % 8 == 0
        and steps == 2 * tiles * LANES
        and kernel_weights.shape[:1] + kernel_weights.shape[2:3] == (2, owners * LANES)
        and band_observers.shape[0] % 8 == 0
    )


def general(surface_raw, area_normals, kernel_weights, block_map, band_observers, band_lags):
    blocks = lax.axis_size("cfd")
    faces, steps = surface_raw.shape[1:]
    size = faces // blocks
    outgoing = prepare(surface_raw, area_normals, block_map[0, 0])
    arrived = lax.all_to_all(outgoing, "cfd", split_axis=0, concat_axis=0, tiled=True)
    arrived = arrived.reshape(blocks, 2, size, steps)
    if size % 8:
        arrived = arrived.transpose(1, 0, 2, 3).reshape(2 * faces, steps)
    shape = (blocks // 2, kernel_weights.shape[2] // blocks, steps // 2)
    kept, sent = banded_call(
        halves_kernel,
        [jax.ShapeDtypeStruct(shape, kind) for kind in (jnp.float32, jnp.bfloat16)],
        arrived,
        kernel_weights,
        band_observers,
        band_lags,
        (lax.axis_index("cfd") & 1).astype(jnp.int32).reshape(1),
    )
    return exchange_sums(kept, sent)


def local(surface_raw, area_normals, kernel_weights, block_map, band_observers, band_lags):
    owners, halves = lax.axis_size("cfd"), lax.axis_size("ac")
    fast = fits_fused(owners, halves, surface_raw, kernel_weights, band_observers)
    run = fused if fast else general
    return run(surface_raw, area_normals, kernel_weights, block_map, band_observers, band_lags)


def solution(mesh):
    placed = (
        P(None, ("cfd", "ac"), None),
        P(None, ("cfd", "ac")),
        P(None, None, None, ("cfd", "ac")),
        P("ac", "cfd", None),
        P(),
        P(),
    )
    return jax.shard_map(
        local, mesh=mesh, in_specs=placed, out_specs=P("cfd", "ac"), check_vma=False
    )
```

```python
import functools

import jax
import jax.numpy as jnp
from jax import lax
from jax.experimental import pallas as pl
from jax.experimental.pallas import tpu as pltpu
from jax.sharding import PartitionSpec as P

LANES = 128


def prepare_kernel(src_ref, normals_ref, surface_ref, out_ref):
    along = surface_ref[2].astype(jnp.float32) * normals_ref[:, 0:1]
    along = along + surface_ref[3].astype(jnp.float32) * normals_ref[:, 1:2]
    along = along + surface_ref[4].astype(jnp.float32) * normals_ref[:, 2:3]
    thick = (surface_ref[1].astype(jnp.float32) * along).astype(jnp.bfloat16)
    both = jnp.concatenate([thick, surface_ref[0]], axis=0)
    rows = both.shape[0]
    column = lax.broadcasted_iota(jnp.int32, (rows, rows), 1)
    onehot = jnp.where(column == src_ref[...], 1.0, 0.0).astype(jnp.bfloat16)
    picked = jnp.dot(onehot, both, preferred_element_type=jnp.float32)
    out_ref[...] = picked.astype(jnp.bfloat16)


def prepare(surface_raw, area_normals, block_order):
    faces, steps = surface_raw.shape[1:]
    blocks = block_order.shape[0]
    size = faces // blocks
    src = (
        jnp.arange(2, dtype=jnp.int32)[None, :, None] * faces
        + block_order[:, None, None] * size
        + jnp.arange(size, dtype=jnp.int32)[None, None, :]
    ).reshape(2 * faces, 1)
    return pl.pallas_call(
        prepare_kernel,
        out_shape=jax.ShapeDtypeStruct((2 * faces, steps), jnp.bfloat16),
        name="prepare",
    )(src, area_normals.T.astype(jnp.float32), surface_raw)


def scatter_bands(lags_ref, ids_ref, arrived_ref, weights_ref, sources, band, rows):
    index = pl.program_id(0)
    taps, terms, width, faces = weights_ref.shape
    steps = sources.shape[1]
    out_len = steps // 2
    chunks = out_len // LANES

    @pl.when(index == 0)
    def _():
        series = arrived_ref[...].astype(jnp.float32)
        if len(arrived_ref.shape) == 4:
            thick = series[:, 0].reshape(faces, steps)
            pressure = series[:, 1].reshape(faces, steps)
        else:
            thick, pressure = series[:faces], series[faces:]
        step = lax.broadcasted_iota(jnp.int32, (faces, steps), 1)

        def rate(x):
            moved = jnp.where(step > 0, x - pltpu.roll(x, 1, 1), 0.0)
            return moved.astype(jnp.bfloat16).astype(jnp.float32)

        for c, x in enumerate((rate(thick), rate(pressure), pressure)):
            for k in range(taps):
                late = pltpu.roll(x, k, 1) if k else x
                sources[pl.ds((k * terms + c) * faces, faces), :] = late.astype(jnp.bfloat16)

    start = out_len - lags_ref[index]
    tile = jnp.minimum(start // LANES, steps // LANES - chunks - 1)
    rest = start - tile * LANES
    shift = lax.rem(LANES - rest, LANES)
    chosen = jnp.concatenate(
        [weights_ref[k, c] for k in range(taps) for c in range(terms)], axis=1
    )
    window = sources[:, pl.ds(pl.multiple_of(tile * LANES, LANES), out_len + LANES)]
    wide = jnp.dot(chosen, window, preferred_element_type=jnp.float32)
    lane = lax.broadcasted_iota(jnp.int32, (width, LANES), 1)
    parts = [
        pltpu.roll(wide[:, t * LANES : (t + 1) * LANES], shift, 1) for t in range(chunks + 1)
    ]
    for t in range(chunks):
        band[pl.ds(t, width, stride=chunks), :] = jnp.where(
            lane < LANES - rest, parts[t], parts[t + 1]
        )

    unroll = 32

    @pl.loop(0, width // unroll)
    def _(group):
        slots = [group * unroll + m for m in range(unroll)]
        places = [ids_ref[index * width + slot] for slot in slots]
        values = [
            band[pl.ds(pl.multiple_of(slot * chunks, chunks), chunks), :] for slot in slots
        ]
        for place, value in zip(places, values):
            rows[pl.ds(pl.multiple_of(place * chunks, chunks), chunks), :] = value


def halves_kernel(
    lags_ref, ids_ref, mine_ref, arrived_ref, weights_ref, kept_ref, sent_ref, sources, band, rows
):
    scatter_bands(lags_ref, ids_ref, arrived_ref, weights_ref, sources, band, rows)
    pairs, height, out_len = kept_ref.shape
    chunks = out_len // LANES
    mine = mine_ref[0]

    @pl.when(pl.program_id(0) == pl.num_programs(0) - 1)
    def _():
        for pair in range(pairs):
            for t in range(chunks):
                lanes = slice(t * LANES, (t + 1) * LANES)
                for out, owner in ((kept_ref, 2 * pair + mine), (sent_ref, 2 * pair + 1 - mine)):
                    first = pl.multiple_of(owner * (height * chunks), height * chunks)
                    part = rows[pl.ds(first + t, height, stride=chunks), :]
                    out[pair, :, lanes] = part.astype(out.dtype)


def banded_call(kernel, outs, arrived, kernel_weights, band_observers, band_lags, mine):
    taps, terms, observers, faces = kernel_weights.shape
    bands, width = band_observers.shape
    steps = arrived.shape[-1]
    chunks = steps // 2 // LANES
    rank = len(arrived.shape)
    return pl.pallas_call(
        kernel,
        out_shape=outs,
        grid_spec=pltpu.PrefetchScalarGridSpec(
            num_scalar_prefetch=3,
            grid=(bands,),
            in_specs=[
                pl.BlockSpec(arrived.shape, lambda b, *_: (0,) * rank),
                pl.BlockSpec((taps, terms, width, faces), lambda b, *_: (0, 0, b, 0)),
            ],
            out_specs=jax.tree.map(
                lambda o: pl.BlockSpec(o.shape, lambda b, *_: (0,) * len(o.shape)), outs
            ),
            scratch_shapes=[
                pltpu.VMEM((taps * terms * faces, steps), jnp.bfloat16),
                pltpu.VMEM((width * chunks, LANES), jnp.float32),
                pltpu.VMEM((observers * chunks, LANES), jnp.float32),
            ],
        ),
        compiler_params=pltpu.CompilerParams(dimension_semantics=("arbitrary",)),
        name="bands",
    )(band_lags, band_observers.reshape(-1), mine, arrived, kernel_weights)


def halve(total, axis, bit):
    size = lax.axis_size(axis)
    mine = (lax.axis_index(axis) >> bit) & 1
    if axis == "cfd":
        owners, rows, times = total.shape
        pairs = total.reshape(owners // 2, 2, rows, times)
        first, second = pairs[:, 0], pairs[:, 1]
    else:
        first, second = jnp.split(total, 2, axis=2)
    kept = jnp.where(mine == 1, second, first)
    sent = jnp.where(mine == 1, first, second).astype(jnp.bfloat16)
    partners = [(i, i ^ (1 << bit)) for i in range(size)]
    return kept + lax.ppermute(sent, axis, partners).astype(jnp.float32)


def exchange_sums(kept, sent):
    owners = lax.axis_size("cfd")
    near = [("cfd", b) for b in range(owners.bit_length() - 1)]
    across = [("ac", b) for b in reversed(range(lax.axis_size("ac").bit_length() - 1))]
    orders = (near[:2] + across + near[2:], near[:1] + across + near[1:])
    partners = [(i, i ^ 1) for i in range(owners)]
    total = kept + lax.ppermute(sent, "cfd", partners).astype(jnp.float32)
    streams = jnp.split(total, len(orders), axis=1)
    for step in range(1, len(near) + len(across)):
        streams = [halve(part, *order[step]) for part, order in zip(streams, orders)]
    return jnp.concatenate([part[0] for part in streams], axis=0)


def flip(place, mask):
    out = place
    for bit in range(mask.bit_length()):
        if mask >> bit & 1:
            out = out + (1 << bit) * (1 - 2 * lax.rem(lax.div(place, 1 << bit), 2))
    return out


def fused_kernel(
    lags_ref,
    map_ref,
    ids_ref,
    normals_ref,
    surface_ref,
    weights_ref,
    first_ref,
    second_ref,
    lags,
    block_at,
    ids_here,
    flat_normals,
    surface,
    weights,
    normals,
    outgoing,
    arrived,
    sources,
    before,
    wide,
    spread,
    found,
    inverse,
    slots,
    rows,
    core_out,
    core_in,
    x_out,
    x_in,
    x_kept,
    y_out,
    y_in,
    y_kept,
    xy_out,
    xy_in,
    z_out,
    z_in,
    load_sems,
    block_send,
    block_recv,
    core_send,
    core_recv,
    first_send,
    first_recv,
    second_send,
    second_recv,
    z_send,
    z_recv,
):
    me = lax.axis_index("cfd")
    owners, pieces = outgoing.shape[:2]
    span = outgoing.shape[-1]
    zs = owners // 4
    core, x, z = lax.rem(me, 2), lax.rem(lax.div(me, 2), 2), lax.div(me, 4)
    y = lax.axis_index("ac")
    taps, terms, observers, faces = weights.shape
    bands, width = ids_here.shape
    size, steps = surface_ref.shape[2:]
    out_len = steps // 2
    chunks = out_len // LANES
    height = observers // owners
    half = chunks // 2
    near = owners // zs

    barrier = pltpu.get_barrier_semaphore()
    for k in range(owners - 1, 0, -1):
        pl.semaphore_signal(
            barrier, inc=1, device_id={"cfd": flip(me, k)}, device_id_type=pl.DeviceIdType.MESH
        )
    pl.semaphore_signal(barrier, inc=1, device_id={"ac": 1 - y}, device_id_type=pl.DeviceIdType.MESH)

    get_surface = [
        pltpu.make_async_copy(
            surface_ref.at[:, :, :, pl.ds(c * span, span)], surface[c], load_sems.at[7 + c]
        )
        for c in range(pieces)
    ]
    get_weights = pltpu.make_async_copy(weights_ref, weights, load_sems.at[1])
    small = [
        pltpu.make_async_copy(src, dst, load_sems.at[3 + n])
        for n, (src, dst) in enumerate(
            (
                (normals_ref, flat_normals),
                (map_ref, block_at),
                (ids_ref, ids_here),
                (lags_ref, lags),
            )
        )
    ]
    get_surface[0].start()
    for copy in small + get_surface[1:]:
        copy.start()

    def remote(src, dst, send, recv, **peer):
        return pltpu.make_async_remote_copy(
            src_ref=src, dst_ref=dst, send_sem=send, recv_sem=recv,
            device_id=peer, device_id_type=pl.DeviceIdType.MESH,
        )

    for copy in small:
        copy.wait()
    flat = flat_normals[...].astype(jnp.float32)
    tall = jnp.concatenate([flat, jnp.zeros((LANES - flat.shape[0], faces), jnp.float32)], axis=0)
    normals[...] = tall.T.reshape(owners, size, LANES)

    def wait_all(ref, sem):
        pltpu.make_async_copy(ref, ref, sem).wait()

    def blocks(c, place):
        along = surface[c][2, place].astype(jnp.float32) * normals[place, :, 0:1]
        along = along + surface[c][3, place].astype(jnp.float32) * normals[place, :, 1:2]
        along = along + surface[c][4, place].astype(jnp.float32) * normals[place, :, 2:3]
        thick = (surface[c][1, place].astype(jnp.float32) * along).astype(jnp.bfloat16)
        return thick, surface[c][0, place]

    order = sorted(range(1, owners), key=lambda k: send_order(k, near))
    for c in range(pieces):
        get_surface[c].wait()
        for k in order:
            outgoing[k, c, 0], outgoing[k, c, 1] = blocks(c, block_at[flip(me, k)])
        if c == 0:
            pl.semaphore_wait(barrier, owners)
        for k in order:
            remote(
                outgoing.at[k, c],
                arrived.at[c, me],
                block_send.at[0],
                block_recv.at[c],
                cfd=flip(me, k),
            ).start()
        arrived[c, me, 0], arrived[c, me, 1] = blocks(c, block_at[me])
    get_weights.start()

    ids = ids_here[...]
    down = jnp.concatenate([ids, jnp.zeros((LANES - bands, width), jnp.int32)], axis=0).T
    for b in range(bands):
        spread[b] = jnp.broadcast_to(down[:, b : b + 1], (width, LANES))
    lane = lax.broadcasted_iota(jnp.int32, (width, LANES), 1)
    slot = lax.broadcasted_iota(jnp.int32, (width, LANES), 0)

    @pl.loop(0, observers // LANES)
    def _(part):
        def add(b, total):
            hit = spread[b] == lane + part * LANES
            return jnp.where(hit, slot + b * width, total)

        total = lax.fori_loop(0, bands, add, jnp.zeros((width, LANES), jnp.int32))
        found[pl.ds(part, 1), :] = jnp.max(total, axis=0, keepdims=True)

    get_inverse = pltpu.make_async_copy(found, inverse, load_sems.at[2])
    get_inverse.start()

    start_lane = lax.broadcasted_iota(jnp.int32, (faces, LANES), 1) == 0
    bands_each = 8
    rows_each = bands_each * width

    def source_tile(c, u):
        tile = c * (span // LANES) + u
        lanes = slice(u * LANES, (u + 1) * LANES)

        def late(value, place):
            turned = pltpu.roll(value, 1, 1)
            moved = jnp.where(start_lane, before[place], turned) if tile else turned
            before[place] = turned
            return moved

        for n in range(2):
            value = arrived[c, :, n, :, lanes].astype(jnp.float32).reshape(faces, LANES)
            last = late(value, 2 * n)
            rate = value - last
            if tile == 0:
                rate = jnp.where(start_lane, 0.0, rate)
            rate = rate.astype(jnp.bfloat16).astype(jnp.float32)
            taken = [(n, rate, late(rate, 2 * n + 1))]
            if n == 1:
                taken.append((2, value, last))
            for term, now, then in taken:
                for k, series in enumerate((now, then)):
                    here = pl.ds((k * terms + term) * faces, faces)
                    sources[here, lanes] = series.astype(jnp.bfloat16)

    def shift_band(b, first, last):
        start = out_len - lags[b]
        tile = jnp.minimum(lax.div(start, LANES), steps // LANES - chunks - 1)
        rest = start - tile * LANES
        shift = lax.rem(LANES - rest, LANES)
        early = lane[:8] >= rest
        for top in range(0, width, 8):
            tiles = [wide[tile + t, b, top : top + 8] for t in range(first, last + 1)]
            for t in range(first, last):
                here = pl.ds(b * (width * chunks) + top * chunks + t, 8, stride=chunks)
                mixed = jnp.where(early, tiles[t - first], tiles[t - first + 1])
                slots[here, :] = pltpu.roll(mixed, shift, 1)

    for c in range(pieces):
        wait_all(arrived.at[c, pl.ds(0, owners - 1)], block_recv.at[c])
        for u in range(span // LANES):
            source_tile(c, u)
        if c == 0:
            get_weights.wait()

        @pl.loop(0, observers // rows_each)
        def _(part):
            if c == pieces - 1:
                for m in range(bands_each):
                    shift_band(part * bands_each + m, 0, half)
            here = pl.ds(pl.multiple_of(part * rows_each, rows_each), rows_each)
            chosen = jnp.concatenate(
                [weights[k, t, here, :] for k in range(taps) for t in range(terms)], axis=1
            )
            product = jnp.dot(chosen, sources[...], preferred_element_type=jnp.float32)
            for u in range(span // LANES):
                wide[c * (span // LANES) + u, pl.ds(part * bands_each, bands_each)] = product[
                    :, u * LANES : (u + 1) * LANES
                ].reshape(bands_each, width, LANES)

    @pl.loop(0, bands // 4)
    def _(group):
        for m in range(4):
            shift_band(group * 4 + m, half, chunks)

    get_inverse.wait()
    unroll = 32

    def gather(top, side):
        @pl.loop(0, 2)
        def _(other):
            owner = top + other * 2 + side
            base = pl.multiple_of(owner * (height * chunks), height * chunks)
            for first in range(0, height, unroll):
                places = [inverse[owner, first + m] for m in range(unroll)]
                values = [slots.reshape(observers, chunks, LANES)[place] for place in places]
                for m, value in enumerate(values):
                    rows[pl.ds(base + (first + m) * chunks, chunks), :] = value

    def unit(owner, t):
        return rows[pl.ds(owner * (height * chunks) + t, height, stride=chunks), :]

    def narrow(value):
        return value.astype(jnp.bfloat16)

    def wide_of(value):
        return value.astype(jnp.float32)

    core_copies, x_copies, y_copies, xy_copies, yx_copies = {}, {}, {}, {}, {}

    def send_core(j):
        top = flip(z, j) * near
        gather(top, 1 - core)
        for other in range(2):
            for t in range(chunks):
                core_out[j, other, t] = narrow(unit(top + other * 2 + 1 - core, t))
        core_copies[j] = remote(
            core_out.at[j], core_in.at[j], core_send.at[0], core_recv.at[j], cfd=flip(me, 1)
        )
        core_copies[j].start()
        gather(top, core)

    def send_first(j):
        top = flip(z, j) * near
        core_copies[j].wait_recv()

        def total(other, t):
            return unit(top + other * 2 + core, t) + wide_of(core_in[j, other, t])

        for n, (side, other) in enumerate(((1 - y, 1 - x), (y, x))):
            x_out[j, side] = narrow(total(1 - x, side * half))
            x_copies[j, n] = remote(
                x_out.at[j, side],
                x_in.at[j, side],
                first_send.at[0],
                first_recv.at[0, n, j],
                cfd=flip(me, 2),
            )
            x_copies[j, n].start()
            y_out[j, other] = narrow(total(other, (1 - y) * half + 1))
            y_copies[j, n] = remote(
                y_out.at[j, other],
                y_in.at[j, other],
                first_send.at[1],
                first_recv.at[1, n, j],
                ac=1 - y,
            )
            y_copies[j, n].start()
        for side in range(2):
            x_kept[j, side] = total(x, side * half)
        for other in range(2):
            y_kept[j, other] = total(other, y * half + 1)

    def send_second(j):
        x_copies[j, 0].wait_recv()
        xy_out[0, j] = narrow(x_kept[j, 1 - y] + wide_of(x_in[j, 1 - y]))
        xy_copies[j] = remote(
            xy_out.at[0, j], xy_in.at[0, j], second_send.at[0], second_recv.at[0, j], ac=1 - y
        )
        xy_copies[j].start()
        y_copies[j, 0].wait_recv()
        xy_out[1, j] = narrow(y_kept[j, 1 - x] + wide_of(y_in[j, 1 - x]))
        yx_copies[j] = remote(
            xy_out.at[1, j],
            xy_in.at[1, j],
            second_send.at[0],
            second_recv.at[1, j],
            cfd=flip(me, 2),
        )
        yx_copies[j].start()

    def finish_second(j):
        x_copies[j, 1].wait_recv()
        xy_copies[j].wait_recv()
        from_x = x_kept[j, y] + wide_of(x_in[j, y]) + wide_of(xy_in[0, j])
        y_copies[j, 1].wait_recv()
        yx_copies[j].wait_recv()
        from_y = y_kept[j, x] + wide_of(y_in[j, x]) + wide_of(xy_in[1, j])
        return from_x, from_y

    def send_z(j, peer, passed, sems):
        for stream, value in enumerate(finish_second(j)):
            if passed:
                z_wait(passed, stream)
                value = value + wide_of(z_in[passed, stream])
            z_out[j, stream] = narrow(value)
            remote(
                z_out.at[j, stream],
                z_in.at[j, stream],
                z_send.at[0],
                z_recv.at[sems[stream]],
                cfd=flip(me, near * peer),
            ).start()

    def z_wait(j, stream):
        wait_all(z_in.at[j, stream], z_recv.at[1 + stream])

    send_core(3)
    send_core(2)
    send_first(3)
    send_core(1)
    send_first(2)
    send_core(0)
    send_second(3)
    send_first(1)
    send_second(2)
    send_first(0)
    send_z(3, 1, 0, (1, 2))
    send_second(1)
    send_z(2, 2, 3, (0, 0))
    send_second(0)
    send_z(1, 1, 0, (0, 0))
    results = list(finish_second(0))
    wait_all(outgoing.at[pl.ds(1, owners - 1)], block_send.at[0])
    wait_all(core_out, core_send.at[0])
    wait_all(x_out, first_send.at[0])
    wait_all(y_out, first_send.at[1])
    wait_all(xy_out, second_send.at[0])
    wait_all(z_out.at[pl.ds(1, zs - 1)], z_send.at[0])
    wait_all(z_in.at[pl.ds(1, 2)], z_recv.at[0])
    for j in (1, 2):
        results = [value + wide_of(z_in[j, s]) for s, value in enumerate(results)]
    for value, result_ref in zip(results, (first_ref, second_ref)):
        result_ref[...] = value


def send_order(k, near):
    j = k // near
    return (0, 3, 1, 2)[j] if j < 4 else j, k


def fused(surface_raw, area_normals, kernel_weights, block_map, band_observers, band_lags):
    owners, halves = lax.axis_size("cfd"), lax.axis_size("ac")
    faces, steps = surface_raw.shape[1:]
    taps, terms, observers, _ = kernel_weights.shape
    bands, width = band_observers.shape
    size, height = faces // owners, observers // owners
    chunks = steps // 2 // LANES
    zs = owners // 4
    near = owners // zs
    bf16, f32, i32 = jnp.bfloat16, jnp.float32, jnp.int32
    tile = (height, LANES)
    dma = pltpu.SemaphoreType.DMA
    vmem, hbm = (pl.BlockSpec(memory_space=space) for space in (pltpu.VMEM, pltpu.HBM))
    pieces = 4
    span = steps // pieces
    first, second = pl.pallas_call(
        fused_kernel,
        out_shape=[jax.ShapeDtypeStruct(tile, f32)] * 2,
        in_specs=[hbm] * 6,
        out_specs=[vmem, vmem],
        scratch_shapes=[
            pltpu.SMEM((bands,), i32),
            pltpu.SMEM((owners,), i32),
            pltpu.VMEM((bands, width), i32),
            pltpu.VMEM(area_normals.shape, bf16),
            [pltpu.VMEM((surface_raw.shape[0], owners, size, span), bf16)] * pieces,
            pltpu.VMEM(kernel_weights.shape, bf16),
            pltpu.VMEM((owners, size, LANES), f32),
            pltpu.VMEM((owners, pieces, 2, size, span), bf16),
            pltpu.VMEM((pieces, owners, 2, size, span), bf16),
            pltpu.VMEM((taps * terms * faces, span), bf16),
            pltpu.VMEM((4,) + tile, f32),
            pltpu.VMEM((steps // LANES, bands, width, LANES), f32),
            pltpu.VMEM((bands, width, LANES), i32),
            pltpu.VMEM((observers // LANES, LANES), i32),
            pltpu.SMEM((observers // LANES, LANES), i32),
            pltpu.VMEM((observers * chunks, LANES), f32),
            pltpu.VMEM((observers * chunks, LANES), f32),
            pltpu.VMEM((zs, 2, chunks) + tile, bf16),
            pltpu.VMEM((zs, 2, chunks) + tile, bf16),
            pltpu.VMEM((zs, 2) + tile, bf16),
            pltpu.VMEM((zs, 2) + tile, bf16),
            pltpu.VMEM((zs, 2) + tile, f32),
            pltpu.VMEM((zs, 2) + tile, bf16),
            pltpu.VMEM((zs, 2) + tile, bf16),
            pltpu.VMEM((zs, 2) + tile, f32),
            pltpu.VMEM((2, zs) + tile, bf16),
            pltpu.VMEM((2, zs) + tile, bf16),
            pltpu.VMEM((zs, 2) + tile, bf16),
            pltpu.VMEM((zs, 2) + tile, bf16),
            dma((7 + pieces,)),
            dma((1,)),
            dma((pieces,)),
            dma((1,)),
            dma((zs,)),
            dma((2,)),
            dma((2, 2, zs)),
            dma((1,)),
            dma((2, zs)),
            dma((1,)),
            dma((3,)),
        ],
        compiler_params=pltpu.CompilerParams(
            collective_id=0, has_side_effects=True, vmem_limit_bytes=40 * 2**20
        ),
        name="fused",
    )(
        *(
            pltpu.with_memory_space_constraint(value, pltpu.HBM)
            for value in (
                band_lags,
                block_map[0, 0],
                band_observers,
                area_normals,
                surface_raw.reshape(surface_raw.shape[0], owners, size, steps),
                kernel_weights,
            )
        )
    )
    return jnp.concatenate([first, second], axis=1)


def fits_fused(owners, halves, surface_raw, kernel_weights, band_observers):
    faces, steps = surface_raw.shape[1:]
    tiles = halves * 2
    return (
        halves == 2
        and owners == 4 * 4
        and faces == LANES
        and band_observers.shape[1] == LANES
        and faces // owners % 8 == 0
        and steps == 2 * tiles * LANES
        and kernel_weights.shape[:1] + kernel_weights.shape[2:3] == (2, owners * LANES)
        and band_observers.shape[0] % 8 == 0
    )


def general(surface_raw, area_normals, kernel_weights, block_map, band_observers, band_lags):
    blocks = lax.axis_size("cfd")
    faces, steps = surface_raw.shape[1:]
    size = faces // blocks
    outgoing = prepare(surface_raw, area_normals, block_map[0, 0])
    arrived = lax.all_to_all(outgoing, "cfd", split_axis=0, concat_axis=0, tiled=True)
    arrived = arrived.reshape(blocks, 2, size, steps)
    if size % 8:
        arrived = arrived.transpose(1, 0, 2, 3).reshape(2 * faces, steps)
    shape = (blocks // 2, kernel_weights.shape[2] // blocks, steps // 2)
    kept, sent = banded_call(
        halves_kernel,
        [jax.ShapeDtypeStruct(shape, kind) for kind in (jnp.float32, jnp.bfloat16)],
        arrived,
        kernel_weights,
        band_observers,
        band_lags,
        (lax.axis_index("cfd") & 1).astype(jnp.int32).reshape(1),
    )
    return exchange_sums(kept, sent)


def local(surface_raw, area_normals, kernel_weights, block_map, band_observers, band_lags):
    owners, halves = lax.axis_size("cfd"), lax.axis_size("ac")
    fast = fits_fused(owners, halves, surface_raw, kernel_weights, band_observers)
    run = fused if fast else general
    return run(surface_raw, area_normals, kernel_weights, block_map, band_observers, band_lags)


def solution(mesh):
    placed = (
        P(None, ("cfd", "ac"), None),
        P(None, ("cfd", "ac")),
        P(None, None, None, ("cfd", "ac")),
        P("ac", "cfd", None),
        P(),
        P(),
    )
    return jax.shard_map(
        local, mesh=mesh, in_specs=placed, out_specs=P("cfd", "ac"), check_vma=False
    )
```

```python
import functools

import jax
import jax.numpy as jnp
from jax import lax
from jax.experimental import pallas as pl
from jax.experimental.pallas import tpu as pltpu
from jax.sharding import PartitionSpec as P

LANES = 128


def prepare_kernel(src_ref, normals_ref, surface_ref, out_ref):
    along = surface_ref[2].astype(jnp.float32) * normals_ref[:, 0:1]
    along = along + surface_ref[3].astype(jnp.float32) * normals_ref[:, 1:2]
    along = along + surface_ref[4].astype(jnp.float32) * normals_ref[:, 2:3]
    thick = (surface_ref[1].astype(jnp.float32) * along).astype(jnp.bfloat16)
    both = jnp.concatenate([thick, surface_ref[0]], axis=0)
    rows = both.shape[0]
    column = lax.broadcasted_iota(jnp.int32, (rows, rows), 1)
    onehot = jnp.where(column == src_ref[...], 1.0, 0.0).astype(jnp.bfloat16)
    picked = jnp.dot(onehot, both, preferred_element_type=jnp.float32)
    out_ref[...] = picked.astype(jnp.bfloat16)


def prepare(surface_raw, area_normals, block_order):
    faces, steps = surface_raw.shape[1:]
    blocks = block_order.shape[0]
    size = faces // blocks
    src = (
        jnp.arange(2, dtype=jnp.int32)[None, :, None] * faces
        + block_order[:, None, None] * size
        + jnp.arange(size, dtype=jnp.int32)[None, None, :]
    ).reshape(2 * faces, 1)
    return pl.pallas_call(
        prepare_kernel,
        out_shape=jax.ShapeDtypeStruct((2 * faces, steps), jnp.bfloat16),
        name="prepare",
    )(src, area_normals.T.astype(jnp.float32), surface_raw)


def scatter_bands(lags_ref, ids_ref, arrived_ref, weights_ref, sources, band, rows):
    index = pl.program_id(0)
    taps, terms, width, faces = weights_ref.shape
    steps = sources.shape[1]
    out_len = steps // 2
    chunks = out_len // LANES

    @pl.when(index == 0)
    def _():
        series = arrived_ref[...].astype(jnp.float32)
        if len(arrived_ref.shape) == 4:
            thick = series[:, 0].reshape(faces, steps)
            pressure = series[:, 1].reshape(faces, steps)
        else:
            thick, pressure = series[:faces], series[faces:]
        step = lax.broadcasted_iota(jnp.int32, (faces, steps), 1)

        def rate(x):
            moved = jnp.where(step > 0, x - pltpu.roll(x, 1, 1), 0.0)
            return moved.astype(jnp.bfloat16).astype(jnp.float32)

        for c, x in enumerate((rate(thick), rate(pressure), pressure)):
            for k in range(taps):
                late = pltpu.roll(x, k, 1) if k else x
                sources[pl.ds((k * terms + c) * faces, faces), :] = late.astype(jnp.bfloat16)

    start = out_len - lags_ref[index]
    tile = jnp.minimum(start // LANES, steps // LANES - chunks - 1)
    rest = start - tile * LANES
    shift = lax.rem(LANES - rest, LANES)
    chosen = jnp.concatenate(
        [weights_ref[k, c] for k in range(taps) for c in range(terms)], axis=1
    )
    window = sources[:, pl.ds(pl.multiple_of(tile * LANES, LANES), out_len + LANES)]
    wide = jnp.dot(chosen, window, preferred_element_type=jnp.float32)
    lane = lax.broadcasted_iota(jnp.int32, (width, LANES), 1)
    parts = [
        pltpu.roll(wide[:, t * LANES : (t + 1) * LANES], shift, 1) for t in range(chunks + 1)
    ]
    for t in range(chunks):
        band[pl.ds(t, width, stride=chunks), :] = jnp.where(
            lane < LANES - rest, parts[t], parts[t + 1]
        )

    unroll = 64

    @pl.loop(0, width // unroll)
    def _(group):
        slots = [group * unroll + m for m in range(unroll)]
        places = [ids_ref[index * width + slot] for slot in slots]
        values = [
            band[pl.ds(pl.multiple_of(slot * chunks, chunks), chunks), :] for slot in slots
        ]
        for place, value in zip(places, values):
            rows[pl.ds(pl.multiple_of(place * chunks, chunks), chunks), :] = value


def halves_kernel(
    lags_ref, ids_ref, mine_ref, arrived_ref, weights_ref, kept_ref, sent_ref, sources, band, rows
):
    scatter_bands(lags_ref, ids_ref, arrived_ref, weights_ref, sources, band, rows)
    pairs, height, out_len = kept_ref.shape
    chunks = out_len // LANES
    mine = mine_ref[0]

    @pl.when(pl.program_id(0) == pl.num_programs(0) - 1)
    def _():
        for pair in range(pairs):
            for t in range(chunks):
                lanes = slice(t * LANES, (t + 1) * LANES)
                for out, owner in ((kept_ref, 2 * pair + mine), (sent_ref, 2 * pair + 1 - mine)):
                    first = pl.multiple_of(owner * (height * chunks), height * chunks)
                    part = rows[pl.ds(first + t, height, stride=chunks), :]
                    out[pair, :, lanes] = part.astype(out.dtype)


def banded_call(kernel, outs, arrived, kernel_weights, band_observers, band_lags, mine):
    taps, terms, observers, faces = kernel_weights.shape
    bands, width = band_observers.shape
    steps = arrived.shape[-1]
    chunks = steps // 2 // LANES
    rank = len(arrived.shape)
    return pl.pallas_call(
        kernel,
        out_shape=outs,
        grid_spec=pltpu.PrefetchScalarGridSpec(
            num_scalar_prefetch=3,
            grid=(bands,),
            in_specs=[
                pl.BlockSpec(arrived.shape, lambda b, *_: (0,) * rank),
                pl.BlockSpec((taps, terms, width, faces), lambda b, *_: (0, 0, b, 0)),
            ],
            out_specs=jax.tree.map(
                lambda o: pl.BlockSpec(o.shape, lambda b, *_: (0,) * len(o.shape)), outs
            ),
            scratch_shapes=[
                pltpu.VMEM((taps * terms * faces, steps), jnp.bfloat16),
                pltpu.VMEM((width * chunks, LANES), jnp.float32),
                pltpu.VMEM((observers * chunks, LANES), jnp.float32),
            ],
        ),
        compiler_params=pltpu.CompilerParams(dimension_semantics=("arbitrary",)),
        name="bands",
    )(band_lags, band_observers.reshape(-1), mine, arrived, kernel_weights)


def halve(total, axis, bit):
    size = lax.axis_size(axis)
    mine = (lax.axis_index(axis) >> bit) & 1
    if axis == "cfd":
        owners, rows, times = total.shape
        pairs = total.reshape(owners // 2, 2, rows, times)
        first, second = pairs[:, 0], pairs[:, 1]
    else:
        first, second = jnp.split(total, 2, axis=2)
    kept = jnp.where(mine == 1, second, first)
    sent = jnp.where(mine == 1, first, second).astype(jnp.bfloat16)
    partners = [(i, i ^ (1 << bit)) for i in range(size)]
    return kept + lax.ppermute(sent, axis, partners).astype(jnp.float32)


def exchange_sums(kept, sent):
    owners = lax.axis_size("cfd")
    near = [("cfd", b) for b in range(owners.bit_length() - 1)]
    across = [("ac", b) for b in reversed(range(lax.axis_size("ac").bit_length() - 1))]
    orders = (near[:2] + across + near[2:], near[:1] + across + near[1:])
    partners = [(i, i ^ 1) for i in range(owners)]
    total = kept + lax.ppermute(sent, "cfd", partners).astype(jnp.float32)
    streams = jnp.split(total, len(orders), axis=1)
    for step in range(1, len(near) + len(across)):
        streams = [halve(part, *order[step]) for part, order in zip(streams, orders)]
    return jnp.concatenate([part[0] for part in streams], axis=0)


def flip(place, mask):
    out = place
    for bit in range(mask.bit_length()):
        if mask >> bit & 1:
            out = out + (1 << bit) * (1 - 2 * lax.rem(lax.div(place, 1 << bit), 2))
    return out


def fused_kernel(
    lags_ref,
    map_ref,
    ids_ref,
    normals_ref,
    surface_ref,
    weights_ref,
    first_ref,
    second_ref,
    lags,
    block_at,
    ids_here,
    flat_normals,
    surface,
    weights,
    normals,
    outgoing,
    arrived,
    sources,
    before,
    wide,
    spread,
    found,
    inverse,
    slots,
    rows,
    core_out,
    core_in,
    x_out,
    x_in,
    x_kept,
    y_out,
    y_in,
    y_kept,
    xy_out,
    xy_in,
    z_out,
    z_in,
    load_sems,
    block_send,
    block_recv,
    core_send,
    core_recv,
    first_send,
    first_recv,
    second_send,
    second_recv,
    z_send,
    z_recv,
):
    me = lax.axis_index("cfd")
    owners, pieces = outgoing.shape[:2]
    span = outgoing.shape[-1]
    zs = owners // 4
    core, x, z = lax.rem(me, 2), lax.rem(lax.div(me, 2), 2), lax.div(me, 4)
    y = lax.axis_index("ac")
    taps, terms, observers, faces = weights.shape
    bands, width = ids_here.shape
    size, steps = surface_ref.shape[2:]
    out_len = steps // 2
    chunks = out_len // LANES
    height = observers // owners
    half = chunks // 2
    near = owners // zs

    barrier = pltpu.get_barrier_semaphore()
    for k in range(owners - 1, 0, -1):
        pl.semaphore_signal(
            barrier, inc=1, device_id={"cfd": flip(me, k)}, device_id_type=pl.DeviceIdType.MESH
        )
    pl.semaphore_signal(barrier, inc=1, device_id={"ac": 1 - y}, device_id_type=pl.DeviceIdType.MESH)

    get_surface = [
        pltpu.make_async_copy(
            surface_ref.at[:, :, :, pl.ds(c * span, span)], surface[c], load_sems.at[7 + c]
        )
        for c in range(pieces)
    ]
    get_weights = pltpu.make_async_copy(weights_ref, weights, load_sems.at[1])
    small = [
        pltpu.make_async_copy(src, dst, load_sems.at[3 + n])
        for n, (src, dst) in enumerate(
            (
                (normals_ref, flat_normals),
                (map_ref, block_at),
                (ids_ref, ids_here),
                (lags_ref, lags),
            )
        )
    ]
    get_surface[0].start()
    for copy in small + get_surface[1:]:
        copy.start()

    def remote(src, dst, send, recv, **peer):
        return pltpu.make_async_remote_copy(
            src_ref=src, dst_ref=dst, send_sem=send, recv_sem=recv,
            device_id=peer, device_id_type=pl.DeviceIdType.MESH,
        )

    for copy in small:
        copy.wait()
    flat = flat_normals[...].astype(jnp.float32)
    tall = jnp.concatenate([flat, jnp.zeros((LANES - flat.shape[0], faces), jnp.float32)], axis=0)
    normals[...] = tall.T.reshape(owners, size, LANES)

    def wait_all(ref, sem):
        pltpu.make_async_copy(ref, ref, sem).wait()

    def blocks(c, place):
        along = surface[c][2, place].astype(jnp.float32) * normals[place, :, 0:1]
        along = along + surface[c][3, place].astype(jnp.float32) * normals[place, :, 1:2]
        along = along + surface[c][4, place].astype(jnp.float32) * normals[place, :, 2:3]
        thick = (surface[c][1, place].astype(jnp.float32) * along).astype(jnp.bfloat16)
        return thick, surface[c][0, place]

    order = sorted(range(1, owners), key=lambda k: send_order(k, near))
    for c in range(pieces):
        get_surface[c].wait()
        for k in order:
            outgoing[k, c, 0], outgoing[k, c, 1] = blocks(c, block_at[flip(me, k)])
        if c == 0:
            pl.semaphore_wait(barrier, owners)
        for k in order:
            remote(
                outgoing.at[k, c],
                arrived.at[c, me],
                block_send.at[0],
                block_recv.at[c],
                cfd=flip(me, k),
            ).start()
        arrived[c, me, 0], arrived[c, me, 1] = blocks(c, block_at[me])
    get_weights.start()

    ids = ids_here[...]
    down = jnp.concatenate([ids, jnp.zeros((LANES - bands, width), jnp.int32)], axis=0).T
    for b in range(bands):
        spread[b] = jnp.broadcast_to(down[:, b : b + 1], (width, LANES))
    lane = lax.broadcasted_iota(jnp.int32, (width, LANES), 1)
    slot = lax.broadcasted_iota(jnp.int32, (width, LANES), 0)

    @pl.loop(0, observers // LANES)
    def _(part):
        def add(b, total):
            hit = spread[b] == lane + part * LANES
            return jnp.where(hit, slot + b * width, total)

        total = lax.fori_loop(0, bands, add, jnp.zeros((width, LANES), jnp.int32))
        found[pl.ds(part, 1), :] = jnp.max(total, axis=0, keepdims=True)

    get_inverse = pltpu.make_async_copy(found, inverse, load_sems.at[2])
    get_inverse.start()

    start_lane = lax.broadcasted_iota(jnp.int32, (faces, LANES), 1) == 0
    bands_each = 8
    rows_each = bands_each * width

    def source_tile(c, u):
        tile = c * (span // LANES) + u
        lanes = slice(u * LANES, (u + 1) * LANES)

        def late(value, place):
            turned = pltpu.roll(value, 1, 1)
            moved = jnp.where(start_lane, before[place], turned) if tile else turned
            before[place] = turned
            return moved

        for n in range(2):
            value = arrived[c, :, n, :, lanes].astype(jnp.float32).reshape(faces, LANES)
            last = late(value, 2 * n)
            rate = value - last
            if tile == 0:
                rate = jnp.where(start_lane, 0.0, rate)
            rate = rate.astype(jnp.bfloat16).astype(jnp.float32)
            taken = [(n, rate, late(rate, 2 * n + 1))]
            if n == 1:
                taken.append((2, value, last))
            for term, now, then in taken:
                for k, series in enumerate((now, then)):
                    here = pl.ds((k * terms + term) * faces, faces)
                    sources[here, lanes] = series.astype(jnp.bfloat16)

    def shift_band(b, first, last):
        start = out_len - lags[b]
        tile = jnp.minimum(lax.div(start, LANES), steps // LANES - chunks - 1)
        rest = start - tile * LANES
        shift = lax.rem(LANES - rest, LANES)
        early = lane[:8] >= rest
        for top in range(0, width, 8):
            tiles = [wide[tile + t, b, top : top + 8] for t in range(first, last + 1)]
            for t in range(first, last):
                here = pl.ds(b * (width * chunks) + top * chunks + t, 8, stride=chunks)
                mixed = jnp.where(early, tiles[t - first], tiles[t - first + 1])
                slots[here, :] = pltpu.roll(mixed, shift, 1)

    for c in range(pieces):
        wait_all(arrived.at[c, pl.ds(0, owners - 1)], block_recv.at[c])
        for u in range(span // LANES):
            source_tile(c, u)
        if c == 0:
            get_weights.wait()

        @pl.loop(0, observers // rows_each)
        def _(part):
            if c == pieces - 1:
                for m in range(bands_each):
                    shift_band(part * bands_each + m, 0, half)
            here = pl.ds(pl.multiple_of(part * rows_each, rows_each), rows_each)
            chosen = jnp.concatenate(
                [weights[k, t, here, :] for k in range(taps) for t in range(terms)], axis=1
            )
            product = jnp.dot(chosen, sources[...], preferred_element_type=jnp.float32)
            for u in range(span // LANES):
                wide[c * (span // LANES) + u, pl.ds(part * bands_each, bands_each)] = product[
                    :, u * LANES : (u + 1) * LANES
                ].reshape(bands_each, width, LANES)

    @pl.loop(0, bands // 8)
    def _(group):
        for m in range(8):
            shift_band(group * 8 + m, half, chunks)

    get_inverse.wait()
    unroll = 64

    def gather(top, side):
        @pl.loop(0, 2)
        def _(other):
            owner = top + other * 2 + side
            base = pl.multiple_of(owner * (height * chunks), height * chunks)
            for first in range(0, height, unroll):
                places = [inverse[owner, first + m] for m in range(unroll)]
                values = [slots.reshape(observers, chunks, LANES)[place] for place in places]
                for m, value in enumerate(values):
                    rows[pl.ds(base + (first + m) * chunks, chunks), :] = value

    def unit(owner, t):
        return rows[pl.ds(owner * (height * chunks) + t, height, stride=chunks), :]

    def narrow(value):
        return value.astype(jnp.bfloat16)

    def wide_of(value):
        return value.astype(jnp.float32)

    core_copies, x_copies, y_copies, xy_copies, yx_copies = {}, {}, {}, {}, {}

    def send_core(j):
        top = flip(z, j) * near
        gather(top, 1 - core)
        for other in range(2):
            for t in range(chunks):
                core_out[j, other, t] = narrow(unit(top + other * 2 + 1 - core, t))
        core_copies[j] = remote(
            core_out.at[j], core_in.at[j], core_send.at[0], core_recv.at[j], cfd=flip(me, 1)
        )
        core_copies[j].start()
        gather(top, core)

    def send_first(j):
        top = flip(z, j) * near
        core_copies[j].wait_recv()

        def total(other, t):
            return unit(top + other * 2 + core, t) + wide_of(core_in[j, other, t])

        for n, (side, other) in enumerate(((1 - y, 1 - x), (y, x))):
            x_out[j, side] = narrow(total(1 - x, side * half))
            x_copies[j, n] = remote(
                x_out.at[j, side],
                x_in.at[j, side],
                first_send.at[0],
                first_recv.at[0, n, j],
                cfd=flip(me, 2),
            )
            x_copies[j, n].start()
            y_out[j, other] = narrow(total(other, (1 - y) * half + 1))
            y_copies[j, n] = remote(
                y_out.at[j, other],
                y_in.at[j, other],
                first_send.at[1],
                first_recv.at[1, n, j],
                ac=1 - y,
            )
            y_copies[j, n].start()
        for side in range(2):
            x_kept[j, side] = total(x, side * half)
        for other in range(2):
            y_kept[j, other] = total(other, y * half + 1)

    def send_second(j):
        x_copies[j, 0].wait_recv()
        xy_out[0, j] = narrow(x_kept[j, 1 - y] + wide_of(x_in[j, 1 - y]))
        xy_copies[j] = remote(
            xy_out.at[0, j], xy_in.at[0, j], second_send.at[0], second_recv.at[0, j], ac=1 - y
        )
        xy_copies[j].start()
        y_copies[j, 0].wait_recv()
        xy_out[1, j] = narrow(y_kept[j, 1 - x] + wide_of(y_in[j, 1 - x]))
        yx_copies[j] = remote(
            xy_out.at[1, j],
            xy_in.at[1, j],
            second_send.at[0],
            second_recv.at[1, j],
            cfd=flip(me, 2),
        )
        yx_copies[j].start()

    def finish_second(j):
        x_copies[j, 1].wait_recv()
        xy_copies[j].wait_recv()
        from_x = x_kept[j, y] + wide_of(x_in[j, y]) + wide_of(xy_in[0, j])
        y_copies[j, 1].wait_recv()
        yx_copies[j].wait_recv()
        from_y = y_kept[j, x] + wide_of(y_in[j, x]) + wide_of(xy_in[1, j])
        return from_x, from_y

    def send_z(j, peer, passed, sems):
        for stream, value in enumerate(finish_second(j)):
            if passed:
                z_wait(passed, stream)
                value = value + wide_of(z_in[passed, stream])
            z_out[j, stream] = narrow(value)
            remote(
                z_out.at[j, stream],
                z_in.at[j, stream],
                z_send.at[0],
                z_recv.at[sems[stream]],
                cfd=flip(me, near * peer),
            ).start()

    def z_wait(j, stream):
        wait_all(z_in.at[j, stream], z_recv.at[1 + stream])

    send_core(3)
    send_core(2)
    send_first(3)
    send_core(1)
    send_first(2)
    send_core(0)
    send_second(3)
    send_first(1)
    send_second(2)
    send_first(0)
    send_z(3, 1, 0, (1, 2))
    send_second(1)
    send_z(2, 2, 3, (0, 0))
    send_second(0)
    send_z(1, 1, 0, (0, 0))
    results = list(finish_second(0))
    wait_all(outgoing.at[pl.ds(1, owners - 1)], block_send.at[0])
    wait_all(core_out, core_send.at[0])
    wait_all(x_out, first_send.at[0])
    wait_all(y_out, first_send.at[1])
    wait_all(xy_out, second_send.at[0])
    wait_all(z_out.at[pl.ds(1, zs - 1)], z_send.at[0])
    wait_all(z_in.at[pl.ds(1, 2)], z_recv.at[0])
    for j in (1, 2):
        results = [value + wide_of(z_in[j, s]) for s, value in enumerate(results)]
    for value, result_ref in zip(results, (first_ref, second_ref)):
        result_ref[...] = value


def send_order(k, near):
    j = k // near
    return (0, 3, 1, 2)[j] if j < 4 else j, k


def fused(surface_raw, area_normals, kernel_weights, block_map, band_observers, band_lags):
    owners, halves = lax.axis_size("cfd"), lax.axis_size("ac")
    faces, steps = surface_raw.shape[1:]
    taps, terms, observers, _ = kernel_weights.shape
    bands, width = band_observers.shape
    size, height = faces // owners, observers // owners
    chunks = steps // 2 // LANES
    zs = owners // 4
    near = owners // zs
    bf16, f32, i32 = jnp.bfloat16, jnp.float32, jnp.int32
    tile = (height, LANES)
    dma = pltpu.SemaphoreType.DMA
    vmem, hbm = (pl.BlockSpec(memory_space=space) for space in (pltpu.VMEM, pltpu.HBM))
    pieces = 4
    span = steps // pieces
    first, second = pl.pallas_call(
        fused_kernel,
        out_shape=[jax.ShapeDtypeStruct(tile, f32)] * 2,
        in_specs=[hbm] * 6,
        out_specs=[vmem, vmem],
        scratch_shapes=[
            pltpu.SMEM((bands,), i32),
            pltpu.SMEM((owners,), i32),
            pltpu.VMEM((bands, width), i32),
            pltpu.VMEM(area_normals.shape, bf16),
            [pltpu.VMEM((surface_raw.shape[0], owners, size, span), bf16)] * pieces,
            pltpu.VMEM(kernel_weights.shape, bf16),
            pltpu.VMEM((owners, size, LANES), f32),
            pltpu.VMEM((owners, pieces, 2, size, span), bf16),
            pltpu.VMEM((pieces, owners, 2, size, span), bf16),
            pltpu.VMEM((taps * terms * faces, span), bf16),
            pltpu.VMEM((4,) + tile, f32),
            pltpu.VMEM((steps // LANES, bands, width, LANES), f32),
            pltpu.VMEM((bands, width, LANES), i32),
            pltpu.VMEM((observers // LANES, LANES), i32),
            pltpu.SMEM((observers // LANES, LANES), i32),
            pltpu.VMEM((observers * chunks, LANES), f32),
            pltpu.VMEM((observers * chunks, LANES), f32),
            pltpu.VMEM((zs, 2, chunks) + tile, bf16),
            pltpu.VMEM((zs, 2, chunks) + tile, bf16),
            pltpu.VMEM((zs, 2) + tile, bf16),
            pltpu.VMEM((zs, 2) + tile, bf16),
            pltpu.VMEM((zs, 2) + tile, f32),
            pltpu.VMEM((zs, 2) + tile, bf16),
            pltpu.VMEM((zs, 2) + tile, bf16),
            pltpu.VMEM((zs, 2) + tile, f32),
            pltpu.VMEM((2, zs) + tile, bf16),
            pltpu.VMEM((2, zs) + tile, bf16),
            pltpu.VMEM((zs, 2) + tile, bf16),
            pltpu.VMEM((zs, 2) + tile, bf16),
            dma((7 + pieces,)),
            dma((1,)),
            dma((pieces,)),
            dma((1,)),
            dma((zs,)),
            dma((2,)),
            dma((2, 2, zs)),
            dma((1,)),
            dma((2, zs)),
            dma((1,)),
            dma((3,)),
        ],
        compiler_params=pltpu.CompilerParams(
            collective_id=0, has_side_effects=True, vmem_limit_bytes=40 * 2**20
        ),
        name="fused",
    )(
        *(
            pltpu.with_memory_space_constraint(value, pltpu.HBM)
            for value in (
                band_lags,
                block_map[0, 0],
                band_observers,
                area_normals,
                surface_raw.reshape(surface_raw.shape[0], owners, size, steps),
                kernel_weights,
            )
        )
    )
    return jnp.concatenate([first, second], axis=1)


def fits_fused(owners, halves, surface_raw, kernel_weights, band_observers):
    faces, steps = surface_raw.shape[1:]
    tiles = halves * 2
    return (
        halves == 2
        and owners == 4 * 4
        and faces == LANES
        and band_observers.shape[1] == LANES
        and faces // owners % 8 == 0
        and steps == 2 * tiles * LANES
        and kernel_weights.shape[:1] + kernel_weights.shape[2:3] == (2, owners * LANES)
        and band_observers.shape[0] % 8 == 0
    )


def general(surface_raw, area_normals, kernel_weights, block_map, band_observers, band_lags):
    blocks = lax.axis_size("cfd")
    faces, steps = surface_raw.shape[1:]
    size = faces // blocks
    outgoing = prepare(surface_raw, area_normals, block_map[0, 0])
    arrived = lax.all_to_all(outgoing, "cfd", split_axis=0, concat_axis=0, tiled=True)
    arrived = arrived.reshape(blocks, 2, size, steps)
    if size % 8:
        arrived = arrived.transpose(1, 0, 2, 3).reshape(2 * faces, steps)
    shape = (blocks // 2, kernel_weights.shape[2] // blocks, steps // 2)
    kept, sent = banded_call(
        halves_kernel,
        [jax.ShapeDtypeStruct(shape, kind) for kind in (jnp.float32, jnp.bfloat16)],
        arrived,
        kernel_weights,
        band_observers,
        band_lags,
        (lax.axis_index("cfd") & 1).astype(jnp.int32).reshape(1),
    )
    return exchange_sums(kept, sent)


def local(surface_raw, area_normals, kernel_weights, block_map, band_observers, band_lags):
    owners, halves = lax.axis_size("cfd"), lax.axis_size("ac")
    fast = fits_fused(owners, halves, surface_raw, kernel_weights, band_observers)
    run = fused if fast else general
    return run(surface_raw, area_normals, kernel_weights, block_map, band_observers, band_lags)


def solution(mesh):
    placed = (
        P(None, ("cfd", "ac"), None),
        P(None, ("cfd", "ac")),
        P(None, None, None, ("cfd", "ac")),
        P("ac", "cfd", None),
        P(),
        P(),
    )
    return jax.shard_map(
        local, mesh=mesh, in_specs=placed, out_specs=P("cfd", "ac"), check_vma=False
    )
```

```python
import functools

import jax
import jax.numpy as jnp
from jax import lax
from jax.experimental import pallas as pl
from jax.experimental.pallas import tpu as pltpu
from jax.sharding import PartitionSpec as P

LANES = 128


def prepare_kernel(src_ref, normals_ref, surface_ref, out_ref):
    along = surface_ref[2].astype(jnp.float32) * normals_ref[:, 0:1]
    along = along + surface_ref[3].astype(jnp.float32) * normals_ref[:, 1:2]
    along = along + surface_ref[4].astype(jnp.float32) * normals_ref[:, 2:3]
    thick = (surface_ref[1].astype(jnp.float32) * along).astype(jnp.bfloat16)
    both = jnp.concatenate([thick, surface_ref[0]], axis=0)
    rows = both.shape[0]
    column = lax.broadcasted_iota(jnp.int32, (rows, rows), 1)
    onehot = jnp.where(column == src_ref[...], 1.0, 0.0).astype(jnp.bfloat16)
    picked = jnp.dot(onehot, both, preferred_element_type=jnp.float32)
    out_ref[...] = picked.astype(jnp.bfloat16)


def prepare(surface_raw, area_normals, block_order):
    faces, steps = surface_raw.shape[1:]
    blocks = block_order.shape[0]
    size = faces // blocks
    src = (
        jnp.arange(2, dtype=jnp.int32)[None, :, None] * faces
        + block_order[:, None, None] * size
        + jnp.arange(size, dtype=jnp.int32)[None, None, :]
    ).reshape(2 * faces, 1)
    return pl.pallas_call(
        prepare_kernel,
        out_shape=jax.ShapeDtypeStruct((2 * faces, steps), jnp.bfloat16),
        name="prepare",
    )(src, area_normals.T.astype(jnp.float32), surface_raw)


def scatter_bands(lags_ref, ids_ref, arrived_ref, weights_ref, sources, band, rows):
    index = pl.program_id(0)
    taps, terms, width, faces = weights_ref.shape
    steps = sources.shape[1]
    out_len = steps // 2
    chunks = out_len // LANES

    @pl.when(index == 0)
    def _():
        series = arrived_ref[...].astype(jnp.float32)
        if len(arrived_ref.shape) == 4:
            thick = series[:, 0].reshape(faces, steps)
            pressure = series[:, 1].reshape(faces, steps)
        else:
            thick, pressure = series[:faces], series[faces:]
        step = lax.broadcasted_iota(jnp.int32, (faces, steps), 1)

        def rate(x):
            moved = jnp.where(step > 0, x - pltpu.roll(x, 1, 1), 0.0)
            return moved.astype(jnp.bfloat16).astype(jnp.float32)

        for c, x in enumerate((rate(thick), rate(pressure), pressure)):
            for k in range(taps):
                late = pltpu.roll(x, k, 1) if k else x
                sources[pl.ds((k * terms + c) * faces, faces), :] = late.astype(jnp.bfloat16)

    start = out_len - lags_ref[index]
    tile = jnp.minimum(start // LANES, steps // LANES - chunks - 1)
    rest = start - tile * LANES
    shift = lax.rem(LANES - rest, LANES)
    chosen = jnp.concatenate(
        [weights_ref[k, c] for k in range(taps) for c in range(terms)], axis=1
    )
    window = sources[:, pl.ds(pl.multiple_of(tile * LANES, LANES), out_len + LANES)]
    wide = jnp.dot(chosen, window, preferred_element_type=jnp.float32)
    lane = lax.broadcasted_iota(jnp.int32, (width, LANES), 1)
    parts = [
        pltpu.roll(wide[:, t * LANES : (t + 1) * LANES], shift, 1) for t in range(chunks + 1)
    ]
    for t in range(chunks):
        band[pl.ds(t, width, stride=chunks), :] = jnp.where(
            lane < LANES - rest, parts[t], parts[t + 1]
        )

    unroll = 64

    @pl.loop(0, width // unroll)
    def _(group):
        slots = [group * unroll + m for m in range(unroll)]
        places = [ids_ref[index * width + slot] for slot in slots]
        values = [
            band[pl.ds(pl.multiple_of(slot * chunks, chunks), chunks), :] for slot in slots
        ]
        for place, value in zip(places, values):
            rows[pl.ds(pl.multiple_of(place * chunks, chunks), chunks), :] = value


def halves_kernel(
    lags_ref, ids_ref, mine_ref, arrived_ref, weights_ref, kept_ref, sent_ref, sources, band, rows
):
    scatter_bands(lags_ref, ids_ref, arrived_ref, weights_ref, sources, band, rows)
    pairs, height, out_len = kept_ref.shape
    chunks = out_len // LANES
    mine = mine_ref[0]

    @pl.when(pl.program_id(0) == pl.num_programs(0) - 1)
    def _():
        for pair in range(pairs):
            for t in range(chunks):
                lanes = slice(t * LANES, (t + 1) * LANES)
                for out, owner in ((kept_ref, 2 * pair + mine), (sent_ref, 2 * pair + 1 - mine)):
                    first = pl.multiple_of(owner * (height * chunks), height * chunks)
                    part = rows[pl.ds(first + t, height, stride=chunks), :]
                    out[pair, :, lanes] = part.astype(out.dtype)


def banded_call(kernel, outs, arrived, kernel_weights, band_observers, band_lags, mine):
    taps, terms, observers, faces = kernel_weights.shape
    bands, width = band_observers.shape
    steps = arrived.shape[-1]
    chunks = steps // 2 // LANES
    rank = len(arrived.shape)
    return pl.pallas_call(
        kernel,
        out_shape=outs,
        grid_spec=pltpu.PrefetchScalarGridSpec(
            num_scalar_prefetch=3,
            grid=(bands,),
            in_specs=[
                pl.BlockSpec(arrived.shape, lambda b, *_: (0,) * rank),
                pl.BlockSpec((taps, terms, width, faces), lambda b, *_: (0, 0, b, 0)),
            ],
            out_specs=jax.tree.map(
                lambda o: pl.BlockSpec(o.shape, lambda b, *_: (0,) * len(o.shape)), outs
            ),
            scratch_shapes=[
                pltpu.VMEM((taps * terms * faces, steps), jnp.bfloat16),
                pltpu.VMEM((width * chunks, LANES), jnp.float32),
                pltpu.VMEM((observers * chunks, LANES), jnp.float32),
            ],
        ),
        compiler_params=pltpu.CompilerParams(dimension_semantics=("arbitrary",)),
        name="bands",
    )(band_lags, band_observers.reshape(-1), mine, arrived, kernel_weights)


def halve(total, axis, bit):
    size = lax.axis_size(axis)
    mine = (lax.axis_index(axis) >> bit) & 1
    if axis == "cfd":
        owners, rows, times = total.shape
        pairs = total.reshape(owners // 2, 2, rows, times)
        first, second = pairs[:, 0], pairs[:, 1]
    else:
        first, second = jnp.split(total, 2, axis=2)
    kept = jnp.where(mine == 1, second, first)
    sent = jnp.where(mine == 1, first, second).astype(jnp.bfloat16)
    partners = [(i, i ^ (1 << bit)) for i in range(size)]
    return kept + lax.ppermute(sent, axis, partners).astype(jnp.float32)


def exchange_sums(kept, sent):
    owners = lax.axis_size("cfd")
    near = [("cfd", b) for b in range(owners.bit_length() - 1)]
    across = [("ac", b) for b in reversed(range(lax.axis_size("ac").bit_length() - 1))]
    orders = (near[:2] + across + near[2:], near[:1] + across + near[1:])
    partners = [(i, i ^ 1) for i in range(owners)]
    total = kept + lax.ppermute(sent, "cfd", partners).astype(jnp.float32)
    streams = jnp.split(total, len(orders), axis=1)
    for step in range(1, len(near) + len(across)):
        streams = [halve(part, *order[step]) for part, order in zip(streams, orders)]
    return jnp.concatenate([part[0] for part in streams], axis=0)


def flip(place, mask):
    out = place
    for bit in range(mask.bit_length()):
        if mask >> bit & 1:
            out = out + (1 << bit) * (1 - 2 * lax.rem(lax.div(place, 1 << bit), 2))
    return out


def fused_kernel(
    lags_ref,
    map_ref,
    ids_ref,
    normals_ref,
    surface_ref,
    weights_ref,
    first_ref,
    second_ref,
    lags,
    block_at,
    ids_here,
    flat_normals,
    surface,
    weights,
    normals,
    outgoing,
    arrived,
    sources,
    before,
    wide,
    spread,
    found,
    inverse,
    slots,
    rows,
    core_out,
    core_in,
    x_out,
    x_in,
    x_kept,
    y_out,
    y_in,
    y_kept,
    xy_out,
    xy_in,
    z_out,
    z_in,
    load_sems,
    block_send,
    block_recv,
    core_send,
    core_recv,
    first_send,
    first_recv,
    second_send,
    second_recv,
    z_send,
    z_recv,
):
    me = lax.axis_index("cfd")
    owners, pieces = outgoing.shape[:2]
    span = outgoing.shape[-1]
    zs = owners // 4
    core, x, z = lax.rem(me, 2), lax.rem(lax.div(me, 2), 2), lax.div(me, 4)
    y = lax.axis_index("ac")
    taps, terms, observers, faces = weights.shape
    bands, width = ids_here.shape
    size, steps = surface_ref.shape[2:]
    out_len = steps // 2
    chunks = out_len // LANES
    height = observers // owners
    half = chunks // 2
    near = owners // zs

    barrier = pltpu.get_barrier_semaphore()
    for k in range(owners - 1, 0, -1):
        pl.semaphore_signal(
            barrier, inc=1, device_id={"cfd": flip(me, k)}, device_id_type=pl.DeviceIdType.MESH
        )
    pl.semaphore_signal(barrier, inc=1, device_id={"ac": 1 - y}, device_id_type=pl.DeviceIdType.MESH)

    get_surface = [
        pltpu.make_async_copy(
            surface_ref.at[:, :, :, pl.ds(c * span, span)], surface[c], load_sems.at[7 + c]
        )
        for c in range(pieces)
    ]
    get_weights = pltpu.make_async_copy(weights_ref, weights, load_sems.at[1])
    small = [
        pltpu.make_async_copy(src, dst, load_sems.at[3 + n])
        for n, (src, dst) in enumerate(
            (
                (normals_ref, flat_normals),
                (map_ref, block_at),
                (ids_ref, ids_here),
                (lags_ref, lags),
            )
        )
    ]
    get_surface[0].start()
    for copy in small + get_surface[1:]:
        copy.start()

    def remote(src, dst, send, recv, **peer):
        return pltpu.make_async_remote_copy(
            src_ref=src, dst_ref=dst, send_sem=send, recv_sem=recv,
            device_id=peer, device_id_type=pl.DeviceIdType.MESH,
        )

    for copy in small:
        copy.wait()
    flat = flat_normals[...].astype(jnp.float32)
    tall = jnp.concatenate([flat, jnp.zeros((LANES - flat.shape[0], faces), jnp.float32)], axis=0)
    normals[...] = tall.T.reshape(owners, size, LANES)

    def wait_all(ref, sem):
        pltpu.make_async_copy(ref, ref, sem).wait()

    def blocks(c, place):
        along = surface[c][2, place].astype(jnp.float32) * normals[place, :, 0:1]
        along = along + surface[c][3, place].astype(jnp.float32) * normals[place, :, 1:2]
        along = along + surface[c][4, place].astype(jnp.float32) * normals[place, :, 2:3]
        thick = (surface[c][1, place].astype(jnp.float32) * along).astype(jnp.bfloat16)
        return thick, surface[c][0, place]

    order = sorted(range(1, owners), key=lambda k: send_order(k, near))
    for c in range(pieces):
        get_surface[c].wait()
        for k in order:
            outgoing[k, c, 0], outgoing[k, c, 1] = blocks(c, block_at[flip(me, k)])
        if c == 0:
            pl.semaphore_wait(barrier, owners)
        for k in order:
            remote(
                outgoing.at[k, c],
                arrived.at[c, me],
                block_send.at[0],
                block_recv.at[c],
                cfd=flip(me, k),
            ).start()
        arrived[c, me, 0], arrived[c, me, 1] = blocks(c, block_at[me])
    get_weights.start()

    ids = ids_here[...]
    down = jnp.concatenate([ids, jnp.zeros((LANES - bands, width), jnp.int32)], axis=0).T
    for b in range(bands):
        spread[b] = jnp.broadcast_to(down[:, b : b + 1], (width, LANES))
    lane = lax.broadcasted_iota(jnp.int32, (width, LANES), 1)
    slot = lax.broadcasted_iota(jnp.int32, (width, LANES), 0)

    @pl.loop(0, observers // LANES)
    def _(part):
        def add(b, total):
            hit = spread[b] == lane + part * LANES
            return jnp.where(hit, slot + b * width, total)

        total = lax.fori_loop(0, bands, add, jnp.zeros((width, LANES), jnp.int32))
        found[pl.ds(part, 1), :] = jnp.max(total, axis=0, keepdims=True)

    get_inverse = pltpu.make_async_copy(found, inverse, load_sems.at[2])
    get_inverse.start()

    start_lane = lax.broadcasted_iota(jnp.int32, (faces, LANES), 1) == 0
    bands_each = 8
    rows_each = bands_each * width

    def source_tile(c, u):
        tile = c * (span // LANES) + u
        lanes = slice(u * LANES, (u + 1) * LANES)

        def late(value, place):
            turned = pltpu.roll(value, 1, 1)
            moved = jnp.where(start_lane, before[place], turned) if tile else turned
            before[place] = turned
            return moved

        for n in range(2):
            value = arrived[c, :, n, :, lanes].astype(jnp.float32).reshape(faces, LANES)
            last = late(value, 2 * n)
            rate = value - last
            if tile == 0:
                rate = jnp.where(start_lane, 0.0, rate)
            rate = rate.astype(jnp.bfloat16).astype(jnp.float32)
            taken = [(n, rate, late(rate, 2 * n + 1))]
            if n == 1:
                taken.append((2, value, last))
            for term, now, then in taken:
                for k, series in enumerate((now, then)):
                    here = pl.ds((k * terms + term) * faces, faces)
                    sources[here, lanes] = series.astype(jnp.bfloat16)

    def shift_band(b, first, last):
        start = out_len - lags[b]
        tile = jnp.minimum(lax.div(start, LANES), steps // LANES - chunks - 1)
        rest = start - tile * LANES
        shift = lax.rem(LANES - rest, LANES)
        early = lane[:8] >= rest
        for top in range(0, width, 8):
            tiles = [wide[tile + t, b, top : top + 8] for t in range(first, last + 1)]
            for t in range(first, last):
                here = pl.ds(b * (width * chunks) + top * chunks + t, 8, stride=chunks)
                mixed = jnp.where(early, tiles[t - first], tiles[t - first + 1])
                slots[here, :] = pltpu.roll(mixed, shift, 1)

    for c in range(pieces):
        wait_all(arrived.at[c, pl.ds(0, owners - 1)], block_recv.at[c])
        for u in range(span // LANES):
            source_tile(c, u)
        if c == 0:
            get_weights.wait()

        @pl.loop(0, observers // rows_each)
        def _(part):
            if c == pieces - 1:
                for m in range(bands_each):
                    shift_band(part * bands_each + m, 0, half)
            here = pl.ds(pl.multiple_of(part * rows_each, rows_each), rows_each)
            chosen = jnp.concatenate(
                [weights[k, t, here, :] for k in range(taps) for t in range(terms)], axis=1
            )
            product = jnp.dot(chosen, sources[...], preferred_element_type=jnp.float32)
            for u in range(span // LANES):
                wide[c * (span // LANES) + u, pl.ds(part * bands_each, bands_each)] = product[
                    :, u * LANES : (u + 1) * LANES
                ].reshape(bands_each, width, LANES)

    @pl.loop(0, bands // 8)
    def _(group):
        for m in range(8):
            shift_band(group * 8 + m, half, chunks)

    get_inverse.wait()
    unroll = 64

    def gather(top, side):
        @pl.loop(0, 2)
        def _(other):
            owner = top + other * 2 + side
            base = pl.multiple_of(owner * (height * chunks), height * chunks)
            for first in range(0, height, unroll):
                places = [inverse[owner, first + m] for m in range(unroll)]
                values = [slots.reshape(observers, chunks, LANES)[place] for place in places]
                for m, value in enumerate(values):
                    rows[pl.ds(base + (first + m) * chunks, chunks), :] = value

    def unit(owner, t):
        return rows[pl.ds(owner * (height * chunks) + t, height, stride=chunks), :]

    def narrow(value):
        return value.astype(jnp.bfloat16)

    def wide_of(value):
        return value.astype(jnp.float32)

    core_copies, x_copies, y_copies, xy_copies, yx_copies = {}, {}, {}, {}, {}

    def send_core(j):
        top = flip(z, j) * near
        gather(top, 1 - core)
        for other in range(2):
            for t in range(chunks):
                core_out[j, other, t] = narrow(unit(top + other * 2 + 1 - core, t))
        core_copies[j] = remote(
            core_out.at[j], core_in.at[j], core_send.at[0], core_recv.at[j], cfd=flip(me, 1)
        )
        core_copies[j].start()
        gather(top, core)

    def send_first(j):
        top = flip(z, j) * near
        core_copies[j].wait_recv()

        def total(other, t):
            return unit(top + other * 2 + core, t) + wide_of(core_in[j, other, t])

        for n, (side, other) in enumerate(((1 - y, 1 - x), (y, x))):
            x_out[j, side] = narrow(total(1 - x, side * half))
            x_copies[j, n] = remote(
                x_out.at[j, side],
                x_in.at[j, side],
                first_send.at[0],
                first_recv.at[0, n, j],
                cfd=flip(me, 2),
            )
            x_copies[j, n].start()
            y_out[j, other] = narrow(total(other, (1 - y) * half + 1))
            y_copies[j, n] = remote(
                y_out.at[j, other],
                y_in.at[j, other],
                first_send.at[1],
                first_recv.at[1, n, j],
                ac=1 - y,
            )
            y_copies[j, n].start()
        for side in range(2):
            x_kept[j, side] = total(x, side * half)
        for other in range(2):
            y_kept[j, other] = total(other, y * half + 1)

    def send_second(j):
        x_copies[j, 0].wait_recv()
        xy_out[0, j] = narrow(x_kept[j, 1 - y] + wide_of(x_in[j, 1 - y]))
        xy_copies[j] = remote(
            xy_out.at[0, j], xy_in.at[0, j], second_send.at[0], second_recv.at[0, j], ac=1 - y
        )
        xy_copies[j].start()
        y_copies[j, 0].wait_recv()
        xy_out[1, j] = narrow(y_kept[j, 1 - x] + wide_of(y_in[j, 1 - x]))
        yx_copies[j] = remote(
            xy_out.at[1, j],
            xy_in.at[1, j],
            second_send.at[0],
            second_recv.at[1, j],
            cfd=flip(me, 2),
        )
        yx_copies[j].start()

    def finish_second(j):
        x_copies[j, 1].wait_recv()
        xy_copies[j].wait_recv()
        from_x = x_kept[j, y] + wide_of(x_in[j, y]) + wide_of(xy_in[0, j])
        y_copies[j, 1].wait_recv()
        yx_copies[j].wait_recv()
        from_y = y_kept[j, x] + wide_of(y_in[j, x]) + wide_of(xy_in[1, j])
        return from_x, from_y

    def send_z(j, peer, passed, sems):
        for stream, value in enumerate(finish_second(j)):
            if passed:
                z_wait(passed, stream)
                value = value + wide_of(z_in[passed, stream])
            z_out[j, stream] = narrow(value)
            remote(
                z_out.at[j, stream],
                z_in.at[j, stream],
                z_send.at[0],
                z_recv.at[sems[stream]],
                cfd=flip(me, near * peer),
            ).start()

    def z_wait(j, stream):
        wait_all(z_in.at[j, stream], z_recv.at[1 + stream])

    send_core(3)
    send_core(2)
    send_first(3)
    send_core(1)
    send_first(2)
    send_core(0)
    send_second(3)
    send_first(1)
    send_second(2)
    send_first(0)
    send_z(3, 1, 0, (1, 2))
    send_second(1)
    send_z(2, 2, 3, (0, 0))
    send_second(0)
    send_z(1, 1, 0, (0, 0))
    results = list(finish_second(0))
    wait_all(outgoing.at[pl.ds(1, owners - 1)], block_send.at[0])
    wait_all(core_out, core_send.at[0])
    wait_all(x_out, first_send.at[0])
    wait_all(y_out, first_send.at[1])
    wait_all(xy_out, second_send.at[0])
    wait_all(z_out.at[pl.ds(1, zs - 1)], z_send.at[0])
    wait_all(z_in.at[pl.ds(1, 2)], z_recv.at[0])
    for j in (1, 2):
        results = [value + wide_of(z_in[j, s]) for s, value in enumerate(results)]
    for value, result_ref in zip(results, (first_ref, second_ref)):
        result_ref[...] = value


def send_order(k, near):
    j = k // near
    return (3, 0, 1, 2)[j] if j < 4 else j, k


def fused(surface_raw, area_normals, kernel_weights, block_map, band_observers, band_lags):
    owners, halves = lax.axis_size("cfd"), lax.axis_size("ac")
    faces, steps = surface_raw.shape[1:]
    taps, terms, observers, _ = kernel_weights.shape
    bands, width = band_observers.shape
    size, height = faces // owners, observers // owners
    chunks = steps // 2 // LANES
    zs = owners // 4
    near = owners // zs
    bf16, f32, i32 = jnp.bfloat16, jnp.float32, jnp.int32
    tile = (height, LANES)
    dma = pltpu.SemaphoreType.DMA
    vmem, hbm = (pl.BlockSpec(memory_space=space) for space in (pltpu.VMEM, pltpu.HBM))
    pieces = 4
    span = steps // pieces
    first, second = pl.pallas_call(
        fused_kernel,
        out_shape=[jax.ShapeDtypeStruct(tile, f32)] * 2,
        in_specs=[hbm] * 6,
        out_specs=[vmem, vmem],
        scratch_shapes=[
            pltpu.SMEM((bands,), i32),
            pltpu.SMEM((owners,), i32),
            pltpu.VMEM((bands, width), i32),
            pltpu.VMEM(area_normals.shape, bf16),
            [pltpu.VMEM((surface_raw.shape[0], owners, size, span), bf16)] * pieces,
            pltpu.VMEM(kernel_weights.shape, bf16),
            pltpu.VMEM((owners, size, LANES), f32),
            pltpu.VMEM((owners, pieces, 2, size, span), bf16),
            pltpu.VMEM((pieces, owners, 2, size, span), bf16),
            pltpu.VMEM((taps * terms * faces, span), bf16),
            pltpu.VMEM((4,) + tile, f32),
            pltpu.VMEM((steps // LANES, bands, width, LANES), f32),
            pltpu.VMEM((bands, width, LANES), i32),
            pltpu.VMEM((observers // LANES, LANES), i32),
            pltpu.SMEM((observers // LANES, LANES), i32),
            pltpu.VMEM((observers * chunks, LANES), f32),
            pltpu.VMEM((observers * chunks, LANES), f32),
            pltpu.VMEM((zs, 2, chunks) + tile, bf16),
            pltpu.VMEM((zs, 2, chunks) + tile, bf16),
            pltpu.VMEM((zs, 2) + tile, bf16),
            pltpu.VMEM((zs, 2) + tile, bf16),
            pltpu.VMEM((zs, 2) + tile, f32),
            pltpu.VMEM((zs, 2) + tile, bf16),
            pltpu.VMEM((zs, 2) + tile, bf16),
            pltpu.VMEM((zs, 2) + tile, f32),
            pltpu.VMEM((2, zs) + tile, bf16),
            pltpu.VMEM((2, zs) + tile, bf16),
            pltpu.VMEM((zs, 2) + tile, bf16),
            pltpu.VMEM((zs, 2) + tile, bf16),
            dma((7 + pieces,)),
            dma((1,)),
            dma((pieces,)),
            dma((1,)),
            dma((zs,)),
            dma((2,)),
            dma((2, 2, zs)),
            dma((1,)),
            dma((2, zs)),
            dma((1,)),
            dma((3,)),
        ],
        compiler_params=pltpu.CompilerParams(
            collective_id=0, has_side_effects=True, vmem_limit_bytes=40 * 2**20
        ),
        name="fused",
    )(
        *(
            pltpu.with_memory_space_constraint(value, pltpu.HBM)
            for value in (
                band_lags,
                block_map[0, 0],
                band_observers,
                area_normals,
                surface_raw.reshape(surface_raw.shape[0], owners, size, steps),
                kernel_weights,
            )
        )
    )
    return jnp.concatenate([first, second], axis=1)


def fits_fused(owners, halves, surface_raw, kernel_weights, band_observers):
    faces, steps = surface_raw.shape[1:]
    tiles = halves * 2
    return (
        halves == 2
        and owners == 4 * 4
        and faces == LANES
        and band_observers.shape[1] == LANES
        and faces // owners % 8 == 0
        and steps == 2 * tiles * LANES
        and kernel_weights.shape[:1] + kernel_weights.shape[2:3] == (2, owners * LANES)
        and band_observers.shape[0] % 8 == 0
    )


def general(surface_raw, area_normals, kernel_weights, block_map, band_observers, band_lags):
    blocks = lax.axis_size("cfd")
    faces, steps = surface_raw.shape[1:]
    size = faces // blocks
    outgoing = prepare(surface_raw, area_normals, block_map[0, 0])
    arrived = lax.all_to_all(outgoing, "cfd", split_axis=0, concat_axis=0, tiled=True)
    arrived = arrived.reshape(blocks, 2, size, steps)
    if size % 8:
        arrived = arrived.transpose(1, 0, 2, 3).reshape(2 * faces, steps)
    shape = (blocks // 2, kernel_weights.shape[2] // blocks, steps // 2)
    kept, sent = banded_call(
        halves_kernel,
        [jax.ShapeDtypeStruct(shape, kind) for kind in (jnp.float32, jnp.bfloat16)],
        arrived,
        kernel_weights,
        band_observers,
        band_lags,
        (lax.axis_index("cfd") & 1).astype(jnp.int32).reshape(1),
    )
    return exchange_sums(kept, sent)


def local(surface_raw, area_normals, kernel_weights, block_map, band_observers, band_lags):
    owners, halves = lax.axis_size("cfd"), lax.axis_size("ac")
    fast = fits_fused(owners, halves, surface_raw, kernel_weights, band_observers)
    run = fused if fast else general
    return run(surface_raw, area_normals, kernel_weights, block_map, band_observers, band_lags)


def solution(mesh):
    placed = (
        P(None, ("cfd", "ac"), None),
        P(None, ("cfd", "ac")),
        P(None, None, None, ("cfd", "ac")),
        P("ac", "cfd", None),
        P(),
        P(),
    )
    return jax.shard_map(
        local, mesh=mesh, in_specs=placed, out_specs=P("cfd", "ac"), check_vma=False
    )
```
